32 devices in a mesh: mem: 4 (over x, core), lat: 8 (over z, y).
Axes of the slice: x: 2, y: 2, z: 4, core: 2. Of those that a mesh axis runs over, the one named last changes fastest.
Arguments:
- perturbation: bfloat16 [64, 128, 2048], P('mem', 'lat'), may hold values from -6 to 6
- obs_cells: int32 [8, 2048], P('lat'), may hold values from 0 to 32767
- obs_count: int32 [8], P('lat'), may hold values from 682 to 2048, as said below
- innovation: float32 [8, 2048], P('lat'), may hold values from -8 to 8
- obs_scale: float32 [8, 2048], P('lat'), may hold values from 0.3 to 3
Outputs:
- control: float32 [64, 64, 1024], P('mem', 'lat')
- increment: float32 [128, 2048], P('lat', 'mem')
The draws below stay inside these ranges and needn't reach their ends.
Inputs may be any that keep to these rules, and one draw needn't show every extreme that they name: `obs_count`: at most 2048 live slots in a band, and some band has exactly 2048.
All inputs are finite; a program needn't handle non-finite values.
Results may differ from the reference program's by a relative error of at most 0.00035.
Values sent between devices are 32-bit elements; how exact they have to be, the bound alone decides.
No kernel may reach another device: no remote copies, remote signals or barrier semaphores. Data moves between devices by JAX's collectives and lax.ppermute only.
A program may use at most 64 MiB of HBM per device.

```python
import math
import jax
import jax.numpy as jnp
from jax import lax

MEM_DEV = 16
MEMBERS = 64
FROWS = 16
NLON = 2048
HALO = 8
LSIG = 3
OBS = 2048
ITERS = 3
BANDS = 8
NFR = 128
NCR = 64
NLONC = 1024
N_MEM = 4


def draw_obs_count(key, part):
    base = jax.random.fold_in(key, 11)
    count_key, band_key = jax.random.split(base)
    counts = jax.random.randint(count_key, (BANDS,), OBS // 3, OBS + 1)
    full_band = jax.random.randint(band_key, (), 0, BANDS)
    return jnp.where(jnp.arange(BANDS) == full_band, OBS, counts).astype(jnp.int32)


def set_ends(values, key, smallest, largest):
    dims = values.shape
    place = [jax.random.randint(jax.random.fold_in(key, axis), (), 0, dims[axis]) for axis in range(len(dims))]
    values = values.at[tuple(place)].set(smallest)
    longest = dims.index(max(dims))
    place[longest] = (place[longest] + 1) % dims[longest]
    return values.at[tuple(place)].set(largest)


def steps_of(key, shape, cuts, low, top_value):
    loudness = 1.0
    for position, parts in cuts:
        draws = jax.random.uniform(jax.random.fold_in(jax.random.fold_in(key, 6), position), (parts,), jnp.float32, low / len(cuts), top_value / len(cuts))
        loudness = loudness * jnp.repeat(jnp.exp(draws), shape[position] // parts).reshape((-1,) + (1,) * (len(shape) - 1 - position))
    return loudness


def noise(own_key, shape, deviation, most, cuts=(), held_as=jnp.bfloat16):
    result = deviation * jax.random.normal(own_key, shape, jnp.float32)
    if cuts:
        result = result * steps_of(own_key, shape, cuts, -0.22, 0.18)
    return jnp.clip(result, -most, most).astype(held_as)


def setup_inputs(seed: int = 0) -> dict:
    arg_keys = jax.random.split(jax.random.key(seed), 6)
    return {
        "perturbation": noise(arg_keys[0], (MEMBERS, NFR, NLON), 1.0, 6.0, ((0, 4), (1, 8))),
        "obs_cells": set_ends(jax.random.randint(arg_keys[1], (BANDS, OBS), 0, FROWS * NLON), jax.random.fold_in(arg_keys[1], 1), 0, (FROWS * NLON) - 1).astype(jnp.int32),
        "obs_count": draw_obs_count(jax.random.fold_in(arg_keys[5], 71), 0),
        "innovation": noise(arg_keys[3], (BANDS, OBS), 2.0, 8.0, ((0, 8),), jnp.float32),
        "obs_scale": jnp.clip(jnp.exp(math.log(3.0) - 2.3025851 * jax.random.uniform(arg_keys[4], (BANDS, OBS), jnp.float32) ** steps_of(arg_keys[4], (BANDS, OBS), ((0, 8),), -0.2, 0.2)), 0.3, 3.0),
    }


def lat_weights():
    offsets = jnp.arange(2 * HALO + 1).astype(jnp.float32) - HALO
    spread = HALO / 2.0
    return 0.5 * jnp.exp(-offsets * offsets / (2.0 * spread * spread))


def lon_weights(coarse_cols):
    columns = jnp.arange(coarse_cols).astype(jnp.int32)
    distance = jnp.abs(columns[:, None] - columns[None, :])
    distance = jnp.minimum(distance, coarse_cols - distance).astype(jnp.float32)
    return jnp.exp(-distance * distance / (2.0 * LSIG * LSIG))


def lat_apply(padded, row_count, lat_taps):
    filtered = lat_taps[0] * padded[:, 0:row_count]
    for offset in range(1, 2 * HALO + 1):
        filtered = filtered + lat_taps[offset] * padded[:, offset:offset + row_count]
    return filtered


def widen_lon(coarse):
    odd_part = 0.5 * (coarse + jnp.roll(coarse, -1, axis=-1))
    return jnp.stack([coarse, odd_part], axis=-1).reshape(coarse.shape[:-1] + (2 * coarse.shape[-1],))


def narrow_lon(fine):
    paired = fine.reshape(fine.shape[:-1] + (fine.shape[-1] // 2, 2))
    odd_part = paired[..., 1]
    return paired[..., 0] + 0.5 * odd_part + 0.5 * jnp.roll(odd_part, 1, axis=-1)


def reference(perturbation, obs_cells, obs_count, innovation, obs_scale):
    lat_taps = lat_weights()
    circulant = lon_weights(NLONC)
    member_scale = (MEMBERS - 1) ** -0.5
    groups = perturbation.reshape(N_MEM, MEM_DEV, NFR, NLON)

    def forward(direction):
        padded = jnp.pad(direction, ((0, 0), (HALO, HALO), (0, 0)))
        smoothed = lat_apply(padded, NCR, lat_taps).reshape(N_MEM, MEM_DEV, NCR, NLONC)

        def accumulate(running, block):
            smooth_block, pert_block = block
            along = jnp.dot(smooth_block, circulant, precision=lax.Precision.HIGHEST, preferred_element_type=jnp.float32)
            fine_block = jnp.repeat(widen_lon(along), 2, axis=1)
            return running + jnp.sum(pert_block.astype(jnp.float32) * fine_block, axis=0) * member_scale, None

        image_field, unused = lax.scan(accumulate, jnp.zeros((NFR, NLON), jnp.float32), (smoothed, groups))
        return image_field

    def adjoint(obs_field):
        def fold(pert_block):
            weighted = pert_block.astype(jnp.float32) * obs_field[None] * member_scale
            folded = narrow_lon(weighted.reshape(MEM_DEV, NCR, 2, NLON).sum(axis=2))
            return jnp.dot(folded, circulant, precision=lax.Precision.HIGHEST, preferred_element_type=jnp.float32)

        coarse = lax.map(fold, groups).reshape(MEMBERS, NCR, NLONC)
        padded = jnp.pad(coarse, ((0, 0), (HALO, HALO), (0, 0)))
        return lat_apply(padded, NCR, lat_taps)

    band_start = (jnp.arange(BANDS).astype(jnp.int32) * (FROWS * NLON))[:, None]
    flat_index = (obs_cells.astype(jnp.int32) + band_start).reshape(-1)
    active = (jnp.arange(OBS).astype(jnp.int32)[None, :] < obs_count[:, None]).reshape(-1)
    target = innovation.reshape(-1)
    saturation = obs_scale.reshape(-1)
    control = jnp.zeros((MEMBERS, NCR, NLONC), jnp.float32)
    increment = jnp.zeros((NFR, NLON), jnp.float32)
    observed = jnp.zeros((BANDS * OBS,), jnp.float32)
    for iteration in range(ITERS):
        misfit = target - observed
        bounded = jnp.tanh(misfit / saturation)
        pull = jnp.where(active, saturation * bounded, 0.0)
        weight = jnp.where(active, 1.0 - bounded * bounded, 0.0)
        obs_field = jnp.zeros((NFR * NLON,), jnp.float32).at[flat_index].add(pull).reshape(NFR, NLON)
        gradient = control - adjoint(obs_field)
        grad_norm = jnp.sum(gradient * gradient)
        direction = -gradient
        image_field = forward(direction)
        hits = image_field.reshape(-1)[flat_index]
        bending = jnp.sum(weight * hits * hits)
        step_size = grad_norm / (grad_norm + bending + 1e-6)
        control = control + step_size * direction
        increment = increment + step_size * image_field
        observed = observed + step_size * hits
    return control, increment
```

```python
import functools

import jax
import jax.numpy as jnp
import numpy as np
from jax import lax
from jax.experimental import pallas as pl
from jax.experimental.pallas import tpu as pltpu
from jax.sharding import PartitionSpec as P

HALO = 8
LSIG = 3
ITERS = 3
REACH = 2
NREL = 2 * REACH + 1
BLK = 256
EDGE = 128
META = 8


def lat_tables(bands, coarse_rows):
    rows = bands * coarse_rows
    offset = np.arange(rows)[:, None] - np.arange(rows)[None, :]
    spread = HALO / 2.0
    r1 = np.where(np.abs(offset) <= HALO, 0.5 * np.exp(-offset * offset / (2.0 * spread * spread)), 0.0)
    r2 = r1 @ r1
    out = np.zeros((bands, 2, NREL, coarse_rows, 128), np.float32)
    for b in range(bands):
        for d in range(NREL):
            s = b + d - REACH
            if 0 <= s < bands:
                own = slice(b * coarse_rows, (b + 1) * coarse_rows)
                other = slice(s * coarse_rows, (s + 1) * coarse_rows)
                out[b, 0, d, :, :coarse_rows] = r2[own, other]
                out[b, 1, d, :, :coarse_rows] = r1[own, other]
    return out


def lon_blocks(coarse_cols):
    d = np.arange(coarse_cols)
    d = np.minimum(d, coarse_cols - d).astype(np.float32)
    c1 = np.exp(-d * d / np.float32(2.0 * LSIG * LSIG)).astype(np.float32).astype(np.float64)
    c2 = np.real(np.fft.ifft(np.fft.fft(c1) ** 2))
    away = np.arange(BLK + 2 * EDGE)[:, None] - EDGE - np.arange(BLK)[None, :]
    inside = np.abs(away) <= EDGE
    blocks = []
    for c in (c1, c2):
        t = jnp.asarray(np.where(inside, c[away % coarse_cols], 0.0).astype(np.float32))
        hi = t.astype(jnp.bfloat16)
        lo = (t - hi.astype(jnp.float32)).astype(jnp.bfloat16)
        blocks.append(jnp.stack([hi, lo]))
    return blocks


def split(a):
    hi = a.astype(jnp.bfloat16)
    return hi, (a - hi.astype(jnp.float32)).astype(jnp.bfloat16)


def dot(a, b, dims=((1,), (0,))):
    return lax.dot_general(a, b, (dims, ((), ())), preferred_element_type=jnp.float32)


def full(ref_shape, dim):
    return lax.broadcasted_iota(jnp.int32, ref_shape, dim).astype(jnp.float32)


def pick_kernel(p_ref, meta_ref, out_ref, *, members, fine_rows, chunk):
    lon = p_ref.shape[1]
    slots = meta_ref.shape[1]

    def body(n, _):
        at = pl.ds(pl.multiple_of(n * chunk, chunk), chunk)
        col = 2.0 * meta_ref[0:1, at]
        row = meta_ref[1:2, at]
        one = jnp.where(full((lon, chunk), 0) == col, 1.0, 0.0).astype(jnp.bfloat16)
        got = dot(p_ref[...], one).reshape(members, fine_rows, chunk)
        mask = jnp.where(full((fine_rows, chunk), 0) == row, 1.0, 0.0)
        out_ref[0:members, at] = jnp.sum(got * mask[None], axis=1)
        out_ref[members : members + META, at] = meta_ref[:, at]
        return 0

    lax.fori_loop(0, slots // chunk, body, 0)


def scatter(q_ref, tab, v_of, first, last, lhs_ref, x_ref, members, coarse_rows):
    cols = x_ref.shape[1]
    slots = q_ref.shape[2]
    half = members * coarse_rows
    x_ref[...] = jnp.zeros_like(x_ref)

    def band(d, _):
        at_col = q_ref[d, members : members + 1, :]
        row = jnp.floor(q_ref[d, members + 1 : members + 2, :] * 0.5)
        v = v_of(d)
        weights = jnp.zeros((coarse_rows, slots), jnp.float32)
        for r in range(coarse_rows):
            weights = jnp.where(row == float(r), tab[d, :, r : r + 1], weights)
        weights = weights * v
        for k in range(members):
            hi, lo = split(weights * q_ref[d, k : k + 1, :])
            lhs_ref[k * coarse_rows : (k + 1) * coarse_rows, :] = hi
            lhs_ref[half + k * coarse_rows : half + (k + 1) * coarse_rows, :] = lo

        def block(c, _):
            base = (c * BLK).astype(jnp.float32)
            near = jnp.where(jnp.logical_and(c == 0, at_col > cols - 1.0), at_col - float(cols), at_col)
            hat = jnp.maximum(1.0 - jnp.abs((near - base) - full((BLK, slots), 0)), 0.0)
            got = dot(lhs_ref[...], hat.astype(jnp.bfloat16), ((1,), (1,)))
            at = pl.ds(pl.multiple_of(c * BLK, BLK), BLK)
            x_ref[:, at] = x_ref[:, at] + (got[:half] + got[half:])
            return 0

        return lax.fori_loop(0, cols // BLK, block, 0)

    lax.fori_loop(first, last, band, 0)


def lon_filter(x, t_ref):
    half, cols = x.shape
    ext = jnp.concatenate([x[:, cols - EDGE :], x, x[:, :EDGE]], axis=1)
    hi, lo = split(ext)
    parts = []
    for c in range(cols // BLK):
        at = slice(c * BLK, (c + 1) * BLK + 2 * EDGE)
        parts.append(dot(hi[:, at], t_ref[0]) + dot(lo[:, at], t_ref[0]) + dot(hi[:, at], t_ref[1]))
    return jnp.concatenate(parts, axis=1)


def step_of(hits, v, w):
    gg = jnp.sum(v * hits)
    cc = jnp.sum(w * hits * hits)
    gg = jnp.full((1, 128), gg, jnp.float32)
    cc = jnp.full((1, 128), cc, jnp.float32)
    return gg / (gg + cc + 1e-6)


def iter_kernel(slot_ref, obs_ref, q_ref, tab_ref, t2_ref, *refs, members, coarse_rows, scale2, first):
    if first:
        (part_ref, b_ref, state_ref, lhs_ref, x_ref, bhl_ref) = refs
    else:
        (old_ref, hits_ref, part_ref, b_ref, state_ref, step_ref, lhs_ref, x_ref, bhl_ref) = refs
    slots = q_ref.shape[2]
    cols = x_ref.shape[1]
    half = members * coarse_rows
    target, saturation, live = obs_ref[0], obs_ref[1], obs_ref[2]
    if first:
        observed = jnp.zeros_like(target)
        lam = jnp.zeros_like(target)
    else:
        hits = hits_ref[...]
        step = step_of(hits, old_ref[0], old_ref[1])
        step_ref[...] = step
        observed = old_ref[2] + step[0:1, 0:1] * hits
        lam = old_ref[3] + step[0:1, 0:1] * old_ref[0]
    bounded = jnp.tanh((target - observed) / saturation)
    v = jnp.where(live > 0.5, saturation * bounded, 0.0) - lam
    state_ref[0] = v
    state_ref[1] = jnp.where(live > 0.5, 1.0 - bounded * bounded, 0.0)
    state_ref[2] = observed
    state_ref[3] = lam

    def v_of(d):
        return state_ref[0, pl.ds(slot_ref[d], 1), :]

    scatter(q_ref, tab_ref, v_of, 0, NREL, lhs_ref, x_ref, members, coarse_rows)
    b = lon_filter(x_ref[...], t2_ref)
    b_ref[...] = b
    hi, lo = split(b)
    bhl_ref[:half] = hi
    bhl_ref[half:] = lo
    chunk = 512

    def gather(n, _):
        at = pl.ds(pl.multiple_of(n * chunk, chunk), chunk)
        at_col = q_ref[REACH, members : members + 1, at]
        row = jnp.floor(q_ref[REACH, members + 1 : members + 2, at] * 0.5)
        away = jnp.abs(at_col - full((cols, chunk), 0))
        hat = jnp.maximum(1.0 - jnp.minimum(away, cols - away), 0.0).astype(jnp.bfloat16)
        got = dot(bhl_ref[...], hat)
        mask = jnp.where(full((coarse_rows, chunk), 0) == row, scale2, 0.0)
        total = jnp.zeros((coarse_rows, chunk), jnp.float32)
        for k in range(members):
            r = slice(k * coarse_rows, (k + 1) * coarse_rows)
            r2 = slice(half + k * coarse_rows, half + (k + 1) * coarse_rows)
            total = total + q_ref[REACH, k : k + 1, at] * (got[r] + got[r2])
        part_ref[:, at] = jnp.sum(total * mask, axis=0, keepdims=True)
        return 0

    lax.fori_loop(0, slots // chunk, gather, 0)


def final_kernel(
    slot_ref, state_ref, hits_ref, q_ref, tab_ref, t1_ref, b0_ref, b1_ref, b2_ref, s0_ref, s1_ref, p_ref,
    control_ref, image_ref, lam_ref, lhs_ref, x_ref, *, members, fine_rows, coarse_rows, scale,
):
    hits = hits_ref[...]
    v = state_ref[0]
    step = step_of(hits, v, state_ref[1])[0:1, 0:1]
    lam_ref[...] = state_ref[3] + step * v

    def v_of(d):
        return lam_ref[pl.ds(slot_ref[d], 1), :]

    scatter(q_ref, tab_ref, v_of, REACH - 1, REACH + 2, lhs_ref, x_ref, members, coarse_rows)
    control_ref[...] = scale * lon_filter(x_ref[...], t1_ref)

    b = s0_ref[0:1, 0:1] * b0_ref[...] + s1_ref[0:1, 0:1] * b1_ref[...] + step * b2_ref[...]
    half, cols = b.shape
    wide = 2 * half
    repeat = jnp.where(
        lax.broadcasted_iota(jnp.int32, (wide, half), 0) // 2 == lax.broadcasted_iota(jnp.int32, (wide, half), 1), 1.0, 0.0
    ).astype(jnp.bfloat16)
    hi, lo = split(jnp.concatenate([b, b[:, :EDGE]], axis=1))
    hi = dot(repeat, hi).astype(jnp.bfloat16)
    lo = dot(repeat, lo).astype(jnp.bfloat16)
    hat = jnp.maximum(1.0 - jnp.abs(0.5 * full((2 * EDGE, 2 * EDGE), 1) - full((2 * EDGE, 2 * EDGE), 0)), 0.0)
    hat = hat.astype(jnp.bfloat16)
    for f in range(cols // EDGE):
        at = slice(f * EDGE, f * EDGE + 2 * EDGE)
        fine = slice(2 * f * EDGE, 2 * (f + 1) * EDGE)
        field = dot(hi[:, at], hat) + dot(lo[:, at], hat)
        product = p_ref[:, fine].astype(jnp.float32) * field
        image_ref[:, fine] = (scale * scale) * jnp.sum(product.reshape(members, fine_rows, 2 * EDGE), axis=0)


def swap(a, axis, bit):
    count = lax.axis_size(axis)
    return lax.ppermute(a, axis, [(i, i ^ bit) for i in range(count)])


def gather_lat(a, dim):
    bit = 1
    while bit < lax.axis_size("lat"):
        a = jnp.concatenate([a, swap(a, "lat", bit)], axis=dim)
        bit *= 2
    return a


def sum_mem(a):
    bit = 1
    while bit < lax.axis_size("mem"):
        a = a + swap(a, "mem", bit)
        bit *= 2
    return a


def scatter_mem(a):
    bit = lax.axis_size("mem") // 2
    me = lax.axis_index("mem")
    while bit:
        width = a.shape[1] // 2
        low, high = a[:, :width], a[:, width:]
        upper = (me & bit) != 0
        a = jnp.where(upper, high, low) + swap(jnp.where(upper, low, high), "mem", bit)
        bit //= 2
    return a


def on_device(perturbation, obs_cells, obs_count, innovation, obs_scale):
    bands = lax.axis_size("lat")
    members, fine_rows, lon_cells = perturbation.shape
    coarse_rows = fine_rows // 2
    coarse_cols = lon_cells // 2
    slots = obs_cells.shape[1]
    half = members * coarse_rows
    scale = float((members * lax.axis_size("mem") - 1) ** (-0.5))
    band = lax.axis_index("lat")
    t1, t2 = lon_blocks(coarse_cols)
    tables = lax.dynamic_index_in_dim(jnp.asarray(lat_tables(bands, coarse_rows)), band, 0, keepdims=False)
    slot = (band ^ (band + jnp.arange(NREL, dtype=jnp.int32) - REACH)) & (bands - 1)

    smem = pl.BlockSpec(memory_space=pltpu.SMEM)
    vmem = pl.BlockSpec(memory_space=pltpu.VMEM)
    f32 = functools.partial(jax.ShapeDtypeStruct, dtype=jnp.float32)

    live = (jnp.arange(slots, dtype=jnp.int32)[None] < obs_count[0]).astype(jnp.float32)
    obs = gather_lat(jnp.stack([innovation, obs_scale, live]), 1)

    field = perturbation.reshape(members * fine_rows, lon_cells)
    meta = jnp.concatenate(
        [
            (obs_cells % lon_cells).astype(jnp.float32) * 0.5,
            (obs_cells // lon_cells).astype(jnp.float32),
            jnp.zeros((META - 2, slots), jnp.float32),
        ]
    )
    own = pl.pallas_call(
        functools.partial(pick_kernel, members=members, fine_rows=fine_rows, chunk=256),
        out_shape=f32((members + META, slots)),
        in_specs=[vmem, vmem],
        out_specs=vmem,
        cost_estimate=pl.CostEstimate(flops=4 * 10**9, bytes_accessed=2 * 10**6, transcendentals=0),
        name="pick",
    )(field, meta)
    near = []
    for d in range(-REACH, REACH + 1):
        near.append(lax.ppermute(own, "lat", [(s, s - d) for s in range(bands) if 0 <= s - d < bands]) if d else own)
    near = jnp.stack(near)

    scratch = [pltpu.VMEM((2 * half, slots), jnp.bfloat16), pltpu.VMEM((half, coarse_cols), jnp.float32)]
    state, hits, images, steps = None, None, [], []
    for iteration in range(ITERS):
        first = iteration == 0
        ins = [slot, obs, near, tables[0], t2] + ([] if first else [state, hits])
        outs = [f32((1, slots)), f32((half, coarse_cols)), f32((4, bands, slots))] + ([] if first else [f32((1, 128))])
        got = pl.pallas_call(
            functools.partial(iter_kernel, members=members, coarse_rows=coarse_rows, scale2=scale * scale, first=first),
            out_shape=outs,
            in_specs=[smem] + [vmem] * (len(ins) - 1),
            out_specs=[vmem] * len(outs),
            scratch_shapes=scratch + [pltpu.VMEM((2 * half, coarse_cols), jnp.bfloat16)],
            cost_estimate=pl.CostEstimate(flops=7 * 10**9, bytes_accessed=3 * 10**6, transcendentals=0),
            name="iterate",
        )(*ins)
        part, image, state = got[:3]
        images.append(image)
        steps += got[3:]
        hits = gather_lat(sum_mem(part), 0)
    control, image = pl.pallas_call(
        functools.partial(final_kernel, members=members, fine_rows=fine_rows, coarse_rows=coarse_rows, scale=scale),
        out_shape=[f32((half, coarse_cols)), f32((fine_rows, lon_cells))],
        in_specs=[smem] + [vmem] * 11,
        out_specs=[vmem] * 2,
        scratch_shapes=[pltpu.VMEM((bands, slots), jnp.float32)] + scratch,
        cost_estimate=pl.CostEstimate(flops=5 * 10**9, bytes_accessed=6 * 10**6, transcendentals=0),
        name="finish",
    )(slot, state, hits, near, tables[1], t1, *images, *steps, field)
    return control.reshape(members, coarse_rows, coarse_cols), scatter_mem(image)


def solution(mesh):
    in_specs = (P("mem", "lat", None), P("lat", None), P("lat"), P("lat", None), P("lat", None))
    out_specs = (P("mem", "lat", None), P("lat", "mem"))
    return jax.shard_map(on_device, mesh=mesh, in_specs=in_specs, out_specs=out_specs, check_vma=False)
```

```python
import functools

import jax
import jax.numpy as jnp
import numpy as np
from jax import lax
from jax.experimental import pallas as pl
from jax.experimental.pallas import tpu as pltpu
from jax.sharding import PartitionSpec as P

HALO = 8
LSIG = 3
ITERS = 3
REACH = 2
NREL = 2 * REACH + 1
BLK = 256
EDGE = 128
META = 8


def lat_tables(bands, coarse_rows):
    rows = bands * coarse_rows
    offset = np.arange(rows)[:, None] - np.arange(rows)[None, :]
    spread = HALO / 2.0
    r1 = np.where(np.abs(offset) <= HALO, 0.5 * np.exp(-offset * offset / (2.0 * spread * spread)), 0.0)
    r2 = r1 @ r1
    out = np.zeros((bands, 2, NREL, coarse_rows, 128), np.float32)
    for b in range(bands):
        for d in range(NREL):
            s = b + d - REACH
            if 0 <= s < bands:
                own = slice(b * coarse_rows, (b + 1) * coarse_rows)
                other = slice(s * coarse_rows, (s + 1) * coarse_rows)
                out[b, 0, d, :, :coarse_rows] = r2[own, other]
                out[b, 1, d, :, :coarse_rows] = r1[own, other]
    return out


def lon_blocks(coarse_cols):
    d = np.arange(coarse_cols)
    d = np.minimum(d, coarse_cols - d).astype(np.float32)
    c1 = np.exp(-d * d / np.float32(2.0 * LSIG * LSIG)).astype(np.float32).astype(np.float64)
    c2 = np.real(np.fft.ifft(np.fft.fft(c1) ** 2))
    away = np.arange(BLK + 2 * EDGE)[:, None] - EDGE - np.arange(BLK)[None, :]
    inside = np.abs(away) <= EDGE
    blocks = []
    for c in (c1, c2):
        t = jnp.asarray(np.where(inside, c[away % coarse_cols], 0.0).astype(np.float32))
        hi = t.astype(jnp.bfloat16)
        lo = (t - hi.astype(jnp.float32)).astype(jnp.bfloat16)
        blocks.append(jnp.stack([hi, lo]))
    return blocks


def split(a):
    hi = a.astype(jnp.bfloat16)
    return hi, (a - hi.astype(jnp.float32)).astype(jnp.bfloat16)


def dot(a, b, dims=((1,), (0,))):
    return lax.dot_general(a, b, (dims, ((), ())), preferred_element_type=jnp.float32)


def full(ref_shape, dim):
    return lax.broadcasted_iota(jnp.int32, ref_shape, dim).astype(jnp.float32)


def hat_of(x, count):
    middle = 0.5 * (count - 1)
    near = x - middle
    near = jnp.where(jnp.abs(near) > middle + 0.75, float(count), near).astype(jnp.bfloat16)
    j = (full((count, x.shape[1]), 0) - middle).astype(jnp.bfloat16)
    one = jnp.asarray(1, jnp.bfloat16)
    return jnp.maximum(one - jnp.abs(near - j), jnp.asarray(0, jnp.bfloat16))


def pick_kernel(p_ref, meta_ref, out_ref, *, members, fine_rows, chunk):
    lon = p_ref.shape[1]
    slots = meta_ref.shape[1]

    def body(n, _):
        at = pl.ds(pl.multiple_of(n * chunk, chunk), chunk)
        col = 2.0 * meta_ref[0:1, at]
        row = meta_ref[1:2, at]
        one = jnp.where(full((lon, chunk), 0) == col, 1.0, 0.0).astype(jnp.bfloat16)
        got = dot(p_ref[...], one).reshape(members, fine_rows, chunk)
        mask = jnp.where(full((fine_rows, chunk), 0) == row, 1.0, 0.0)
        out_ref[0:members, at] = jnp.sum(got * mask[None], axis=1)
        out_ref[members : members + META, at] = meta_ref[:, at]
        return 0

    lax.fori_loop(0, slots // chunk, body, 0)


def scatter(q_ref, tab, v_of, first, last, lhs_ref, x_ref, members, coarse_rows):
    cols = x_ref.shape[1]
    slots = q_ref.shape[2]
    half = members * coarse_rows
    x_ref[...] = jnp.zeros_like(x_ref)

    def band(d, _):
        at_col = q_ref[d, members : members + 1, :]
        row = jnp.floor(q_ref[d, members + 1 : members + 2, :] * 0.5)
        v = v_of(d)
        weights = jnp.zeros((coarse_rows, slots), jnp.float32)
        for r in range(coarse_rows):
            weights = jnp.where(row == float(r), tab[d, :, r : r + 1], weights)
        weights = weights * v
        for k in range(members):
            hi, lo = split(weights * q_ref[d, k : k + 1, :])
            lhs_ref[k * coarse_rows : (k + 1) * coarse_rows, :] = hi
            lhs_ref[half + k * coarse_rows : half + (k + 1) * coarse_rows, :] = lo

        def block(c, _):
            base = (c * BLK).astype(jnp.float32)
            near = jnp.where(jnp.logical_and(c == 0, at_col > cols - 1.0), at_col - float(cols), at_col)
            got = dot(lhs_ref[...], hat_of(near - base, BLK), ((1,), (1,)))
            at = pl.ds(pl.multiple_of(c * BLK, BLK), BLK)
            x_ref[:, at] = x_ref[:, at] + (got[:half] + got[half:])
            return 0

        return lax.fori_loop(0, cols // BLK, block, 0)

    lax.fori_loop(first, last, band, 0)


def lon_filter(x, t_ref):
    half, cols = x.shape
    ext = jnp.concatenate([x[:, cols - EDGE :], x, x[:, :EDGE]], axis=1)
    hi, lo = split(ext)
    parts = []
    for c in range(cols // BLK):
        at = slice(c * BLK, (c + 1) * BLK + 2 * EDGE)
        parts.append(dot(hi[:, at], t_ref[0]) + dot(lo[:, at], t_ref[0]) + dot(hi[:, at], t_ref[1]))
    return jnp.concatenate(parts, axis=1)


def step_of(hits, v, w):
    gg = jnp.full((1, 128), jnp.sum(v * hits), jnp.float32)
    cc = jnp.full((1, 128), jnp.sum(w * hits * hits), jnp.float32)
    return gg / (gg + cc + 1e-6)


def sum_mem(parts):
    return lambda bands: jnp.sum(parts.reshape(parts.shape[0] // bands, bands, parts.shape[1]), axis=0)


def pull_of(target, saturation, live):
    bounded = jnp.tanh(target / saturation)
    return (
        jnp.where(live > 0.5, saturation * bounded, 0.0),
        jnp.where(live > 0.5, 1.0 - bounded * bounded, 0.0),
    )


def iter_kernel(slot_ref, q_ref, tab_ref, t2_ref, *refs, members, coarse_rows, scale2, order):
    slots = q_ref.shape[2]
    if order == 0:
        part_ref, b_ref, lhs_ref, x_ref, bhl_ref = refs

        def v_of(d):
            rows = q_ref[d, members : members + META, :]
            return pull_of(rows[2:3], rows[3:4], rows[4:5])[0]

    else:
        old_ref, hits_ref, part_ref, b_ref, state_ref, step_ref, lhs_ref, x_ref, bhl_ref = refs
        bands = old_ref.shape[1]
        hits = sum_mem(hits_ref[...])(bands)
        if order == 1:
            for b in range(bands):
                state_ref[0:3, b : b + 1, :] = old_ref[:, pl.ds(slot_ref[1, b], 1), :]
            v, w = pull_of(state_ref[0], state_ref[1], state_ref[2])
            observed, lam = 0.0, 0.0
        else:
            state_ref[0:3] = old_ref[0:3]
            v, w, observed, lam = old_ref[3], old_ref[4], old_ref[5], old_ref[6]
        step = step_of(hits, v, w)
        step_ref[...] = step
        observed = observed + step[0:1, 0:1] * hits
        lam = lam + step[0:1, 0:1] * v
        pull, weight = pull_of(state_ref[0] - observed, state_ref[1], state_ref[2])
        state_ref[3] = pull - lam
        state_ref[4] = weight
        state_ref[5] = observed
        state_ref[6] = lam

        def v_of(d):
            return state_ref[3, pl.ds(slot_ref[0, d], 1), :]

    cols = x_ref.shape[1]
    half = members * coarse_rows
    scatter(q_ref, tab_ref, v_of, 0, NREL, lhs_ref, x_ref, members, coarse_rows)
    b = lon_filter(x_ref[...], t2_ref)
    b_ref[...] = b
    hi, lo = split(b)
    bhl_ref[:half] = hi
    bhl_ref[half:] = lo
    chunk = 512

    def gather(n, _):
        at = pl.ds(pl.multiple_of(n * chunk, chunk), chunk)
        at_col = q_ref[REACH, members : members + 1, at]
        row = jnp.floor(q_ref[REACH, members + 1 : members + 2, at] * 0.5)
        hats = [hat_of(jnp.where(at_col > cols - 1.0, at_col - float(cols), at_col), BLK)]
        hats += [hat_of(at_col - float(c * BLK), BLK) for c in range(1, cols // BLK)]
        hat = jnp.concatenate(hats, axis=0)
        got = dot(bhl_ref[...], hat)
        mask = jnp.where(full((coarse_rows, chunk), 0) == row, scale2, 0.0)
        total = jnp.zeros((coarse_rows, chunk), jnp.float32)
        for k in range(members):
            r = slice(k * coarse_rows, (k + 1) * coarse_rows)
            r2 = slice(half + k * coarse_rows, half + (k + 1) * coarse_rows)
            total = total + q_ref[REACH, k : k + 1, at] * (got[r] + got[r2])
        part_ref[:, at] = jnp.broadcast_to(jnp.sum(total * mask, axis=0, keepdims=True), (part_ref.shape[0], chunk))
        return 0

    lax.fori_loop(0, slots // chunk, gather, 0)


def final_kernel(
    slot_ref, state_ref, hits_ref, q_ref, tab_ref, t1_ref, b0_ref, b1_ref, b2_ref, s0_ref, s1_ref, p_ref,
    control_ref, image_ref, lam_ref, lhs_ref, x_ref, *, members, fine_rows, coarse_rows, scale,
):
    hits = sum_mem(hits_ref[...])(state_ref.shape[1])
    v = state_ref[3]
    step = step_of(hits, v, state_ref[4])[0:1, 0:1]
    lam_ref[...] = state_ref[6] + step * v

    def v_of(d):
        return lam_ref[pl.ds(slot_ref[0, d], 1), :]

    scatter(q_ref, tab_ref, v_of, REACH - 1, REACH + 2, lhs_ref, x_ref, members, coarse_rows)
    control_ref[...] = scale * lon_filter(x_ref[...], t1_ref)

    b = s0_ref[0:1, 0:1] * b0_ref[...] + s1_ref[0:1, 0:1] * b1_ref[...] + step * b2_ref[...]
    half, cols = b.shape
    wide = 2 * half
    repeat = jnp.where(
        lax.broadcasted_iota(jnp.int32, (wide, half), 0) // 2 == lax.broadcasted_iota(jnp.int32, (wide, half), 1), 1.0, 0.0
    ).astype(jnp.bfloat16)
    hi, lo = split(jnp.concatenate([b, b[:, :EDGE]], axis=1))
    hi = dot(repeat, hi).astype(jnp.bfloat16)
    lo = dot(repeat, lo).astype(jnp.bfloat16)
    hat = jnp.maximum(1.0 - jnp.abs(0.5 * full((2 * EDGE, 2 * EDGE), 1) - full((2 * EDGE, 2 * EDGE), 0)), 0.0)
    hat = hat.astype(jnp.bfloat16)
    for f in range(cols // EDGE):
        at = slice(f * EDGE, f * EDGE + 2 * EDGE)
        fine = slice(2 * f * EDGE, 2 * (f + 1) * EDGE)
        field = dot(hi[:, at], hat) + dot(lo[:, at], hat)
        product = p_ref[:, fine].astype(jnp.float32) * field
        image_ref[:, fine] = (scale * scale) * jnp.sum(product.reshape(members, fine_rows, 2 * EDGE), axis=0)


def swap(a, axis, bit):
    count = lax.axis_size(axis)
    return lax.ppermute(a, axis, [(i, i ^ bit) for i in range(count)])


def gather_lat(a, dim):
    bit = 1
    while bit < lax.axis_size("lat"):
        a = jnp.concatenate([a, swap(a, "lat", bit)], axis=dim)
        bit *= 2
    return a


def scatter_mem(a):
    bit = lax.axis_size("mem") // 2
    me = lax.axis_index("mem")
    while bit:
        width = a.shape[1] // 2
        low, high = a[:, :width], a[:, width:]
        upper = (me & bit) != 0
        a = jnp.where(upper, high, low) + swap(jnp.where(upper, low, high), "mem", bit)
        bit //= 2
    return a


def on_device(perturbation, obs_cells, obs_count, innovation, obs_scale):
    bands = lax.axis_size("lat")
    members, fine_rows, lon_cells = perturbation.shape
    coarse_rows = fine_rows // 2
    coarse_cols = lon_cells // 2
    slots = obs_cells.shape[1]
    half = members * coarse_rows
    scale = float((members * lax.axis_size("mem") - 1) ** (-0.5))
    band = lax.axis_index("lat")
    t1, t2 = lon_blocks(coarse_cols)
    tables = lax.dynamic_index_in_dim(jnp.asarray(lat_tables(bands, coarse_rows)), band, 0, keepdims=False)
    every = jnp.arange(max(NREL, bands), dtype=jnp.int32)
    slot = jnp.stack([jnp.clip(band + every - REACH, 0, bands - 1), (band ^ every) & (bands - 1)])

    smem = pl.BlockSpec(memory_space=pltpu.SMEM)
    vmem = pl.BlockSpec(memory_space=pltpu.VMEM)
    f32 = functools.partial(jax.ShapeDtypeStruct, dtype=jnp.float32)

    live = (jnp.arange(slots, dtype=jnp.int32)[None] < obs_count[0]).astype(jnp.float32)
    obs = gather_lat(jnp.stack([innovation, obs_scale, live]), 1)

    field = perturbation.reshape(members * fine_rows, lon_cells)
    meta = jnp.concatenate(
        [
            (obs_cells % lon_cells).astype(jnp.float32) * 0.5,
            (obs_cells // lon_cells).astype(jnp.float32),
            innovation,
            obs_scale,
            live,
            jnp.zeros((META - 5, slots), jnp.float32),
        ]
    )
    own = pl.pallas_call(
        functools.partial(pick_kernel, members=members, fine_rows=fine_rows, chunk=256),
        out_shape=f32((members + META, slots)),
        in_specs=[vmem, vmem],
        out_specs=vmem,
        cost_estimate=pl.CostEstimate(flops=4 * 10**9, bytes_accessed=2 * 10**6, transcendentals=0),
        name="pick",
    )(field, meta)
    near = []
    for d in range(-REACH, REACH + 1):
        near.append(lax.ppermute(own, "lat", [(s, s - d) for s in range(bands) if 0 <= s - d < bands]) if d else own)
    near = jnp.stack(near)

    scratch = [pltpu.VMEM((2 * half, slots), jnp.bfloat16), pltpu.VMEM((half, coarse_cols), jnp.float32)]
    state, hits, images, steps = obs, None, [], []
    devices = bands * lax.axis_size("mem")
    for iteration in range(ITERS):
        ins = [slot, near, tables[0], t2] + ([state, hits] if iteration else [])
        outs = [f32((devices, slots)), f32((half, coarse_cols))] + ([f32((7, bands, slots)), f32((1, 128))] if iteration else [])
        got = pl.pallas_call(
            functools.partial(
                iter_kernel, members=members, coarse_rows=coarse_rows, scale2=scale * scale, order=min(iteration, 2)
            ),
            out_shape=outs,
            in_specs=[smem] + [vmem] * (len(ins) - 1),
            out_specs=[vmem] * len(outs),
            scratch_shapes=scratch + [pltpu.VMEM((2 * half, coarse_cols), jnp.bfloat16)],
            cost_estimate=pl.CostEstimate(flops=7 * 10**9, bytes_accessed=3 * 10**6, transcendentals=0),
            name="iterate",
        )(*ins)
        images.append(got[1])
        if iteration:
            state = got[2]
            steps.append(got[3])
        hits = lax.all_to_all(got[0], ("mem", "lat"), 0, 0, tiled=True)
    control, image = pl.pallas_call(
        functools.partial(final_kernel, members=members, fine_rows=fine_rows, coarse_rows=coarse_rows, scale=scale),
        out_shape=[f32((half, coarse_cols)), f32((fine_rows, lon_cells))],
        in_specs=[smem] + [vmem] * 11,
        out_specs=[vmem] * 2,
        scratch_shapes=[pltpu.VMEM((bands, slots), jnp.float32)] + scratch,
        cost_estimate=pl.CostEstimate(flops=5 * 10**9, bytes_accessed=6 * 10**6, transcendentals=0),
        name="finish",
    )(slot, state, hits, near, tables[1], t1, *images, *steps, field)
    return control.reshape(members, coarse_rows, coarse_cols), scatter_mem(image)


def solution(mesh):
    in_specs = (P("mem", "lat", None), P("lat", None), P("lat"), P("lat", None), P("lat", None))
    out_specs = (P("mem", "lat", None), P("lat", "mem"))
    return jax.shard_map(on_device, mesh=mesh, in_specs=in_specs, out_specs=out_specs, check_vma=False)
```

```python
import functools

import jax
import jax.numpy as jnp
import numpy as np
from jax import lax
from jax.experimental import pallas as pl
from jax.experimental.pallas import tpu as pltpu
from jax.sharding import PartitionSpec as P

HALO = 8
LSIG = 3
ITERS = 3
REACH = 2
NREL = 2 * REACH + 1
BLK = 256
EDGE = 128
META = 8


def lat_tables(bands, coarse_rows):
    rows = bands * coarse_rows
    offset = np.arange(rows)[:, None] - np.arange(rows)[None, :]
    spread = HALO / 2.0
    r1 = np.where(np.abs(offset) <= HALO, 0.5 * np.exp(-offset * offset / (2.0 * spread * spread)), 0.0)
    r2 = r1 @ r1
    out = np.zeros((bands, 2, NREL, coarse_rows, 128), np.float32)
    for b in range(bands):
        for d in range(NREL):
            s = b + d - REACH
            if 0 <= s < bands:
                own = slice(b * coarse_rows, (b + 1) * coarse_rows)
                other = slice(s * coarse_rows, (s + 1) * coarse_rows)
                out[b, 0, d, :, :coarse_rows] = r2[own, other]
                out[b, 1, d, :, :coarse_rows] = r1[own, other]
    return out


def lon_blocks(coarse_cols):
    d = np.arange(coarse_cols)
    d = np.minimum(d, coarse_cols - d).astype(np.float32)
    c1 = np.exp(-d * d / np.float32(2.0 * LSIG * LSIG)).astype(np.float32).astype(np.float64)
    c2 = np.real(np.fft.ifft(np.fft.fft(c1) ** 2))
    away = np.arange(BLK + 2 * EDGE)[:, None] - EDGE - np.arange(BLK)[None, :]
    inside = np.abs(away) <= EDGE
    blocks = []
    for c in (c1, c2):
        t = jnp.asarray(np.where(inside, c[away % coarse_cols], 0.0).astype(np.float32))
        hi = t.astype(jnp.bfloat16)
        lo = (t - hi.astype(jnp.float32)).astype(jnp.bfloat16)
        blocks.append(jnp.stack([hi, lo]))
    return blocks


def split(a):
    hi = a.astype(jnp.bfloat16)
    return hi, (a - hi.astype(jnp.float32)).astype(jnp.bfloat16)


def dot(a, b, dims=((1,), (0,))):
    return lax.dot_general(a, b, (dims, ((), ())), preferred_element_type=jnp.float32)


def full(ref_shape, dim):
    return lax.broadcasted_iota(jnp.int32, ref_shape, dim).astype(jnp.float32)


def hat_of(x, count):
    middle = 0.5 * (count - 1)
    near = x - middle
    near = jnp.where(jnp.abs(near) > middle + 0.75, float(count), near).astype(jnp.bfloat16)
    j = (full((count, x.shape[1]), 0) - middle).astype(jnp.bfloat16)
    one = jnp.asarray(1, jnp.bfloat16)
    return jnp.maximum(one - jnp.abs(near - j), jnp.asarray(0, jnp.bfloat16))


def pick_kernel(p_ref, meta_ref, out_ref, *, members, fine_rows, chunk):
    lon = p_ref.shape[1]
    slots = meta_ref.shape[1]

    def body(n, _):
        at = pl.ds(pl.multiple_of(n * chunk, chunk), chunk)
        col = 2.0 * meta_ref[0:1, at]
        row = meta_ref[1:2, at]
        one = jnp.where(full((lon, chunk), 0) == col, 1.0, 0.0).astype(jnp.bfloat16)
        got = dot(p_ref[...], one).reshape(members, fine_rows, chunk)
        mask = jnp.where(full((fine_rows, chunk), 0) == row, 1.0, 0.0)
        out_ref[0:members, at] = jnp.sum(got * mask[None], axis=1)
        out_ref[members : members + META, at] = meta_ref[:, at]
        return 0

    lax.fori_loop(0, slots // chunk, body, 0)


def scatter(q_ref, tab, v_of, first, last, lhs_ref, x_ref, members, coarse_rows):
    cols = x_ref.shape[1]
    slots = q_ref.shape[2]
    half = members * coarse_rows
    x_ref[...] = jnp.zeros_like(x_ref)

    def band(d, _):
        at_col = q_ref[d, members : members + 1, :]
        row = jnp.floor(q_ref[d, members + 1 : members + 2, :] * 0.5)
        v = v_of(d)
        weights = jnp.zeros((coarse_rows, slots), jnp.float32)
        taps = tab(d)
        for r in range(coarse_rows):
            weights = jnp.where(row == float(r), taps[:, r : r + 1], weights)
        weights = weights * v
        for k in range(members):
            hi, lo = split(weights * q_ref[d, k : k + 1, :])
            lhs_ref[k * coarse_rows : (k + 1) * coarse_rows, :] = hi
            lhs_ref[half + k * coarse_rows : half + (k + 1) * coarse_rows, :] = lo

        def block(c, _):
            base = (c * BLK).astype(jnp.float32)
            near = jnp.where(jnp.logical_and(c == 0, at_col > cols - 1.0), at_col - float(cols), at_col)
            got = dot(lhs_ref[...], hat_of(near - base, BLK), ((1,), (1,)))
            at = pl.ds(pl.multiple_of(c * BLK, BLK), BLK)
            x_ref[:, at] = x_ref[:, at] + (got[:half] + got[half:])
            return 0

        return lax.fori_loop(0, cols // BLK, block, 0)

    lax.fori_loop(first, last, band, 0)


def lon_filter(x, t_ref):
    half, cols = x.shape
    ext = jnp.concatenate([x[:, cols - EDGE :], x, x[:, :EDGE]], axis=1)
    hi, lo = split(ext)
    parts = []
    for c in range(cols // BLK):
        at = slice(c * BLK, (c + 1) * BLK + 2 * EDGE)
        parts.append(dot(hi[:, at], t_ref[0]) + dot(lo[:, at], t_ref[0]) + dot(hi[:, at], t_ref[1]))
    return jnp.concatenate(parts, axis=1)


def step_of(hits, v, w):
    gg = jnp.full((1, 128), jnp.sum(v * hits), jnp.float32)
    cc = jnp.full((1, 128), jnp.sum(w * hits * hits), jnp.float32)
    return gg / (gg + cc + 1e-6)


def sum_mem(parts, bands):
    return jnp.sum(parts.reshape((parts.shape[0] // bands, bands) + parts.shape[1:]), axis=0)


def pull_of(target, signed):
    bounded = jnp.tanh(target / jnp.abs(signed))
    return jnp.where(signed > 0.0, signed * bounded, 0.0), jnp.where(signed > 0.0, 1.0 - bounded * bounded, 0.0)


def lay_rows(rows_ref, tile_of, bands):
    for d in range(NREL):
        tile = tile_of(jnp.clip(bands[0] + d - REACH, 0, bands[1] - 1))
        for i in range(tile.shape[0]):
            rows_ref[d : d + 1, i * 128 : (i + 1) * 128] = tile[i : i + 1, :]


def iter_kernel(place_ref, q_ref, tab_ref, t2_ref, *refs, members, coarse_rows, scale2, order, bands, groups):
    slots = q_ref.shape[2]
    tiles = slots // 128
    share = tiles // groups
    band = place_ref[1]
    if order == 0:
        part_ref, b_ref, lhs_ref, x_ref, bhl_ref, rows_ref = refs
        for d in range(NREL):
            rows_ref[d : d + 1, :] = pull_of(q_ref[d, members + 2 : members + 3, :], q_ref[d, members + 3 : members + 4, :])[0]
    else:
        old_ref, hits_ref, part_ref, b_ref, state_ref, step_ref, lhs_ref, x_ref, bhl_ref, rows_ref = refs
        hits = sum_mem(hits_ref[:, :tiles, :], bands)
        if order == 1:
            for g in range(groups):
                mine = slice(g * bands, (g + 1) * bands)
                at = slice(g * share, (g + 1) * share)
                state_ref[0, :, at, :] = hits_ref[mine, tiles : tiles + share, :]
                state_ref[1, :, at, :] = hits_ref[mine, tiles + share : tiles + 2 * share, :]
            v, w = pull_of(state_ref[0], state_ref[1])
            observed, lam = 0.0, 0.0
        else:
            state_ref[0:2] = old_ref[0:2]
            v, w, observed, lam = old_ref[2], old_ref[3], old_ref[4], old_ref[5]
        step = step_of(hits, v, w)
        step_ref[...] = step
        step = step[0:1, 0:1][None]
        observed = observed + step * hits
        lam = lam + step * v
        pull, weight = pull_of(state_ref[0] - observed, state_ref[1])
        state_ref[2] = pull - lam
        state_ref[3] = weight
        state_ref[4] = observed
        state_ref[5] = lam
        lay_rows(rows_ref, lambda b: state_ref[2, b], (band, bands))

    def v_of(d):
        return rows_ref[pl.ds(d, 1), :]

    cols = x_ref.shape[1]
    half = members * coarse_rows
    scatter(q_ref, lambda d: tab_ref[band, 0, d], v_of, 0, NREL, lhs_ref, x_ref, members, coarse_rows)
    b = lon_filter(x_ref[...], t2_ref)
    b_ref[...] = b
    hi, lo = split(b)
    bhl_ref[:half] = hi
    bhl_ref[half:] = lo
    chunk = 512
    per = chunk // 128

    def gather(n, _):
        at = pl.ds(pl.multiple_of(n * chunk, chunk), chunk)
        at_col = q_ref[REACH, members : members + 1, at]
        row = jnp.floor(q_ref[REACH, members + 1 : members + 2, at] * 0.5)
        hats = [hat_of(jnp.where(at_col > cols - 1.0, at_col - float(cols), at_col), BLK)]
        hats += [hat_of(at_col - float(c * BLK), BLK) for c in range(1, cols // BLK)]
        hat = jnp.concatenate(hats, axis=0)
        got = dot(bhl_ref[...], hat)
        mask = jnp.where(full((coarse_rows, chunk), 0) == row, scale2, 0.0)
        total = jnp.zeros((coarse_rows, chunk), jnp.float32)
        for k in range(members):
            r = slice(k * coarse_rows, (k + 1) * coarse_rows)
            r2 = slice(half + k * coarse_rows, half + (k + 1) * coarse_rows)
            total = total + q_ref[REACH, k : k + 1, at] * (got[r] + got[r2])
        part = jnp.sum(total * mask, axis=0, keepdims=True)
        for i in range(per):
            part_ref[0, pl.ds(n * per + i, 1), :] = part[:, i * 128 : (i + 1) * 128]
        return 0

    lax.fori_loop(0, slots // chunk, gather, 0)
    if order == 0:
        for r in range(2):
            mine = pl.ds(pl.multiple_of(place_ref[0] * (share * 128), 128), share * 128)
            row = q_ref[REACH, members + 2 + r : members + 3 + r, mine]
            for i in range(share):
                to = tiles + r * share + i
                part_ref[0, to : to + 1, :] = row[:, i * 128 : (i + 1) * 128]
    part_ref[1:] = jnp.broadcast_to(part_ref[0][None], (part_ref.shape[0] - 1,) + part_ref.shape[1:])


def final_kernel(
    place_ref, state_ref, hits_ref, q_ref, tab_ref, t1_ref, b0_ref, b1_ref, b2_ref, s0_ref, s1_ref, p_ref,
    control_ref, image_ref, lam_ref, lhs_ref, x_ref, rows_ref, *, members, fine_rows, coarse_rows, scale,
):
    bands = state_ref.shape[1]
    hits = sum_mem(hits_ref[...], bands)
    v = state_ref[2]
    step = step_of(hits, v, state_ref[3])[0:1, 0:1]
    lam_ref[...] = state_ref[5] + step[None] * v
    lay_rows(rows_ref, lambda b: lam_ref[b], (place_ref[1], bands))

    def v_of(d):
        return rows_ref[pl.ds(d, 1), :]

    scatter(q_ref, lambda d: tab_ref[place_ref[1], 1, d], v_of, REACH - 1, REACH + 2, lhs_ref, x_ref, members, coarse_rows)
    control_ref[...] = scale * lon_filter(x_ref[...], t1_ref)

    b = s0_ref[0:1, 0:1] * b0_ref[...] + s1_ref[0:1, 0:1] * b1_ref[...] + step * b2_ref[...]
    half, cols = b.shape
    wide = 2 * half
    repeat = jnp.where(
        lax.broadcasted_iota(jnp.int32, (wide, half), 0) // 2 == lax.broadcasted_iota(jnp.int32, (wide, half), 1), 1.0, 0.0
    ).astype(jnp.bfloat16)
    hi, lo = split(jnp.concatenate([b, b[:, :EDGE]], axis=1))
    hi = dot(repeat, hi).astype(jnp.bfloat16)
    lo = dot(repeat, lo).astype(jnp.bfloat16)
    hat = jnp.maximum(1.0 - jnp.abs(0.5 * full((2 * EDGE, 2 * EDGE), 1) - full((2 * EDGE, 2 * EDGE), 0)), 0.0)
    hat = hat.astype(jnp.bfloat16)
    for f in range(cols // EDGE):
        at = slice(f * EDGE, f * EDGE + 2 * EDGE)
        fine = slice(2 * f * EDGE, 2 * (f + 1) * EDGE)
        field = dot(hi[:, at], hat) + dot(lo[:, at], hat)
        product = p_ref[:, fine].astype(jnp.float32) * field
        image_ref[:, fine] = (scale * scale) * jnp.sum(product.reshape(members, fine_rows, 2 * EDGE), axis=0)


def swap(a, axis, bit):
    count = lax.axis_size(axis)
    return lax.ppermute(a, axis, [(i, i ^ bit) for i in range(count)])


def scatter_mem(a):
    bit = lax.axis_size("mem") // 2
    me = lax.axis_index("mem")
    while bit:
        width = a.shape[1] // 2
        low, high = a[:, :width], a[:, width:]
        upper = (me & bit) != 0
        a = jnp.where(upper, high, low) + swap(jnp.where(upper, low, high), "mem", bit)
        bit //= 2
    return a


def on_device(perturbation, obs_cells, obs_count, innovation, obs_scale):
    bands = lax.axis_size("lat")
    members, fine_rows, lon_cells = perturbation.shape
    coarse_rows = fine_rows // 2
    coarse_cols = lon_cells // 2
    slots = obs_cells.shape[1]
    half = members * coarse_rows
    scale = float((members * lax.axis_size("mem") - 1) ** (-0.5))
    t1, t2 = lon_blocks(coarse_cols)
    tables = jnp.asarray(lat_tables(bands, coarse_rows))
    groups = lax.axis_size("mem")
    place = jnp.stack([lax.axis_index("mem"), lax.axis_index("lat")]).astype(jnp.int32)

    smem = pl.BlockSpec(memory_space=pltpu.SMEM)
    vmem = pl.BlockSpec(memory_space=pltpu.VMEM)
    f32 = functools.partial(jax.ShapeDtypeStruct, dtype=jnp.float32)

    live = jnp.arange(slots, dtype=jnp.int32)[None] < obs_count[0]
    field = perturbation.reshape(members * fine_rows, lon_cells)
    meta = jnp.concatenate(
        [
            (obs_cells % lon_cells).astype(jnp.float32) * 0.5,
            (obs_cells // lon_cells).astype(jnp.float32),
            innovation,
            jnp.where(live, obs_scale, -obs_scale),
            jnp.zeros((META - 4, slots), jnp.float32),
        ]
    )
    own = pl.pallas_call(
        functools.partial(pick_kernel, members=members, fine_rows=fine_rows, chunk=256),
        out_shape=f32((members + META, slots)),
        in_specs=[vmem, vmem],
        out_specs=vmem,
        cost_estimate=pl.CostEstimate(flops=4 * 10**9, bytes_accessed=2 * 10**6, transcendentals=0),
        name="pick",
    )(field, meta)
    near = []
    for d in range(-REACH, REACH + 1):
        near.append(lax.ppermute(own, "lat", [(s, s - d) for s in range(bands) if 0 <= s - d < bands]) if d else own)
    near = jnp.stack(near)

    rows = pltpu.VMEM((8, slots), jnp.float32)
    scratch = [pltpu.VMEM((2 * half, slots), jnp.bfloat16), pltpu.VMEM((half, coarse_cols), jnp.float32)]
    tiles = slots // 128
    state, hits, images, steps = None, None, [], []
    for iteration in range(ITERS):
        order = min(iteration, 2)
        ins = [place, near, tables, t2] + [[], [obs_cells, hits], [state, hits]][order]
        block = (groups * bands, tiles + (0 if iteration else 2 * (tiles // groups)), 128)
        outs = [f32(block), f32((half, coarse_cols))] + ([f32((6, bands, tiles, 128)), f32((1, 128))] if iteration else [])
        got = pl.pallas_call(
            functools.partial(
                iter_kernel, members=members, coarse_rows=coarse_rows, scale2=scale * scale, order=order, bands=bands, groups=groups
            ),
            out_shape=outs,
            in_specs=[smem] + [vmem] * (len(ins) - 1),
            out_specs=[vmem] * len(outs),
            scratch_shapes=scratch + [pltpu.VMEM((2 * half, coarse_cols), jnp.bfloat16), rows],
            cost_estimate=pl.CostEstimate(flops=7 * 10**9, bytes_accessed=3 * 10**6, transcendentals=0),
            name="iterate",
        )(*ins)
        images.append(got[1])
        if iteration:
            state = got[2]
            steps.append(got[3])
        hits = lax.all_to_all(got[0], ("mem", "lat"), 0, 0, tiled=True)
    control, image = pl.pallas_call(
        functools.partial(final_kernel, members=members, fine_rows=fine_rows, coarse_rows=coarse_rows, scale=scale),
        out_shape=[f32((half, coarse_cols)), f32((fine_rows, lon_cells))],
        in_specs=[smem] + [vmem] * 11,
        out_specs=[vmem] * 2,
        scratch_shapes=[pltpu.VMEM((bands, tiles, 128), jnp.float32)] + scratch + [rows],
        cost_estimate=pl.CostEstimate(flops=5 * 10**9, bytes_accessed=6 * 10**6, transcendentals=0),
        name="finish",
    )(place, state, hits, near, tables, t1, *images, *steps, field)
    return control.reshape(members, coarse_rows, coarse_cols), scatter_mem(image)


def solution(mesh):
    in_specs = (P("mem", "lat", None), P("lat", None), P("lat"), P("lat", None), P("lat", None))
    out_specs = (P("mem", "lat", None), P("lat", "mem"))
    return jax.shard_map(on_device, mesh=mesh, in_specs=in_specs, out_specs=out_specs, check_vma=False)
```

```python
import functools

import jax
import jax.numpy as jnp
import numpy as np
from jax import lax
from jax.experimental import pallas as pl
from jax.experimental.pallas import tpu as pltpu
from jax.sharding import PartitionSpec as P

HALO = 8
LSIG = 3
ITERS = 3
REACH = 2
NREL = 2 * REACH + 1
BLK = 256
EDGE = 128
META = 8
WINDOW = 768


def lat_tables(bands, coarse_rows):
    rows = bands * coarse_rows
    offset = np.arange(rows)[:, None] - np.arange(rows)[None, :]
    spread = HALO / 2.0
    r1 = np.where(np.abs(offset) <= HALO, 0.5 * np.exp(-offset * offset / (2.0 * spread * spread)), 0.0)
    r2 = r1 @ r1
    out = np.zeros((bands, 2, NREL, coarse_rows, 128), np.float32)
    for b in range(bands):
        for d in range(NREL):
            s = b + d - REACH
            if 0 <= s < bands:
                own = slice(b * coarse_rows, (b + 1) * coarse_rows)
                other = slice(s * coarse_rows, (s + 1) * coarse_rows)
                out[b, 0, d, :, :coarse_rows] = r2[own, other]
                out[b, 1, d, :, :coarse_rows] = r1[own, other]
    return out


def lon_blocks(coarse_cols):
    d = np.arange(coarse_cols)
    d = np.minimum(d, coarse_cols - d).astype(np.float32)
    c1 = np.exp(-d * d / np.float32(2.0 * LSIG * LSIG)).astype(np.float32).astype(np.float64)
    c2 = np.real(np.fft.ifft(np.fft.fft(c1) ** 2))
    away = np.arange(BLK + 2 * EDGE)[:, None] - EDGE - np.arange(BLK)[None, :]
    inside = np.abs(away) <= EDGE
    blocks = []
    for c in (c1, c2):
        t = jnp.asarray(np.where(inside, c[away % coarse_cols], 0.0).astype(np.float32))
        hi = t.astype(jnp.bfloat16)
        lo = (t - hi.astype(jnp.float32)).astype(jnp.bfloat16)
        blocks.append(jnp.stack([hi, lo]))
    return blocks


def split(a):
    hi = a.astype(jnp.bfloat16)
    return hi, (a - hi.astype(jnp.float32)).astype(jnp.bfloat16)


def dot(a, b, dims=((1,), (0,))):
    return lax.dot_general(a, b, (dims, ((), ())), preferred_element_type=jnp.float32)


def full(ref_shape, dim):
    return lax.broadcasted_iota(jnp.int32, ref_shape, dim).astype(jnp.float32)


def hat_of(x, count):
    middle = 0.5 * (count - 1)
    near = x - middle
    near = jnp.where(jnp.abs(near) > middle + 0.75, float(count), near).astype(jnp.bfloat16)
    j = (full((count, x.shape[1]), 0) - middle).astype(jnp.bfloat16)
    one = jnp.asarray(1, jnp.bfloat16)
    return jnp.maximum(one - jnp.abs(near - j), jnp.asarray(0, jnp.bfloat16))


def pieces(a):
    out = []
    for _ in range(3):
        out.append(a.astype(jnp.bfloat16))
        a = a - out[-1].astype(jnp.float32)
    return out


def count(mask):
    return jnp.sum(jnp.where(mask, 1.0, 0.0)).astype(jnp.int32)


def prepare_kernel(p_ref, meta_ref, out_ref, key_ref, kcol_ref, srt_ref, *, members, fine_rows):
    lon = p_ref.shape[1]
    slots = meta_ref.shape[1]
    col = 2.0 * meta_ref[0:1, :]
    dead = meta_ref[3:4, :] < 0.0
    key = jnp.where(dead, col + float(lon), col) * float(slots) + full((1, slots), 1)
    key_ref[0:1, :] = key
    top = jnp.floor(key / 65536.0)
    low = key - top * 65536.0
    mid = jnp.floor(low / 256.0)
    parts = jnp.concatenate([top, mid, low - mid * 256.0, jnp.zeros((13, slots), jnp.float32)], axis=0).astype(jnp.bfloat16)
    r = full((16, 128), 0)
    base = jnp.where(r == 0.0, 65536.0, jnp.where(r == 1.0, 256.0, jnp.where(r == 2.0, 1.0, 0.0))).astype(jnp.bfloat16)
    kcol_ref[...] = dot(parts, base, ((0,), (0,)))

    def rank(n, _):
        at = pl.ds(pl.multiple_of(n * 128, 128), 128)
        below = jnp.where(kcol_ref[...] < key_ref[0:1, at], 1.0, 0.0)
        key_ref[1:2, at] = jnp.sum(below, axis=0, keepdims=True)
        return 0

    lax.fori_loop(0, slots // 128, rank, 0)

    srt_ref[...] = jnp.zeros_like(srt_ref)
    high = jnp.floor(col / 256.0)
    rows = [high.astype(jnp.bfloat16), (col - high * 256.0).astype(jnp.bfloat16), meta_ref[1:2, :].astype(jnp.bfloat16)]
    rows += pieces(meta_ref[2:3, :]) + pieces(meta_ref[3:4, :])
    rows.append(jnp.zeros((16 - len(rows), slots), jnp.bfloat16))
    rows = jnp.concatenate([a.astype(jnp.float32) for a in rows], axis=0).astype(jnp.bfloat16)

    def permute(n, _):
        at = pl.ds(pl.multiple_of(n * BLK, BLK), BLK)
        place = key_ref[1:2, :] - (n * BLK).astype(jnp.float32)
        one = jnp.where(full((BLK, slots), 0) == place, 1.0, 0.0).astype(jnp.bfloat16)
        got = dot(rows, one, ((1,), (1,)))
        srt_ref[members : members + 1, at] = 128.0 * got[0:1] + 0.5 * got[1:2]
        srt_ref[members + 1 : members + 2, at] = got[2:3]
        srt_ref[members + 2 : members + 3, at] = got[3:4] + got[4:5] + got[5:6]
        srt_ref[members + 3 : members + 4, at] = got[6:7] + got[7:8] + got[8:9]
        return 0

    lax.fori_loop(0, slots // BLK, permute, 0)

    lane = full((1, 128), 1)
    bounds = jnp.zeros((1, 128), jnp.float32)
    blocks = lon // (2 * BLK)
    for c in range(blocks + 1):
        first = jnp.where(jnp.logical_and(jnp.logical_not(dead), col <= 2.0 * BLK * c - 2.0), 1.0, 0.0)
        last = jnp.where(jnp.logical_and(jnp.logical_not(dead), col < 2.0 * BLK * (c + 1)), 1.0, 0.0)
        bounds = jnp.where(lane == float(c), jnp.sum(first, axis=1, keepdims=True), bounds)
        bounds = jnp.where(lane == float(64 + c), jnp.sum(last, axis=1, keepdims=True), bounds)
    srt_ref[members + 4 : members + 5, 0:128] = bounds

    def pick(c, _):
        edge = (c * BLK).astype(jnp.float32)
        live = jnp.logical_not(dead)
        s = count(jnp.logical_and(live, col < edge))
        e = count(jnp.logical_and(live, col < edge + BLK))
        start = s // 128 * 128
        trips = jnp.where(e > s, (e - start + 511) // 512, 0)

        def window(i, _):
            at = pl.ds(pl.multiple_of(start + i * 512, 128), 512)
            cols = 2.0 * srt_ref[members : members + 1, at] - edge
            one = jnp.where(full((BLK, 512), 0) == cols, 1.0, 0.0).astype(jnp.bfloat16)
            field = p_ref[:, pl.ds(pl.multiple_of(c * BLK, BLK), BLK)]
            got = dot(field, one).reshape(members, fine_rows, 512)
            mask = jnp.where(full((fine_rows, 512), 0) == srt_ref[members + 1 : members + 2, at], 1.0, 0.0)
            srt_ref[0:members, at] = srt_ref[0:members, at] + jnp.sum(got * mask[None], axis=1)
            return 0

        return lax.fori_loop(0, trips, window, 0)

    lax.fori_loop(0, lon // BLK, pick, 0)
    out_ref[...] = srt_ref[:, :slots]


def windows(bound_ref, d, c):
    s, e = bound_ref[d, c], bound_ref[d, 64 + c]
    start = s // 128 * 128
    return start, jnp.where(e > s, (e - start + WINDOW - 1) // WINDOW, 0)


def scatter(bound_ref, q_ref, tab, v_of, first, last, lhs_ref, at_ref, x_ref, members, coarse_rows):
    slots = q_ref.shape[2]
    half = members * coarse_rows
    blocks = x_ref.shape[1] // BLK - 1
    x_ref[...] = jnp.zeros_like(x_ref)
    lhs_ref[:, slots:] = jnp.zeros((2 * half, WINDOW), jnp.bfloat16)
    at_ref[...] = jnp.zeros_like(at_ref)

    def band(d, _):
        row = jnp.floor(q_ref[d, members + 1 : members + 2, :] * 0.5)
        v = v_of(d)
        at_ref[0:1, :slots] = q_ref[d, members : members + 1, :]
        weights = jnp.zeros((coarse_rows, slots), jnp.float32)
        taps = tab(d)
        for r in range(coarse_rows):
            weights = jnp.where(row == float(r), taps[:, r : r + 1], weights)
        weights = weights * v
        for k in range(members):
            hi, lo = split(weights * q_ref[d, k : k + 1, :])
            lhs_ref[k * coarse_rows : (k + 1) * coarse_rows, :slots] = hi
            lhs_ref[half + k * coarse_rows : half + (k + 1) * coarse_rows, :slots] = lo

        def one(c, start):
            at = pl.ds(pl.multiple_of(start, 128), WINDOW)
            hat = hat_of(at_ref[0:1, at] - c * float(BLK), BLK)
            got = dot(lhs_ref[:, at], hat, ((1,), (1,)))
            return got[:half] + got[half:]

        for c in range(blocks):
            to = slice(c * BLK, (c + 1) * BLK)
            x_ref[:, to] = x_ref[:, to] + one(float(c), windows(bound_ref, d, c)[0])

        def rest(c, _):
            start, trips = windows(bound_ref, d, c)
            to = pl.ds(pl.multiple_of(c * BLK, BLK), BLK)

            def more(i, _):
                x_ref[:, to] = x_ref[:, to] + one(c.astype(jnp.float32), start + i * WINDOW)
                return 0

            return lax.fori_loop(jnp.where(c < blocks, 1, 0), trips, more, 0)

        return lax.fori_loop(0, blocks + 1, rest, 0)

    lax.fori_loop(first, last, band, 0)
    x_ref[:, :EDGE] = x_ref[:, :EDGE] + x_ref[:, blocks * BLK : blocks * BLK + EDGE]


def lon_filter(x, t_ref):
    half, cols = x.shape
    ext = jnp.concatenate([x[:, cols - EDGE :], x, x[:, :EDGE]], axis=1)
    hi, lo = split(ext)
    parts = []
    for c in range(cols // BLK):
        at = slice(c * BLK, (c + 1) * BLK + 2 * EDGE)
        parts.append(dot(hi[:, at], t_ref[0]) + dot(lo[:, at], t_ref[0]) + dot(hi[:, at], t_ref[1]))
    return jnp.concatenate(parts, axis=1)


def step_of(hits, v, w):
    gg = jnp.full((1, 128), jnp.sum(v * hits), jnp.float32)
    cc = jnp.full((1, 128), jnp.sum(w * hits * hits), jnp.float32)
    return gg / (gg + cc + 1e-6)


def sum_mem(parts, bands):
    return jnp.sum(parts.reshape((parts.shape[0] // bands, bands) + parts.shape[1:]), axis=0)


def pull_of(target, signed):
    bounded = jnp.tanh(target / jnp.abs(signed))
    return jnp.where(signed > 0.0, signed * bounded, 0.0), jnp.where(signed > 0.0, 1.0 - bounded * bounded, 0.0)


def lay_rows(rows_ref, tile_of, bands):
    for d in range(NREL):
        tile = tile_of(jnp.clip(bands[0] + d - REACH, 0, bands[1] - 1))
        for i in range(tile.shape[0]):
            rows_ref[d : d + 1, i * 128 : (i + 1) * 128] = tile[i : i + 1, :]


def iter_kernel(place_ref, bound_ref, q_ref, tab_ref, t2_ref, *refs, members, coarse_rows, scale2, order, bands, groups):
    slots = q_ref.shape[2]
    tiles = slots // 128
    share = tiles // groups
    band = place_ref[1]
    if order == 0:
        part_ref, b_ref, lhs_ref, at_ref, x_ref, rows_ref, bhl_ref, own_ref = refs
        for d in range(NREL):
            rows_ref[d : d + 1, :slots] = pull_of(q_ref[d, members + 2 : members + 3, :], q_ref[d, members + 3 : members + 4, :])[0]
    else:
        old_ref, hits_ref, part_ref, b_ref, state_ref, step_ref, lhs_ref, at_ref, x_ref, rows_ref, bhl_ref, own_ref = refs
        hits = sum_mem(hits_ref[:, :tiles, :], bands)
        if order == 1:
            for g in range(groups):
                mine = slice(g * bands, (g + 1) * bands)
                at = slice(g * share, (g + 1) * share)
                state_ref[0, :, at, :] = hits_ref[mine, tiles : tiles + share, :]
                state_ref[1, :, at, :] = hits_ref[mine, tiles + share : tiles + 2 * share, :]
            v, w = pull_of(state_ref[0], state_ref[1])
            observed, lam = 0.0, 0.0
        else:
            state_ref[0:2] = old_ref[0:2]
            v, w, observed, lam = old_ref[2], old_ref[3], old_ref[4], old_ref[5]
        step = step_of(hits, v, w)
        step_ref[...] = step
        step = step[0:1, 0:1][None]
        observed = observed + step * hits
        lam = lam + step * v
        pull, weight = pull_of(state_ref[0] - observed, state_ref[1])
        state_ref[2] = pull - lam
        state_ref[3] = weight
        state_ref[4] = observed
        state_ref[5] = lam
        lay_rows(rows_ref, lambda b: state_ref[2, b], (band, bands))

    def v_of(d):
        return rows_ref[pl.ds(d, 1), :slots]

    half = members * coarse_rows
    blocks = x_ref.shape[1] // BLK - 1
    cols = blocks * BLK
    scatter(bound_ref, q_ref, lambda d: tab_ref[band, 0, d], v_of, 0, NREL, lhs_ref, at_ref, x_ref, members, coarse_rows)
    b = lon_filter(x_ref[:, :cols], t2_ref)
    b_ref[...] = b
    hi, lo = split(b)
    bhl_ref[:half, :cols] = hi
    bhl_ref[half:, :cols] = lo
    bhl_ref[:, cols:] = bhl_ref[:, :BLK]
    own_ref[:, :slots] = q_ref[REACH]
    own_ref[:, slots:] = jnp.zeros((members + META, WINDOW), jnp.float32)
    rows_ref[...] = jnp.zeros_like(rows_ref)

    def gather(c, start):
        at = pl.ds(pl.multiple_of(start, 128), WINDOW)
        row = jnp.floor(own_ref[members + 1 : members + 2, at] * 0.5)
        hat = hat_of(own_ref[members : members + 1, at] - jnp.float32(c) * float(BLK), BLK)
        got = dot(bhl_ref[:, pl.ds(pl.multiple_of(c * BLK, BLK), BLK)], hat)
        mask = jnp.where(full((coarse_rows, WINDOW), 0) == row, scale2, 0.0)
        total = jnp.zeros((coarse_rows, WINDOW), jnp.float32)
        for k in range(members):
            r = slice(k * coarse_rows, (k + 1) * coarse_rows)
            r2 = slice(half + k * coarse_rows, half + (k + 1) * coarse_rows)
            total = total + own_ref[k : k + 1, at] * (got[r] + got[r2])
        rows_ref[0:1, at] = rows_ref[0:1, at] + jnp.sum(total * mask, axis=0, keepdims=True)

    for c in range(blocks):
        gather(c, windows(bound_ref, REACH, c)[0])

    def rest(c, _):
        start, trips = windows(bound_ref, REACH, c)

        def more(i, _):
            gather(c, start + i * WINDOW)
            return 0

        return lax.fori_loop(jnp.where(c < blocks, 1, 0), trips, more, 0)

    lax.fori_loop(0, blocks + 1, rest, 0)
    for i in range(tiles):
        part_ref[0, i : i + 1, :] = rows_ref[0:1, i * 128 : (i + 1) * 128]
    if order == 0:
        for r in range(2):
            mine = pl.ds(pl.multiple_of(place_ref[0] * (share * 128), 128), share * 128)
            row = q_ref[REACH, members + 2 + r : members + 3 + r, mine]
            for i in range(share):
                to = tiles + r * share + i
                part_ref[0, to : to + 1, :] = row[:, i * 128 : (i + 1) * 128]
    part_ref[1:] = jnp.broadcast_to(part_ref[0][None], (part_ref.shape[0] - 1,) + part_ref.shape[1:])


def final_kernel(
    place_ref, bound_ref, state_ref, hits_ref, q_ref, tab_ref, t1_ref, b0_ref, b1_ref, b2_ref, s0_ref, s1_ref, p_ref,
    control_ref, image_ref, lam_ref, lhs_ref, at_ref, x_ref, rows_ref, *, members, fine_rows, coarse_rows, scale,
):
    bands = state_ref.shape[1]
    slots = q_ref.shape[2]
    hits = sum_mem(hits_ref[...], bands)
    v = state_ref[2]
    step = step_of(hits, v, state_ref[3])[0:1, 0:1]
    lam_ref[...] = state_ref[5] + step[None] * v
    lay_rows(rows_ref, lambda b: lam_ref[b], (place_ref[1], bands))

    def v_of(d):
        return rows_ref[pl.ds(d, 1), :slots]

    tab = lambda d: tab_ref[place_ref[1], 1, d]
    scatter(bound_ref, q_ref, tab, v_of, REACH - 1, REACH + 2, lhs_ref, at_ref, x_ref, members, coarse_rows)
    control_ref[...] = scale * lon_filter(x_ref[:, : b0_ref.shape[1]], t1_ref)

    b = s0_ref[0:1, 0:1] * b0_ref[...] + s1_ref[0:1, 0:1] * b1_ref[...] + step * b2_ref[...]
    half, cols = b.shape
    wide = 2 * half
    repeat = jnp.where(
        lax.broadcasted_iota(jnp.int32, (wide, half), 0) // 2 == lax.broadcasted_iota(jnp.int32, (wide, half), 1), 1.0, 0.0
    ).astype(jnp.bfloat16)
    hi, lo = split(jnp.concatenate([b, b[:, :EDGE]], axis=1))
    hi = dot(repeat, hi).astype(jnp.bfloat16)
    lo = dot(repeat, lo).astype(jnp.bfloat16)
    hat = jnp.maximum(1.0 - jnp.abs(0.5 * full((2 * EDGE, 2 * EDGE), 1) - full((2 * EDGE, 2 * EDGE), 0)), 0.0)
    hat = hat.astype(jnp.bfloat16)
    for f in range(cols // EDGE):
        at = slice(f * EDGE, f * EDGE + 2 * EDGE)
        fine = slice(2 * f * EDGE, 2 * (f + 1) * EDGE)
        field = dot(hi[:, at], hat) + dot(lo[:, at], hat)
        product = p_ref[:, fine].astype(jnp.float32) * field
        image_ref[:, fine] = (scale * scale) * jnp.sum(product.reshape(members, fine_rows, 2 * EDGE), axis=0)


def swap(a, axis, bit):
    count = lax.axis_size(axis)
    return lax.ppermute(a, axis, [(i, i ^ bit) for i in range(count)])


def scatter_mem(a):
    bit = lax.axis_size("mem") // 2
    me = lax.axis_index("mem")
    while bit:
        width = a.shape[1] // 2
        low, high = a[:, :width], a[:, width:]
        upper = (me & bit) != 0
        a = jnp.where(upper, high, low) + swap(jnp.where(upper, low, high), "mem", bit)
        bit //= 2
    return a


def on_device(perturbation, obs_cells, obs_count, innovation, obs_scale):
    bands = lax.axis_size("lat")
    members, fine_rows, lon_cells = perturbation.shape
    coarse_rows = fine_rows // 2
    coarse_cols = lon_cells // 2
    slots = obs_cells.shape[1]
    half = members * coarse_rows
    scale = float((members * lax.axis_size("mem") - 1) ** (-0.5))
    t1, t2 = lon_blocks(coarse_cols)
    tables = jnp.asarray(lat_tables(bands, coarse_rows))
    groups = lax.axis_size("mem")
    place = jnp.stack([lax.axis_index("mem"), lax.axis_index("lat")]).astype(jnp.int32)

    smem = pl.BlockSpec(memory_space=pltpu.SMEM)
    vmem = pl.BlockSpec(memory_space=pltpu.VMEM)
    f32 = functools.partial(jax.ShapeDtypeStruct, dtype=jnp.float32)

    live = jnp.arange(slots, dtype=jnp.int32)[None] < obs_count[0]
    field = perturbation.reshape(members * fine_rows, lon_cells)
    meta = jnp.concatenate(
        [
            (obs_cells % lon_cells).astype(jnp.float32) * 0.5,
            (obs_cells // lon_cells).astype(jnp.float32),
            innovation,
            jnp.where(live, obs_scale, -obs_scale),
            jnp.zeros((META - 4, slots), jnp.float32),
        ]
    )
    own = pl.pallas_call(
        functools.partial(prepare_kernel, members=members, fine_rows=fine_rows),
        out_shape=f32((members + META, slots)),
        in_specs=[vmem, vmem],
        out_specs=vmem,
        scratch_shapes=[
            pltpu.VMEM((8, slots), jnp.float32),
            pltpu.VMEM((slots, 128), jnp.float32),
            pltpu.VMEM((members + META, slots + 512), jnp.float32),
        ],
        cost_estimate=pl.CostEstimate(flops=4 * 10**9, bytes_accessed=2 * 10**6, transcendentals=0),
        name="prepare",
    )(field, meta)
    near = []
    for d in range(-REACH, REACH + 1):
        near.append(lax.ppermute(own, "lat", [(s, s - d) for s in range(bands) if 0 <= s - d < bands]) if d else own)
    near = jnp.stack(near)
    bound = near[:, members + 4, :128].astype(jnp.int32)

    padded = slots + WINDOW
    scratch = [
        pltpu.VMEM((2 * half, padded), jnp.bfloat16),
        pltpu.VMEM((8, padded), jnp.float32),
        pltpu.VMEM((half, coarse_cols + BLK), jnp.float32),
        pltpu.VMEM((8, padded), jnp.float32),
    ]
    tiles = slots // 128
    state, hits, images, steps = None, None, [], []
    for iteration in range(ITERS):
        order = min(iteration, 2)
        ins = [place, bound, near, tables, t2] + [[], [obs_cells, hits], [state, hits]][order]
        block = (groups * bands, tiles + (0 if iteration else 2 * (tiles // groups)), 128)
        outs = [f32(block), f32((half, coarse_cols))] + ([f32((6, bands, tiles, 128)), f32((1, 128))] if iteration else [])
        got = pl.pallas_call(
            functools.partial(
                iter_kernel, members=members, coarse_rows=coarse_rows, scale2=scale * scale, order=order, bands=bands, groups=groups
            ),
            out_shape=outs,
            in_specs=[smem] * 2 + [vmem] * (len(ins) - 2),
            out_specs=[vmem] * len(outs),
            scratch_shapes=scratch
            + [pltpu.VMEM((2 * half, coarse_cols + BLK), jnp.bfloat16), pltpu.VMEM((members + META, padded), jnp.float32)],
            cost_estimate=pl.CostEstimate(flops=7 * 10**9, bytes_accessed=3 * 10**6, transcendentals=0),
            name="iterate",
        )(*ins)
        images.append(got[1])
        if iteration:
            state = got[2]
            steps.append(got[3])
        hits = lax.all_to_all(got[0], ("mem", "lat"), 0, 0, tiled=True)
    control, image = pl.pallas_call(
        functools.partial(final_kernel, members=members, fine_rows=fine_rows, coarse_rows=coarse_rows, scale=scale),
        out_shape=[f32((half, coarse_cols)), f32((fine_rows, lon_cells))],
        in_specs=[smem] * 2 + [vmem] * 11,
        out_specs=[vmem] * 2,
        scratch_shapes=[pltpu.VMEM((bands, tiles, 128), jnp.float32)] + scratch,
        cost_estimate=pl.CostEstimate(flops=5 * 10**9, bytes_accessed=6 * 10**6, transcendentals=0),
        name="finish",
    )(place, bound, state, hits, near, tables, t1, *images, *steps, field)
    return control.reshape(members, coarse_rows, coarse_cols), scatter_mem(image)


def solution(mesh):
    in_specs = (P("mem", "lat", None), P("lat", None), P("lat"), P("lat", None), P("lat", None))
    out_specs = (P("mem", "lat", None), P("lat", "mem"))
    return jax.shard_map(on_device, mesh=mesh, in_specs=in_specs, out_specs=out_specs, check_vma=False)
```

```python
import functools

import jax
import jax.numpy as jnp
import numpy as np
from jax import lax
from jax.experimental import pallas as pl
from jax.experimental.pallas import tpu as pltpu
from jax.sharding import PartitionSpec as P

HALO = 8
LSIG = 3
ITERS = 3
REACH = 2
NREL = 2 * REACH + 1
BLK = 256
EDGE = 128
META = 8
WINDOW = 768


def lat_tables(bands, coarse_rows):
    rows = bands * coarse_rows
    offset = np.arange(rows)[:, None] - np.arange(rows)[None, :]
    spread = HALO / 2.0
    r1 = np.where(np.abs(offset) <= HALO, 0.5 * np.exp(-offset * offset / (2.0 * spread * spread)), 0.0)
    r2 = r1 @ r1
    out = np.zeros((bands, 2, NREL, coarse_rows, 128), np.float32)
    for b in range(bands):
        for d in range(NREL):
            s = b + d - REACH
            if 0 <= s < bands:
                own = slice(b * coarse_rows, (b + 1) * coarse_rows)
                other = slice(s * coarse_rows, (s + 1) * coarse_rows)
                out[b, 0, d, :, :coarse_rows] = r2[own, other]
                out[b, 1, d, :, :coarse_rows] = r1[own, other]
    return out


def lon_blocks(coarse_cols):
    d = np.arange(coarse_cols)
    d = np.minimum(d, coarse_cols - d).astype(np.float32)
    c1 = np.exp(-d * d / np.float32(2.0 * LSIG * LSIG)).astype(np.float32).astype(np.float64)
    c2 = np.real(np.fft.ifft(np.fft.fft(c1) ** 2))
    away = np.arange(BLK + 2 * EDGE)[:, None] - EDGE - np.arange(BLK)[None, :]
    inside = np.abs(away) <= EDGE
    blocks = []
    for c in (c1, c2):
        t = jnp.asarray(np.where(inside, c[away % coarse_cols], 0.0).astype(np.float32))
        hi = t.astype(jnp.bfloat16)
        lo = (t - hi.astype(jnp.float32)).astype(jnp.bfloat16)
        blocks.append(jnp.stack([hi, lo]))
    return blocks


def split(a):
    hi = a.astype(jnp.bfloat16)
    return hi, (a - hi.astype(jnp.float32)).astype(jnp.bfloat16)


def dot(a, b, dims=((1,), (0,))):
    return lax.dot_general(a, b, (dims, ((), ())), preferred_element_type=jnp.float32)


def full(ref_shape, dim):
    return lax.broadcasted_iota(jnp.int32, ref_shape, dim).astype(jnp.float32)


def hat_of(x, count):
    middle = 0.5 * (count - 1)
    near = x - middle
    near = jnp.where(jnp.abs(near) > middle + 0.75, float(count), near).astype(jnp.bfloat16)
    j = (full((count, x.shape[1]), 0) - middle).astype(jnp.bfloat16)
    one = jnp.asarray(1, jnp.bfloat16)
    return jnp.maximum(one - jnp.abs(near - j), jnp.asarray(0, jnp.bfloat16))


def pieces(a):
    out = []
    for _ in range(3):
        out.append(a.astype(jnp.bfloat16))
        a = a - out[-1].astype(jnp.float32)
    return out


def count(mask):
    return jnp.sum(jnp.where(mask, 1.0, 0.0)).astype(jnp.int32)


def prepare_kernel(count_ref, p_ref, cell_ref, innovation_ref, scale_ref, out_ref, key_ref, kcol_ref, srt_ref, *, members, fine_rows):
    lon = p_ref.shape[1]
    slots = cell_ref.shape[1]
    cell = cell_ref[...].astype(jnp.float32)
    row = jnp.floor((cell + 0.5) / float(lon))
    col = cell - row * float(lon)
    dead = full((1, slots), 1) >= count_ref[0].astype(jnp.float32)
    signed = jnp.where(dead, -scale_ref[...], scale_ref[...])
    key = jnp.where(dead, col + float(lon), col) * float(slots) + full((1, slots), 1)
    key_ref[0:1, :] = key
    top = jnp.floor(key / 65536.0)
    low = key - top * 65536.0
    mid = jnp.floor(low / 256.0)
    parts = jnp.concatenate([top, mid, low - mid * 256.0, jnp.zeros((13, slots), jnp.float32)], axis=0).astype(jnp.bfloat16)
    r = full((16, 128), 0)
    base = jnp.where(r == 0.0, 65536.0, jnp.where(r == 1.0, 256.0, jnp.where(r == 2.0, 1.0, 0.0))).astype(jnp.bfloat16)
    kcol_ref[...] = dot(parts, base, ((0,), (0,)))

    def rank(n, _):
        at = pl.ds(pl.multiple_of(n * 128, 128), 128)
        below = jnp.where(kcol_ref[...] < key_ref[0:1, at], 1.0, 0.0)
        below = jnp.sum(below.reshape(slots // 64, 64, 128), axis=0)
        key_ref[1:2, at] = jnp.sum(below, axis=0, keepdims=True)
        return 0

    lax.fori_loop(0, slots // 128, rank, 0)

    srt_ref[...] = jnp.zeros_like(srt_ref)
    high = jnp.floor(col / 256.0)
    rows = [high.astype(jnp.bfloat16), (col - high * 256.0).astype(jnp.bfloat16), row.astype(jnp.bfloat16)]
    rows += pieces(innovation_ref[...]) + pieces(signed)
    rows.append(jnp.zeros((16 - len(rows), slots), jnp.bfloat16))
    rows = jnp.concatenate([a.astype(jnp.float32) for a in rows], axis=0).astype(jnp.bfloat16)

    def permute(n, _):
        at = pl.ds(pl.multiple_of(n * BLK, BLK), BLK)
        place = key_ref[1:2, :] - (n * BLK).astype(jnp.float32)
        one = jnp.where(full((BLK, slots), 0) == place, 1.0, 0.0).astype(jnp.bfloat16)
        got = dot(rows, one, ((1,), (1,)))
        srt_ref[members : members + 1, at] = 128.0 * got[0:1] + 0.5 * got[1:2]
        srt_ref[members + 1 : members + 2, at] = got[2:3]
        srt_ref[members + 2 : members + 3, at] = got[3:4] + got[4:5] + got[5:6]
        srt_ref[members + 3 : members + 4, at] = got[6:7] + got[7:8] + got[8:9]
        return 0

    lax.fori_loop(0, slots // BLK, permute, 0)

    lane = full((1, 128), 1)
    bounds = jnp.zeros((1, 128), jnp.float32)
    blocks = lon // (2 * BLK)
    for c in range(blocks + 1):
        first = jnp.where(jnp.logical_and(jnp.logical_not(dead), col <= 2.0 * BLK * c - 2.0), 1.0, 0.0)
        last = jnp.where(jnp.logical_and(jnp.logical_not(dead), col < 2.0 * BLK * (c + 1)), 1.0, 0.0)
        bounds = jnp.where(lane == float(c), jnp.sum(first, axis=1, keepdims=True), bounds)
        bounds = jnp.where(lane == float(64 + c), jnp.sum(last, axis=1, keepdims=True), bounds)
    srt_ref[members + 4 : members + 5, 0:128] = bounds

    live = jnp.logical_not(dead)
    edges = [count(jnp.logical_and(live, col < float(c * BLK))) for c in range(lon // BLK + 1)]

    def window(c, start):
        at = pl.ds(pl.multiple_of(start, 128), 512)
        cols = 2.0 * srt_ref[members : members + 1, at] - float(c * BLK)
        one = jnp.where(full((BLK, 512), 0) == cols, 1.0, 0.0).astype(jnp.bfloat16)
        got = dot(p_ref[:, c * BLK : (c + 1) * BLK], one).reshape(members, fine_rows, 512)
        mask = jnp.where(full((fine_rows, 512), 0) == srt_ref[members + 1 : members + 2, at], 1.0, 0.0)
        srt_ref[0:members, at] = srt_ref[0:members, at] + jnp.sum(got * mask[None], axis=1)

    starts = [s // 128 * 128 for s in edges[:-1]]
    for c, start in enumerate(starts):
        window(c, start)
    for c, start in enumerate(starts):

        def more(i, _, c=c, start=start):
            window(c, start + i * 512)
            return 0

        lax.fori_loop(1, (edges[c + 1] - start + 511) // 512, more, 0)
    out_ref[...] = srt_ref[:, :slots]


def windows(bound_ref, d, c):
    s, e = bound_ref[d, c], bound_ref[d, 64 + c]
    start = s // 128 * 128
    return start, jnp.where(e > s, (e - start + WINDOW - 1) // WINDOW, 0)


def scatter(bound_ref, q_ref, tab, v_of, first, last, lhs_ref, at_ref, x_ref, members, coarse_rows):
    slots = q_ref.shape[2]
    half = members * coarse_rows
    blocks = x_ref.shape[1] // BLK - 1
    x_ref[...] = jnp.zeros_like(x_ref)
    lhs_ref[:, slots:] = jnp.zeros((2 * half, WINDOW), jnp.bfloat16)
    at_ref[...] = jnp.zeros_like(at_ref)

    def band(d, _):
        row = jnp.floor(q_ref[d, members + 1 : members + 2, :] * 0.5)
        v = v_of(d)
        at_ref[0:1, :slots] = q_ref[d, members : members + 1, :]
        weights = jnp.zeros((coarse_rows, slots), jnp.float32)
        taps = tab(d)
        for r in range(coarse_rows):
            weights = jnp.where(row == float(r), taps[:, r : r + 1], weights)
        weights = weights * v
        for k in range(members):
            hi, lo = split(weights * q_ref[d, k : k + 1, :])
            lhs_ref[k * coarse_rows : (k + 1) * coarse_rows, :slots] = hi
            lhs_ref[half + k * coarse_rows : half + (k + 1) * coarse_rows, :slots] = lo

        def one(c, start):
            at = pl.ds(pl.multiple_of(start, 128), WINDOW)
            hat = hat_of(at_ref[0:1, at] - c * float(BLK), BLK)
            got = dot(lhs_ref[:, at], hat, ((1,), (1,)))
            return got[:half] + got[half:]

        for c in range(blocks):
            to = slice(c * BLK, (c + 1) * BLK)
            x_ref[:, to] = x_ref[:, to] + one(float(c), windows(bound_ref, d, c)[0])

        def rest(c, _):
            start, trips = windows(bound_ref, d, c)
            to = pl.ds(pl.multiple_of(c * BLK, BLK), BLK)

            def more(i, _):
                x_ref[:, to] = x_ref[:, to] + one(c.astype(jnp.float32), start + i * WINDOW)
                return 0

            return lax.fori_loop(jnp.where(c < blocks, 1, 0), trips, more, 0)

        return lax.fori_loop(0, blocks + 1, rest, 0)

    lax.fori_loop(first, last, band, 0)
    x_ref[:, :EDGE] = x_ref[:, :EDGE] + x_ref[:, blocks * BLK : blocks * BLK + EDGE]


def lon_filter(x, t_ref):
    _, cols = x.shape
    ext = jnp.concatenate([x[:, cols - EDGE :], x, x[:, :EDGE]], axis=1)
    hi, lo = split(ext)
    parts = []
    for c in range(cols // BLK):
        at = slice(c * BLK, (c + 1) * BLK + 2 * EDGE)
        parts.append(dot(hi[:, at], t_ref[0]) + dot(lo[:, at], t_ref[0]) + dot(hi[:, at], t_ref[1]))
    return jnp.concatenate(parts, axis=1)


def step_of(hits, v, w):
    gg = jnp.full((1, 128), jnp.sum(v * hits), jnp.float32)
    cc = jnp.full((1, 128), jnp.sum(w * hits * hits), jnp.float32)
    return gg / (gg + cc + 1e-6)


def sum_mem(parts, bands):
    return jnp.sum(parts.reshape((parts.shape[0] // bands, bands) + parts.shape[1:]), axis=0)


def pull_of(target, signed):
    bounded = jnp.tanh(target / jnp.abs(signed))
    return jnp.where(signed > 0.0, signed * bounded, 0.0), jnp.where(signed > 0.0, 1.0 - bounded * bounded, 0.0)


def lay_rows(rows_ref, tile_of, bands):
    for d in range(NREL):
        tile = tile_of(jnp.clip(bands[0] + d - REACH, 0, bands[1] - 1))
        for i in range(tile.shape[0]):
            rows_ref[d : d + 1, i * 128 : (i + 1) * 128] = tile[i : i + 1, :]


def iter_kernel(place_ref, bound_ref, q_ref, tab_ref, t2_ref, *refs, members, coarse_rows, scale2, order, bands, groups):
    slots = q_ref.shape[2]
    tiles = slots // 128
    share = tiles // groups
    band = place_ref[1]
    if order == 0:
        part_ref, b_ref, vrow_ref, lhs_ref, at_ref, x_ref, rows_ref, bhl_ref, own_ref = refs
        for d in range(NREL):
            vrow_ref[d : d + 1, :] = pull_of(q_ref[d, members + 2 : members + 3, :], q_ref[d, members + 3 : members + 4, :])[0]
    else:
        old_ref, hits_ref, part_ref, b_ref, vrow_ref, state_ref, step_ref, lhs_ref, at_ref, x_ref, rows_ref, bhl_ref, own_ref = refs
        hits = sum_mem(hits_ref[:, :tiles, :], bands)
        if order == 1:
            for g in range(groups):
                mine = slice(g * bands, (g + 1) * bands)
                at = slice(g * share, (g + 1) * share)
                state_ref[0, :, at, :] = hits_ref[mine, tiles : tiles + share, :]
                state_ref[1, :, at, :] = hits_ref[mine, tiles + share : tiles + 2 * share, :]
            v, w = pull_of(state_ref[0], state_ref[1])
            observed, lam = 0.0, 0.0
        else:
            state_ref[0:2] = old_ref[0:2]
            v, w, observed, lam = old_ref[2], old_ref[3], old_ref[4], old_ref[5]
        step = step_of(hits, v, w)
        step_ref[...] = step
        step = step[0:1, 0:1][None]
        observed = observed + step * hits
        lam = lam + step * v
        pull, weight = pull_of(state_ref[0] - observed, state_ref[1])
        state_ref[2] = pull - lam
        state_ref[3] = weight
        state_ref[4] = observed
        state_ref[5] = lam
        lay_rows(vrow_ref, lambda b: state_ref[2, b], (band, bands))

    def v_of(d):
        return vrow_ref[pl.ds(d, 1), :]

    half = members * coarse_rows
    blocks = x_ref.shape[1] // BLK - 1
    cols = blocks * BLK
    scatter(bound_ref, q_ref, lambda d: tab_ref[band, 0, d], v_of, 0, NREL, lhs_ref, at_ref, x_ref, members, coarse_rows)
    b = lon_filter(x_ref[:, :cols], t2_ref)
    b_ref[...] = b
    hi, lo = split(b)
    bhl_ref[:half, :cols] = hi
    bhl_ref[half:, :cols] = lo
    bhl_ref[:, cols:] = bhl_ref[:, :BLK]
    own_ref[:, :slots] = q_ref[REACH]
    own_ref[:, slots:] = jnp.zeros((members + META, WINDOW), jnp.float32)
    rows_ref[...] = jnp.zeros_like(rows_ref)

    def gather(c, start):
        at = pl.ds(pl.multiple_of(start, 128), WINDOW)
        row = jnp.floor(own_ref[members + 1 : members + 2, at] * 0.5)
        hat = hat_of(own_ref[members : members + 1, at] - jnp.float32(c) * float(BLK), BLK)
        got = dot(bhl_ref[:, pl.ds(pl.multiple_of(c * BLK, BLK), BLK)], hat)
        mask = jnp.where(full((coarse_rows, WINDOW), 0) == row, scale2, 0.0)
        total = jnp.zeros((coarse_rows, WINDOW), jnp.float32)
        for k in range(members):
            r = slice(k * coarse_rows, (k + 1) * coarse_rows)
            r2 = slice(half + k * coarse_rows, half + (k + 1) * coarse_rows)
            total = total + own_ref[k : k + 1, at] * (got[r] + got[r2])
        rows_ref[0:1, at] = rows_ref[0:1, at] + jnp.sum(total * mask, axis=0, keepdims=True)

    for c in range(blocks):
        gather(c, windows(bound_ref, REACH, c)[0])

    def rest(c, _):
        start, trips = windows(bound_ref, REACH, c)

        def more(i, _):
            gather(c, start + i * WINDOW)
            return 0

        return lax.fori_loop(jnp.where(c < blocks, 1, 0), trips, more, 0)

    lax.fori_loop(0, blocks + 1, rest, 0)
    for i in range(tiles):
        part_ref[0, i : i + 1, :] = rows_ref[0:1, i * 128 : (i + 1) * 128]
    if order == 0:
        for r in range(2):
            mine = pl.ds(pl.multiple_of(place_ref[0] * (share * 128), 128), share * 128)
            row = q_ref[REACH, members + 2 + r : members + 3 + r, mine]
            for i in range(share):
                to = tiles + r * share + i
                part_ref[0, to : to + 1, :] = row[:, i * 128 : (i + 1) * 128]
    part_ref[1:] = jnp.broadcast_to(part_ref[0][None], (part_ref.shape[0] - 1,) + part_ref.shape[1:])


def side_kernel(
    place_ref, bound_ref, vrow_ref, q_ref, tab_ref, t1_ref, b_ref, p_ref, control_ref, image_ref, lhs_ref, at_ref, x_ref,
    *, members, fine_rows, coarse_rows, scale,
):
    def v_of(d):
        return vrow_ref[pl.ds(d, 1), :]

    tab = lambda d: tab_ref[place_ref[1], 1, d]
    scatter(bound_ref, q_ref, tab, v_of, REACH - 1, REACH + 2, lhs_ref, at_ref, x_ref, members, coarse_rows)
    control_ref[...] = scale * lon_filter(x_ref[:, : b_ref.shape[1]], t1_ref)

    b = b_ref[...]
    half, cols = b.shape
    wide = 2 * half
    repeat = jnp.where(
        lax.broadcasted_iota(jnp.int32, (wide, half), 0) // 2 == lax.broadcasted_iota(jnp.int32, (wide, half), 1), 1.0, 0.0
    ).astype(jnp.bfloat16)
    hi, lo = split(jnp.concatenate([b, b[:, :EDGE]], axis=1))
    hi = dot(repeat, hi).astype(jnp.bfloat16)
    lo = dot(repeat, lo).astype(jnp.bfloat16)
    hat = jnp.maximum(1.0 - jnp.abs(0.5 * full((2 * EDGE, 2 * EDGE), 1) - full((2 * EDGE, 2 * EDGE), 0)), 0.0)
    hat = hat.astype(jnp.bfloat16)
    for f in range(cols // EDGE):
        at = slice(f * EDGE, f * EDGE + 2 * EDGE)
        fine = slice(2 * f * EDGE, 2 * (f + 1) * EDGE)
        field = dot(hi[:, at], hat) + dot(lo[:, at], hat)
        product = p_ref[:, fine].astype(jnp.float32) * field
        part = (scale * scale) * jnp.sum(product.reshape(members, fine_rows, 2 * EDGE), axis=0)
        width = image_ref.shape[2]
        for start in range(0, 2 * EDGE, min(width, 2 * EDGE)):
            stop = start + min(width, 2 * EDGE)
            group, to = divmod(2 * f * EDGE + start, width)
            image_ref[group, :, to : to + stop - start] = part[:, start:stop]


def combine_kernel(state_ref, hits_ref, *refs):
    steps, controls, images = refs[: ITERS - 1], refs[ITERS - 1 : 2 * ITERS - 1], refs[2 * ITERS - 1 : 3 * ITERS - 1]
    control_ref, image_ref = refs[3 * ITERS - 1 :]
    last = step_of(sum_mem(hits_ref[...], state_ref.shape[1]), state_ref[2], state_ref[3])[0:1, 0:1]
    steps = [s[0:1, 0:1] for s in steps] + [last]
    control_ref[...] = sum(s * c[...] for s, c in zip(steps, controls))
    image_ref[...] = sum(s * i[...] for s, i in zip(steps, images))


def scatter_mem(a):
    count = lax.axis_size("mem")
    me = lax.axis_index("mem")
    bit = count // 2
    while bit:
        low, high = a[: a.shape[0] // 2], a[a.shape[0] // 2 :]
        upper = (me & bit) != 0
        away = lax.ppermute(jnp.where(upper, low, high), "mem", [(i, i ^ bit) for i in range(count)])
        a = jnp.where(upper, high, low) + away
        bit //= 2
    return a


def on_device(perturbation, obs_cells, obs_count, innovation, obs_scale):
    bands = lax.axis_size("lat")
    members, fine_rows, lon_cells = perturbation.shape
    coarse_rows = fine_rows // 2
    coarse_cols = lon_cells // 2
    slots = obs_cells.shape[1]
    half = members * coarse_rows
    scale = float((members * lax.axis_size("mem") - 1) ** (-0.5))
    t1, t2 = lon_blocks(coarse_cols)
    tables = jnp.asarray(lat_tables(bands, coarse_rows))
    groups = lax.axis_size("mem")
    place = jnp.stack([lax.axis_index("mem"), lax.axis_index("lat")]).astype(jnp.int32)

    smem = pl.BlockSpec(memory_space=pltpu.SMEM)
    vmem = pl.BlockSpec(memory_space=pltpu.VMEM)
    f32 = functools.partial(jax.ShapeDtypeStruct, dtype=jnp.float32)

    field = perturbation.reshape(members * fine_rows, lon_cells)
    own = pl.pallas_call(
        functools.partial(prepare_kernel, members=members, fine_rows=fine_rows),
        out_shape=f32((members + META, slots)),
        in_specs=[smem] + [vmem] * 4,
        out_specs=vmem,
        scratch_shapes=[
            pltpu.VMEM((8, slots), jnp.float32),
            pltpu.VMEM((slots, 128), jnp.float32),
            pltpu.VMEM((members + META, slots + 512), jnp.float32),
        ],
        cost_estimate=pl.CostEstimate(flops=4 * 10**9, bytes_accessed=2 * 10**6, transcendentals=0),
        name="prepare",
    )(obs_count, field, obs_cells, innovation, obs_scale)
    near = []
    for d in range(-REACH, REACH + 1):
        near.append(lax.ppermute(own, "lat", [(s, s - d) for s in range(bands) if 0 <= s - d < bands]) if d else own)
    near = jnp.stack(near)
    bound = near[:, members + 4, :128].astype(jnp.int32)

    padded = slots + WINDOW
    scratch = [
        pltpu.VMEM((2 * half, padded), jnp.bfloat16),
        pltpu.VMEM((8, padded), jnp.float32),
        pltpu.VMEM((half, coarse_cols + BLK), jnp.float32),
    ]
    tiles = slots // 128
    width = lon_cells // groups
    state, hits, steps, controls, images = None, None, [], [], []
    for iteration in range(ITERS):
        order = min(iteration, 2)
        ins = [place, bound, near, tables, t2] + [[], [obs_cells, hits], [state, hits]][order]
        block = (groups * bands, tiles + (0 if iteration else 2 * (tiles // groups)), 128)
        outs = [f32(block), f32((half, coarse_cols)), f32((8, slots))]
        outs += [f32((6, bands, tiles, 128)), f32((1, 128))] if iteration else []
        got = pl.pallas_call(
            functools.partial(
                iter_kernel, members=members, coarse_rows=coarse_rows, scale2=scale * scale, order=order, bands=bands, groups=groups
            ),
            out_shape=outs,
            in_specs=[smem] * 2 + [vmem] * (len(ins) - 2),
            out_specs=[vmem] * len(outs),
            scratch_shapes=scratch
            + [pltpu.VMEM((8, padded), jnp.float32)]
            + [pltpu.VMEM((2 * half, coarse_cols + BLK), jnp.bfloat16), pltpu.VMEM((members + META, padded), jnp.float32)],
            cost_estimate=pl.CostEstimate(flops=7 * 10**9, bytes_accessed=3 * 10**6, transcendentals=0),
            name="iterate",
        )(*ins)
        if iteration:
            state = got[3]
            steps.append(got[4])
        hits = lax.all_to_all(got[0], ("mem", "lat"), 0, 0, tiled=True)
        side = pl.pallas_call(
            functools.partial(side_kernel, members=members, fine_rows=fine_rows, coarse_rows=coarse_rows, scale=scale),
            out_shape=[f32((half, coarse_cols)), f32((groups, fine_rows, width))],
            in_specs=[smem] * 2 + [vmem] * 6,
            out_specs=[vmem] * 2,
            scratch_shapes=scratch,
            cost_estimate=pl.CostEstimate(flops=4 * 10**9, bytes_accessed=6 * 10**6, transcendentals=0),
            name="side",
        )
        control, image = side(place, bound, got[2], near, tables, t1, got[1], field)
        controls.append(control)
        images.append(scatter_mem(image)[0])
    control, image = pl.pallas_call(
        combine_kernel,
        out_shape=[f32((half, coarse_cols)), f32((fine_rows, width))],
        in_specs=[vmem] * (3 * ITERS + 1),
        out_specs=[vmem] * 2,
        cost_estimate=pl.CostEstimate(flops=10**7, bytes_accessed=4 * 10**6, transcendentals=0),
        name="combine",
    )(state, hits, *steps, *controls, *images)
    return control.reshape(members, coarse_rows, coarse_cols), image


def solution(mesh):
    in_specs = (P("mem", "lat", None), P("lat", None), P("lat"), P("lat", None), P("lat", None))
    out_specs = (P("mem", "lat", None), P("lat", "mem"))
    return jax.shard_map(on_device, mesh=mesh, in_specs=in_specs, out_specs=out_specs, check_vma=False)
```

```python
import functools

import jax
import jax.numpy as jnp
import numpy as np
from jax import lax
from jax.experimental import pallas as pl
from jax.experimental.pallas import tpu as pltpu
from jax.sharding import PartitionSpec as P

HALO = 8
LSIG = 3
ITERS = 3
REACH = 2
NREL = 2 * REACH + 1
BLK = 256
EDGE = 128
META = 8
WINDOW = 768


def lat_tables(bands, coarse_rows):
    rows = bands * coarse_rows
    offset = np.arange(rows)[:, None] - np.arange(rows)[None, :]
    spread = HALO / 2.0
    r1 = np.where(np.abs(offset) <= HALO, 0.5 * np.exp(-offset * offset / (2.0 * spread * spread)), 0.0)
    r2 = r1 @ r1
    out = np.zeros((bands, 2, NREL, coarse_rows, 128), np.float32)
    for b in range(bands):
        for d in range(NREL):
            s = b + d - REACH
            if 0 <= s < bands:
                own = slice(b * coarse_rows, (b + 1) * coarse_rows)
                other = slice(s * coarse_rows, (s + 1) * coarse_rows)
                out[b, 0, d, :, :coarse_rows] = r2[own, other]
                out[b, 1, d, :, :coarse_rows] = r1[own, other]
    return out


def lon_blocks(coarse_cols):
    d = np.arange(coarse_cols)
    d = np.minimum(d, coarse_cols - d).astype(np.float32)
    c1 = np.exp(-d * d / np.float32(2.0 * LSIG * LSIG)).astype(np.float32).astype(np.float64)
    c2 = np.real(np.fft.ifft(np.fft.fft(c1) ** 2))
    away = np.arange(BLK + 2 * EDGE)[:, None] - EDGE - np.arange(BLK)[None, :]
    inside = np.abs(away) <= EDGE
    blocks = []
    for c in (c1, c2):
        t = jnp.asarray(np.where(inside, c[away % coarse_cols], 0.0).astype(np.float32))
        hi = t.astype(jnp.bfloat16)
        lo = (t - hi.astype(jnp.float32)).astype(jnp.bfloat16)
        blocks.append(jnp.stack([hi, lo]))
    return blocks


def split(a):
    hi = a.astype(jnp.bfloat16)
    return hi, (a - hi.astype(jnp.float32)).astype(jnp.bfloat16)


def dot(a, b, dims=((1,), (0,))):
    return lax.dot_general(a, b, (dims, ((), ())), preferred_element_type=jnp.float32)


def full(ref_shape, dim):
    return lax.broadcasted_iota(jnp.int32, ref_shape, dim).astype(jnp.float32)


def hat_of(x, count):
    middle = 0.5 * (count - 1)
    near = x - middle
    near = jnp.where(jnp.abs(near) > middle + 0.75, float(count), near).astype(jnp.bfloat16)
    j = (full((count, x.shape[1]), 0) - middle).astype(jnp.bfloat16)
    one = jnp.asarray(1, jnp.bfloat16)
    return jnp.maximum(one - jnp.abs(near - j), jnp.asarray(0, jnp.bfloat16))


def pieces(a):
    out = []
    for _ in range(3):
        out.append(a.astype(jnp.bfloat16))
        a = a - out[-1].astype(jnp.float32)
    return out


def count(mask):
    return jnp.sum(jnp.where(mask, 1.0, 0.0)).astype(jnp.int32)


def prepare_kernel(count_ref, p_ref, cell_ref, innovation_ref, scale_ref, out_ref, key_ref, kcol_ref, srt_ref, *, members, fine_rows):
    lon = p_ref.shape[1]
    slots = cell_ref.shape[1]
    cell = cell_ref[...].astype(jnp.float32)
    row = jnp.floor((cell + 0.5) / float(lon))
    col = cell - row * float(lon)
    dead = full((1, slots), 1) >= count_ref[0].astype(jnp.float32)
    signed = jnp.where(dead, -scale_ref[...], scale_ref[...])
    key = jnp.where(dead, col + float(lon), col) * float(slots) + full((1, slots), 1)
    key_ref[0:1, :] = key
    top = jnp.floor(key / 65536.0)
    low = key - top * 65536.0
    mid = jnp.floor(low / 256.0)
    parts = jnp.concatenate([top, mid, low - mid * 256.0, jnp.zeros((13, slots), jnp.float32)], axis=0).astype(jnp.bfloat16)
    r = full((16, 128), 0)
    base = jnp.where(r == 0.0, 65536.0, jnp.where(r == 1.0, 256.0, jnp.where(r == 2.0, 1.0, 0.0))).astype(jnp.bfloat16)
    kcol_ref[...] = dot(parts, base, ((0,), (0,)))

    def rank(n, _):
        at = pl.ds(pl.multiple_of(n * 128, 128), 128)
        below = jnp.where(kcol_ref[...] < key_ref[0:1, at], 1.0, 0.0)
        below = jnp.sum(below.reshape(slots // 64, 64, 128), axis=0)
        key_ref[1:2, at] = jnp.sum(below, axis=0, keepdims=True)
        return 0

    lax.fori_loop(0, slots // 128, rank, 0)

    srt_ref[...] = jnp.zeros_like(srt_ref)
    high = jnp.floor(col / 256.0)
    rows = [high.astype(jnp.bfloat16), (col - high * 256.0).astype(jnp.bfloat16), row.astype(jnp.bfloat16)]
    rows += pieces(innovation_ref[...]) + pieces(signed)
    rows.append(jnp.zeros((16 - len(rows), slots), jnp.bfloat16))
    rows = jnp.concatenate([a.astype(jnp.float32) for a in rows], axis=0).astype(jnp.bfloat16)

    def permute(n, _):
        at = pl.ds(pl.multiple_of(n * BLK, BLK), BLK)
        place = key_ref[1:2, :] - (n * BLK).astype(jnp.float32)
        one = jnp.where(full((BLK, slots), 0) == place, 1.0, 0.0).astype(jnp.bfloat16)
        got = dot(rows, one, ((1,), (1,)))
        srt_ref[members : members + 1, at] = 128.0 * got[0:1] + 0.5 * got[1:2]
        srt_ref[members + 1 : members + 2, at] = got[2:3]
        srt_ref[members + 2 : members + 3, at] = got[3:4] + got[4:5] + got[5:6]
        srt_ref[members + 3 : members + 4, at] = got[6:7] + got[7:8] + got[8:9]
        return 0

    lax.fori_loop(0, slots // BLK, permute, 0)

    lane = full((1, 128), 1)
    bounds = jnp.zeros((1, 128), jnp.float32)
    blocks = lon // (2 * BLK)
    for c in range(blocks + 1):
        first = jnp.where(jnp.logical_and(jnp.logical_not(dead), col <= 2.0 * BLK * c - 2.0), 1.0, 0.0)
        last = jnp.where(jnp.logical_and(jnp.logical_not(dead), col < 2.0 * BLK * (c + 1)), 1.0, 0.0)
        bounds = jnp.where(lane == float(c), jnp.sum(first, axis=1, keepdims=True), bounds)
        bounds = jnp.where(lane == float(64 + c), jnp.sum(last, axis=1, keepdims=True), bounds)
    srt_ref[members + 4 : members + 5, 0:128] = bounds

    live = jnp.logical_not(dead)
    edges = [count(jnp.logical_and(live, col < float(c * BLK))) for c in range(lon // BLK + 1)]

    def window(c, start):
        at = pl.ds(pl.multiple_of(start, 128), 512)
        cols = 2.0 * srt_ref[members : members + 1, at] - float(c * BLK)
        one = jnp.where(full((BLK, 512), 0) == cols, 1.0, 0.0).astype(jnp.bfloat16)
        got = dot(p_ref[:, c * BLK : (c + 1) * BLK], one).reshape(members, fine_rows, 512)
        mask = jnp.where(full((fine_rows, 512), 0) == srt_ref[members + 1 : members + 2, at], 1.0, 0.0)
        srt_ref[0:members, at] = srt_ref[0:members, at] + jnp.sum(got * mask[None], axis=1)

    starts = [s // 128 * 128 for s in edges[:-1]]
    for c, start in enumerate(starts):
        window(c, start)
    for c, start in enumerate(starts):

        def more(i, _, c=c, start=start):
            window(c, start + i * 512)
            return 0

        lax.fori_loop(1, (edges[c + 1] - start + 511) // 512, more, 0)
    out_ref[...] = srt_ref[:, :slots]


def windows(bound_ref, d, c):
    s, e = bound_ref[d, c], bound_ref[d, 64 + c]
    start = s // 128 * 128
    return start, jnp.where(e > s, (e - start + WINDOW - 1) // WINDOW, 0)


def scatter(bound_ref, q_ref, tab, v_of, first, last, lhs_ref, at_ref, x_ref, members, coarse_rows):
    slots = q_ref.shape[2]
    half = members * coarse_rows
    blocks = x_ref.shape[1] // BLK - 1
    x_ref[...] = jnp.zeros_like(x_ref)
    lhs_ref[:, slots:] = jnp.zeros((2 * half, WINDOW), jnp.bfloat16)
    at_ref[...] = jnp.zeros_like(at_ref)

    def band(d, _):
        row = jnp.floor(q_ref[d, members + 1 : members + 2, :] * 0.5)
        v = v_of(d)
        at_ref[0:1, :slots] = q_ref[d, members : members + 1, :]
        weights = jnp.zeros((coarse_rows, slots), jnp.float32)
        taps = tab(d)
        for r in range(coarse_rows):
            weights = jnp.where(row == float(r), taps[:, r : r + 1], weights)
        weights = weights * v
        for k in range(members):
            hi, lo = split(weights * q_ref[d, k : k + 1, :])
            lhs_ref[k * coarse_rows : (k + 1) * coarse_rows, :slots] = hi
            lhs_ref[half + k * coarse_rows : half + (k + 1) * coarse_rows, :slots] = lo

        def one(c, start):
            at = pl.ds(pl.multiple_of(start, 128), WINDOW)
            hat = hat_of(at_ref[0:1, at] - c * float(BLK), BLK)
            got = dot(lhs_ref[:, at], hat, ((1,), (1,)))
            return got[:half] + got[half:]

        for c in range(blocks):
            to = slice(c * BLK, (c + 1) * BLK)
            x_ref[:, to] = x_ref[:, to] + one(float(c), windows(bound_ref, d, c)[0])

        def rest(c, _):
            start, trips = windows(bound_ref, d, c)
            to = pl.ds(pl.multiple_of(c * BLK, BLK), BLK)

            def more(i, _):
                x_ref[:, to] = x_ref[:, to] + one(c.astype(jnp.float32), start + i * WINDOW)
                return 0

            return lax.fori_loop(jnp.where(c < blocks, 1, 0), trips, more, 0)

        return lax.fori_loop(0, blocks + 1, rest, 0)

    lax.fori_loop(first, last, band, 0)
    x_ref[:, :EDGE] = x_ref[:, :EDGE] + x_ref[:, blocks * BLK : blocks * BLK + EDGE]


def lon_filter(x, t_ref):
    _, cols = x.shape
    ext = jnp.concatenate([x[:, cols - EDGE :], x, x[:, :EDGE]], axis=1)
    hi, lo = split(ext)
    parts = []
    for c in range(cols // BLK):
        at = slice(c * BLK, (c + 1) * BLK + 2 * EDGE)
        parts.append(dot(hi[:, at], t_ref[0]) + dot(lo[:, at], t_ref[0]) + dot(hi[:, at], t_ref[1]))
    return jnp.concatenate(parts, axis=1)


def step_of(hits, v, w):
    gg = jnp.full((1, 128), jnp.sum(v * hits), jnp.float32)
    cc = jnp.full((1, 128), jnp.sum(w * hits * hits), jnp.float32)
    return gg / (gg + cc + 1e-6)


def sum_mem(parts, bands):
    return jnp.sum(parts.reshape((parts.shape[0] // bands, bands) + parts.shape[1:]), axis=0)


def pull_of(target, signed):
    bounded = jnp.tanh(target / jnp.abs(signed))
    return jnp.where(signed > 0.0, signed * bounded, 0.0), jnp.where(signed > 0.0, 1.0 - bounded * bounded, 0.0)


def lay_rows(rows_ref, tile_of, bands):
    for d in range(NREL):
        tile = tile_of(jnp.clip(bands[0] + d - REACH, 0, bands[1] - 1))
        for i in range(tile.shape[0]):
            rows_ref[d : d + 1, i * 128 : (i + 1) * 128] = tile[i : i + 1, :]


def iter_kernel(place_ref, bound_ref, q_ref, tab_ref, t2_ref, *refs, members, coarse_rows, scale2, order, bands, groups):
    slots = q_ref.shape[2]
    tiles = slots // 128
    share = tiles // groups
    band = place_ref[1]
    if order == 0:
        part_ref, b_ref, vrow_ref, lhs_ref, at_ref, x_ref, rows_ref, bhl_ref, own_ref = refs
        for d in range(NREL):
            vrow_ref[d : d + 1, :] = pull_of(q_ref[d, members + 2 : members + 3, :], q_ref[d, members + 3 : members + 4, :])[0]
    else:
        old_ref, hits_ref, part_ref, b_ref, vrow_ref, state_ref, step_ref, lhs_ref, at_ref, x_ref, rows_ref, bhl_ref, own_ref = refs
        hits = sum_mem(hits_ref[:, :tiles, :], bands)
        if order == 1:
            for g in range(groups):
                mine = slice(g * bands, (g + 1) * bands)
                at = slice(g * share, (g + 1) * share)
                state_ref[0, :, at, :] = hits_ref[mine, tiles : tiles + share, :]
                state_ref[1, :, at, :] = hits_ref[mine, tiles + share : tiles + 2 * share, :]
            v, w = pull_of(state_ref[0], state_ref[1])
            observed, lam = 0.0, 0.0
        else:
            state_ref[0:2] = old_ref[0:2]
            v, w, observed, lam = old_ref[2], old_ref[3], old_ref[4], old_ref[5]
        step = step_of(hits, v, w)
        step_ref[...] = step
        step = step[0:1, 0:1][None]
        observed = observed + step * hits
        lam = lam + step * v
        pull, weight = pull_of(state_ref[0] - observed, state_ref[1])
        state_ref[2] = pull - lam
        state_ref[3] = weight
        state_ref[4] = observed
        state_ref[5] = lam
        lay_rows(vrow_ref, lambda b: state_ref[2, b], (band, bands))

    def v_of(d):
        return vrow_ref[pl.ds(d, 1), :]

    half = members * coarse_rows
    blocks = x_ref.shape[1] // BLK - 1
    cols = blocks * BLK
    scatter(bound_ref, q_ref, lambda d: tab_ref[band, 0, d], v_of, 0, NREL, lhs_ref, at_ref, x_ref, members, coarse_rows)
    b = lon_filter(x_ref[:, :cols], t2_ref)
    b_ref[...] = b
    hi, lo = split(b)
    bhl_ref[:half, :cols] = hi
    bhl_ref[half:, :cols] = lo
    bhl_ref[:, cols:] = bhl_ref[:, :BLK]
    own_ref[:, :slots] = q_ref[REACH]
    own_ref[:, slots:] = jnp.zeros((members + META, WINDOW), jnp.float32)
    rows_ref[...] = jnp.zeros_like(rows_ref)

    def gather(c, start):
        at = pl.ds(pl.multiple_of(start, 128), WINDOW)
        row = jnp.floor(own_ref[members + 1 : members + 2, at] * 0.5)
        hat = hat_of(own_ref[members : members + 1, at] - jnp.float32(c) * float(BLK), BLK)
        got = dot(bhl_ref[:, pl.ds(pl.multiple_of(c * BLK, BLK), BLK)], hat)
        mask = jnp.where(full((coarse_rows, WINDOW), 0) == row, scale2, 0.0)
        total = jnp.zeros((coarse_rows, WINDOW), jnp.float32)
        for k in range(members):
            r = slice(k * coarse_rows, (k + 1) * coarse_rows)
            r2 = slice(half + k * coarse_rows, half + (k + 1) * coarse_rows)
            total = total + own_ref[k : k + 1, at] * (got[r] + got[r2])
        rows_ref[0:1, at] = rows_ref[0:1, at] + jnp.sum(total * mask, axis=0, keepdims=True)

    for c in range(blocks):
        gather(c, windows(bound_ref, REACH, c)[0])

    def rest(c, _):
        start, trips = windows(bound_ref, REACH, c)

        def more(i, _):
            gather(c, start + i * WINDOW)
            return 0

        return lax.fori_loop(jnp.where(c < blocks, 1, 0), trips, more, 0)

    lax.fori_loop(0, blocks + 1, rest, 0)
    for i in range(tiles):
        part_ref[0, i : i + 1, :] = rows_ref[0:1, i * 128 : (i + 1) * 128]
    if order == 0:
        for r in range(2):
            mine = pl.ds(pl.multiple_of(place_ref[0] * (share * 128), 128), share * 128)
            row = q_ref[REACH, members + 2 + r : members + 3 + r, mine]
            for i in range(share):
                to = tiles + r * share + i
                part_ref[0, to : to + 1, :] = row[:, i * 128 : (i + 1) * 128]
    part_ref[1:] = jnp.broadcast_to(part_ref[0][None], (part_ref.shape[0] - 1,) + part_ref.shape[1:])


def side_kernel(
    place_ref, bound_ref, vrow_ref, q_ref, tab_ref, t1_ref, b_ref, p_ref, control_ref, image_ref, lhs_ref, at_ref, x_ref,
    *, members, fine_rows, coarse_rows, scale,
):
    def v_of(d):
        return vrow_ref[pl.ds(d, 1), :]

    tab = lambda d: tab_ref[place_ref[1], 1, d]
    scatter(bound_ref, q_ref, tab, v_of, REACH - 1, REACH + 2, lhs_ref, at_ref, x_ref, members, coarse_rows)
    control_ref[...] = scale * lon_filter(x_ref[:, : b_ref.shape[1]], t1_ref)

    b = b_ref[...]
    half, cols = b.shape
    wide = 2 * half
    repeat = jnp.where(
        lax.broadcasted_iota(jnp.int32, (wide, half), 0) // 2 == lax.broadcasted_iota(jnp.int32, (wide, half), 1), 1.0, 0.0
    ).astype(jnp.bfloat16)
    hi, lo = split(jnp.concatenate([b, b[:, :EDGE]], axis=1))
    hi = dot(repeat, hi).astype(jnp.bfloat16)
    lo = dot(repeat, lo).astype(jnp.bfloat16)
    hat = jnp.maximum(1.0 - jnp.abs(0.5 * full((2 * EDGE, 2 * EDGE), 1) - full((2 * EDGE, 2 * EDGE), 0)), 0.0)
    hat = hat.astype(jnp.bfloat16)
    for f in range(cols // EDGE):
        at = slice(f * EDGE, f * EDGE + 2 * EDGE)
        fine = slice(2 * f * EDGE, 2 * (f + 1) * EDGE)
        field = dot(hi[:, at], hat) + dot(lo[:, at], hat)
        product = p_ref[:, fine].astype(jnp.float32) * field
        part = (scale * scale) * jnp.sum(product.reshape(members, fine_rows, 2 * EDGE), axis=0)
        width = image_ref.shape[2]
        for start in range(0, 2 * EDGE, min(width, 2 * EDGE)):
            stop = start + min(width, 2 * EDGE)
            group, to = divmod(2 * f * EDGE + start, width)
            image_ref[group, :, to : to + stop - start] = part[:, start:stop]


def combine_kernel(place_ref, state_ref, hits_ref, *refs):
    steps, controls, images = refs[: ITERS - 1], refs[ITERS - 1 : 2 * ITERS - 1], refs[2 * ITERS - 1 : 3 * ITERS - 1]
    control_ref, block_refs = refs[3 * ITERS - 1], refs[3 * ITERS :]
    last = step_of(sum_mem(hits_ref[...], state_ref.shape[1]), state_ref[2], state_ref[3])[0:1, 0:1]
    steps = [s[0:1, 0:1] for s in steps] + [last]
    for away, block_ref in enumerate(block_refs):
        block_ref[...] = sum(s * i[place_ref[0] ^ away] for s, i in zip(steps, images))
    control_ref[...] = sum(s * c[...] for s, c in zip(steps, controls))


def on_device(perturbation, obs_cells, obs_count, innovation, obs_scale):
    bands = lax.axis_size("lat")
    members, fine_rows, lon_cells = perturbation.shape
    coarse_rows = fine_rows // 2
    coarse_cols = lon_cells // 2
    slots = obs_cells.shape[1]
    half = members * coarse_rows
    scale = float((members * lax.axis_size("mem") - 1) ** (-0.5))
    t1, t2 = lon_blocks(coarse_cols)
    tables = jnp.asarray(lat_tables(bands, coarse_rows))
    groups = lax.axis_size("mem")
    place = jnp.stack([lax.axis_index("mem"), lax.axis_index("lat")]).astype(jnp.int32)

    smem = pl.BlockSpec(memory_space=pltpu.SMEM)
    vmem = pl.BlockSpec(memory_space=pltpu.VMEM)
    f32 = functools.partial(jax.ShapeDtypeStruct, dtype=jnp.float32)

    field = perturbation.reshape(members * fine_rows, lon_cells)
    own = pl.pallas_call(
        functools.partial(prepare_kernel, members=members, fine_rows=fine_rows),
        out_shape=f32((members + META, slots)),
        in_specs=[smem] + [vmem] * 4,
        out_specs=vmem,
        scratch_shapes=[
            pltpu.VMEM((8, slots), jnp.float32),
            pltpu.VMEM((slots, 128), jnp.float32),
            pltpu.VMEM((members + META, slots + 512), jnp.float32),
        ],
        cost_estimate=pl.CostEstimate(flops=4 * 10**9, bytes_accessed=2 * 10**6, transcendentals=0),
        name="prepare",
    )(obs_count, field, obs_cells, innovation, obs_scale)
    near = []
    for d in range(-REACH, REACH + 1):
        near.append(lax.ppermute(own, "lat", [(s, s - d) for s in range(bands) if 0 <= s - d < bands]) if d else own)
    near = jnp.stack(near)
    bound = near[:, members + 4, :128].astype(jnp.int32)

    padded = slots + WINDOW
    scratch = [
        pltpu.VMEM((2 * half, padded), jnp.bfloat16),
        pltpu.VMEM((8, padded), jnp.float32),
        pltpu.VMEM((half, coarse_cols + BLK), jnp.float32),
    ]
    tiles = slots // 128
    width = lon_cells // groups
    state, hits, steps, controls, images = None, None, [], [], []
    for iteration in range(ITERS):
        order = min(iteration, 2)
        ins = [place, bound, near, tables, t2] + [[], [obs_cells, hits], [state, hits]][order]
        block = (groups * bands, tiles + (0 if iteration else 2 * (tiles // groups)), 128)
        outs = [f32(block), f32((half, coarse_cols)), f32((8, slots))]
        outs += [f32((6, bands, tiles, 128)), f32((1, 128))] if iteration else []
        got = pl.pallas_call(
            functools.partial(
                iter_kernel, members=members, coarse_rows=coarse_rows, scale2=scale * scale, order=order, bands=bands, groups=groups
            ),
            out_shape=outs,
            in_specs=[smem] * 2 + [vmem] * (len(ins) - 2),
            out_specs=[vmem] * len(outs),
            scratch_shapes=scratch
            + [pltpu.VMEM((8, padded), jnp.float32)]
            + [pltpu.VMEM((2 * half, coarse_cols + BLK), jnp.bfloat16), pltpu.VMEM((members + META, padded), jnp.float32)],
            cost_estimate=pl.CostEstimate(flops=7 * 10**9, bytes_accessed=3 * 10**6, transcendentals=0),
            name="iterate",
        )(*ins)
        if iteration:
            state = got[3]
            steps.append(got[4])
        hits = lax.all_to_all(got[0], ("mem", "lat"), 0, 0, tiled=True)
        side = pl.pallas_call(
            functools.partial(side_kernel, members=members, fine_rows=fine_rows, coarse_rows=coarse_rows, scale=scale),
            out_shape=[f32((half, coarse_cols)), f32((groups, fine_rows, width))],
            in_specs=[smem] * 2 + [vmem] * 6,
            out_specs=[vmem] * 2,
            scratch_shapes=scratch,
            cost_estimate=pl.CostEstimate(flops=4 * 10**9, bytes_accessed=6 * 10**6, transcendentals=0),
            name="side",
        )
        control, image = side(place, bound, got[2], near, tables, t1, got[1], field)
        controls.append(control)
        images.append(image)
    control, image, *away = pl.pallas_call(
        combine_kernel,
        out_shape=[f32((half, coarse_cols))] + [f32((fine_rows, width))] * groups,
        in_specs=[smem] + [vmem] * (3 * ITERS + 1),
        out_specs=[vmem] * (1 + groups),
        cost_estimate=pl.CostEstimate(flops=10**7, bytes_accessed=4 * 10**6, transcendentals=0),
        name="combine",
    )(place, state, hits, *steps, *controls, *images)
    for n, block in enumerate(away):
        image = image + lax.ppermute(block, "mem", [(i, i ^ (n + 1)) for i in range(groups)])
    return control.reshape(members, coarse_rows, coarse_cols), image


def solution(mesh):
    in_specs = (P("mem", "lat", None), P("lat", None), P("lat"), P("lat", None), P("lat", None))
    out_specs = (P("mem", "lat", None), P("lat", "mem"))
    return jax.shard_map(on_device, mesh=mesh, in_specs=in_specs, out_specs=out_specs, check_vma=False)
```

```python
import functools

import jax
import jax.numpy as jnp
import numpy as np
from jax import lax
from jax.experimental import pallas as pl
from jax.experimental.pallas import tpu as pltpu
from jax.sharding import PartitionSpec as P

HALO = 8
LSIG = 3
ITERS = 3
REACH = 2
NREL = 2 * REACH + 1
BLK = 256
EDGE = 128
META = 8
WINDOW = 768
SMALL = 512
VMEM_LIMIT = 24 * 2**20
REST = 256


def lat_tables(bands, coarse_rows):
    rows = bands * coarse_rows
    offset = np.arange(rows)[:, None] - np.arange(rows)[None, :]
    spread = HALO / 2.0
    r1 = np.where(np.abs(offset) <= HALO, 0.5 * np.exp(-offset * offset / (2.0 * spread * spread)), 0.0)
    r2 = r1 @ r1
    out = np.zeros((bands, 2, NREL, coarse_rows, 128), np.float32)
    for b in range(bands):
        for d in range(NREL):
            s = b + d - REACH
            if 0 <= s < bands:
                own = slice(b * coarse_rows, (b + 1) * coarse_rows)
                other = slice(s * coarse_rows, (s + 1) * coarse_rows)
                out[b, 0, d, :, :coarse_rows] = r2[own, other]
                out[b, 1, d, :, :coarse_rows] = r1[own, other]
    return out


def lon_blocks(coarse_cols):
    d = np.arange(coarse_cols)
    d = np.minimum(d, coarse_cols - d).astype(np.float32)
    c1 = np.exp(-d * d / np.float32(2.0 * LSIG * LSIG)).astype(np.float32).astype(np.float64)
    c2 = np.real(np.fft.ifft(np.fft.fft(c1) ** 2))
    away = np.arange(BLK + 2 * EDGE)[:, None] - EDGE - np.arange(BLK)[None, :]
    inside = np.abs(away) <= EDGE
    blocks = []
    for c in (c1, c2):
        t = jnp.asarray(np.where(inside, c[away % coarse_cols], 0.0).astype(np.float32))
        hi = t.astype(jnp.bfloat16)
        lo = (t - hi.astype(jnp.float32)).astype(jnp.bfloat16)
        blocks.append(jnp.stack([hi, lo]))
    return blocks


def split(a):
    hi = a.astype(jnp.bfloat16)
    return hi, (a - hi.astype(jnp.float32)).astype(jnp.bfloat16)


def dot(a, b, dims=((1,), (0,))):
    return lax.dot_general(a, b, (dims, ((), ())), preferred_element_type=jnp.float32)


def full(ref_shape, dim):
    return lax.broadcasted_iota(jnp.int32, ref_shape, dim).astype(jnp.float32)


def hat_of(x, count):
    middle = 0.5 * (count - 1)
    near = x - middle
    near = jnp.where(jnp.abs(near) > middle + 0.75, float(count), near).astype(jnp.bfloat16)
    j = (full((count, x.shape[1]), 0) - middle).astype(jnp.bfloat16)
    one = jnp.asarray(1, jnp.bfloat16)
    return jnp.maximum(one - jnp.abs(near - j), jnp.asarray(0, jnp.bfloat16))


def pieces(a):
    out = []
    for _ in range(3):
        out.append(a.astype(jnp.bfloat16))
        a = a - out[-1].astype(jnp.float32)
    return out


def count(mask):
    return jnp.sum(jnp.where(mask, 1.0, 0.0)).astype(jnp.int32)


def prepare_kernel(count_ref, p_ref, cell_ref, innovation_ref, scale_ref, out_ref, key_ref, kcol_ref, srt_ref, *, members, fine_rows):
    lon = p_ref.shape[1]
    slots = cell_ref.shape[1]
    cell = cell_ref[...].astype(jnp.float32)
    row = jnp.floor((cell + 0.5) / float(lon))
    col = cell - row * float(lon)
    dead = full((1, slots), 1) >= count_ref[0].astype(jnp.float32)
    signed = jnp.where(dead, -scale_ref[...], scale_ref[...])
    key = jnp.where(dead, col + float(lon), col) * float(slots) + full((1, slots), 1)
    key_ref[0:1, :] = key
    top = jnp.floor(key / 65536.0)
    low = key - top * 65536.0
    mid = jnp.floor(low / 256.0)
    parts = jnp.concatenate([top, mid, low - mid * 256.0, jnp.zeros((13, slots), jnp.float32)], axis=0).astype(jnp.bfloat16)
    r = full((16, 128), 0)
    base = jnp.where(r == 0.0, 65536.0, jnp.where(r == 1.0, 256.0, jnp.where(r == 2.0, 1.0, 0.0))).astype(jnp.bfloat16)
    kcol_ref[...] = dot(parts, base, ((0,), (0,)))

    def rank(n, _):
        at = pl.ds(pl.multiple_of(n * 128, 128), 128)
        below = jnp.where(kcol_ref[...] < key_ref[0:1, at], 1.0, 0.0)
        below = jnp.sum(below.reshape(slots // 64, 64, 128), axis=0)
        key_ref[1:2, at] = jnp.sum(below, axis=0, keepdims=True)
        return 0

    lax.fori_loop(0, slots // 128, rank, 0)

    srt_ref[...] = jnp.zeros_like(srt_ref)
    high = jnp.floor(col / 256.0)
    rows = [high.astype(jnp.bfloat16), (col - high * 256.0).astype(jnp.bfloat16), row.astype(jnp.bfloat16)]
    rows += pieces(innovation_ref[...]) + pieces(signed)
    rows.append(jnp.zeros((16 - len(rows), slots), jnp.bfloat16))
    rows = jnp.concatenate([a.astype(jnp.float32) for a in rows], axis=0).astype(jnp.bfloat16)

    def permute(n, _):
        at = pl.ds(pl.multiple_of(n * BLK, BLK), BLK)
        place = key_ref[1:2, :] - (n * BLK).astype(jnp.float32)
        one = jnp.where(full((BLK, slots), 0) == place, 1.0, 0.0).astype(jnp.bfloat16)
        got = dot(rows, one, ((1,), (1,)))
        srt_ref[members : members + 1, at] = 128.0 * got[0:1] + 0.5 * got[1:2]
        srt_ref[members + 1 : members + 2, at] = got[2:3]
        srt_ref[members + 2 : members + 3, at] = got[3:4] + got[4:5] + got[5:6]
        srt_ref[members + 3 : members + 4, at] = got[6:7] + got[7:8] + got[8:9]
        return 0

    lax.fori_loop(0, slots // BLK, permute, 0)

    lane = full((1, 128), 1)
    bounds = jnp.zeros((1, 128), jnp.float32)
    blocks = lon // (2 * BLK)
    for c in range(blocks + 1):
        first = jnp.where(jnp.logical_and(jnp.logical_not(dead), col <= 2.0 * BLK * c - 2.0), 1.0, 0.0)
        last = jnp.where(jnp.logical_and(jnp.logical_not(dead), col < 2.0 * BLK * (c + 1)), 1.0, 0.0)
        bounds = jnp.where(lane == float(c), jnp.sum(first, axis=1, keepdims=True), bounds)
        bounds = jnp.where(lane == float(64 + c), jnp.sum(last, axis=1, keepdims=True), bounds)
    srt_ref[members + 4 : members + 5, 0:128] = bounds

    live = jnp.logical_not(dead)
    edges = [count(jnp.logical_and(live, col < float(c * BLK))) for c in range(lon // BLK + 1)]

    def window(c, start):
        at = pl.ds(pl.multiple_of(start, 128), 512)
        cols = 2.0 * srt_ref[members : members + 1, at] - float(c * BLK)
        one = jnp.where(full((BLK, 512), 0) == cols, 1.0, 0.0).astype(jnp.bfloat16)
        got = dot(p_ref[:, c * BLK : (c + 1) * BLK], one).reshape(members, fine_rows, 512)
        mask = jnp.where(full((fine_rows, 512), 0) == srt_ref[members + 1 : members + 2, at], 1.0, 0.0)
        srt_ref[0:members, at] = srt_ref[0:members, at] + jnp.sum(got * mask[None], axis=1)

    starts = [s // 128 * 128 for s in edges[:-1]]
    for c, start in enumerate(starts):
        window(c, start)
    for c, start in enumerate(starts):

        def more(i, _, c=c, start=start):
            window(c, start + i * 512)
            return 0

        lax.fori_loop(1, (edges[c + 1] - start + 511) // 512, more, 0)
    out_ref[...] = srt_ref[:, :slots]


def window(bound_ref, d, c):
    return bound_ref[d, c] // 128 * 128, bound_ref[d, 64 + c]


def rest(bound_ref, d, blocks, done, fn):
    def block(c, _):
        start, end = window(bound_ref, d, c)
        start = start + jnp.where(c < blocks, done, 0)
        trips = jnp.where(end > start, (end - start + REST - 1) // REST, 0)

        def more(i, _):
            fn(c, start + i * REST, REST)
            return 0

        return lax.fori_loop(0, trips, more, 0)

    lax.fori_loop(0, blocks + 1, block, 0)


def scatter(bound_ref, q_ref, tab, v_of, first, last, lhs_ref, at_ref, x_ref, members, coarse_rows):
    slots = q_ref.shape[2]
    half = members * coarse_rows
    blocks = x_ref.shape[1] // BLK - 1
    x_ref[...] = jnp.zeros_like(x_ref)
    lhs_ref[:, slots:] = jnp.zeros((2 * half, WINDOW), jnp.bfloat16)
    at_ref[...] = jnp.zeros_like(at_ref)

    def band(d, _):
        row = jnp.floor(q_ref[d, members + 1 : members + 2, :] * 0.5)
        v = v_of(d)
        at_ref[0:1, :slots] = q_ref[d, members : members + 1, :]
        weights = jnp.zeros((coarse_rows, slots), jnp.float32)
        taps = tab(d)
        for r in range(coarse_rows):
            weights = jnp.where(row == float(r), taps[:, r : r + 1], weights)
        weights = weights * v
        for k in range(members):
            hi, lo = split(weights * q_ref[d, k : k + 1, :])
            lhs_ref[k * coarse_rows : (k + 1) * coarse_rows, :slots] = hi
            lhs_ref[half + k * coarse_rows : half + (k + 1) * coarse_rows, :slots] = lo

        def one(c, start, size):
            at = pl.ds(pl.multiple_of(start, 128), size)
            to = pl.ds(pl.multiple_of(c * BLK, BLK), BLK)
            hat = hat_of(at_ref[0:1, at] - jnp.float32(c) * float(BLK), BLK)
            got = dot(lhs_ref[:, at], hat, ((1,), (1,)))
            x_ref[:, to] = x_ref[:, to] + (got[:half] + got[half:])

        longest = 0
        for c in range(blocks):
            start, end = window(bound_ref, d, c)
            longest = jnp.maximum(longest, end - start)

        def run(size):
            for c in range(blocks):
                one(c, window(bound_ref, d, c)[0], size)

        pl.when(longest <= SMALL)(lambda: run(SMALL))
        pl.when(longest > SMALL)(lambda: run(WINDOW))
        rest(bound_ref, d, blocks, WINDOW, one)
        return 0

    lax.fori_loop(first, last, band, 0)
    x_ref[:, :EDGE] = x_ref[:, :EDGE] + x_ref[:, blocks * BLK : blocks * BLK + EDGE]


def lon_filter(x, t_ref):
    _, cols = x.shape
    ext = jnp.concatenate([x[:, cols - EDGE :], x, x[:, :EDGE]], axis=1)
    hi, lo = split(ext)
    parts = []
    for c in range(cols // BLK):
        at = slice(c * BLK, (c + 1) * BLK + 2 * EDGE)
        parts.append(dot(hi[:, at], t_ref[0]) + dot(lo[:, at], t_ref[0]) + dot(hi[:, at], t_ref[1]))
    return jnp.concatenate(parts, axis=1)


def step_of(hits, v, w):
    gg = jnp.full((1, 128), jnp.sum(v * hits), jnp.float32)
    cc = jnp.full((1, 128), jnp.sum(w * hits * hits), jnp.float32)
    return gg / (gg + cc + 1e-6)


def sum_mem(parts, bands):
    return jnp.sum(parts.reshape((parts.shape[0] // bands, bands) + parts.shape[1:]), axis=0)


def pull_of(target, signed):
    bounded = jnp.tanh(target / jnp.abs(signed))
    return jnp.where(signed > 0.0, signed * bounded, 0.0), jnp.where(signed > 0.0, 1.0 - bounded * bounded, 0.0)


def lay_rows(rows_ref, tile_of, bands):
    for d in range(NREL):
        tile = tile_of(jnp.clip(bands[0] + d - REACH, 0, bands[1] - 1))
        for i in range(tile.shape[0]):
            rows_ref[d : d + 1, i * 128 : (i + 1) * 128] = tile[i : i + 1, :]


def iter_kernel(place_ref, bound_ref, q_ref, tab_ref, t2_ref, *refs, members, coarse_rows, scale2, order, bands, groups):
    slots = q_ref.shape[2]
    tiles = slots // 128
    share = tiles // groups
    band = place_ref[1]
    if order == 0:
        out_ref, b_ref, vrow_ref, lhs_ref, at_ref, x_ref, rows_ref, bhl_ref, own_ref, part_ref = refs
        for d in range(NREL):
            vrow_ref[d : d + 1, :] = pull_of(q_ref[d, members + 2 : members + 3, :], q_ref[d, members + 3 : members + 4, :])[0]
    else:
        old_ref, in_ref, out_ref, b_ref, vrow_ref, state_ref, step_ref, lhs_ref, at_ref, x_ref, rows_ref, bhl_ref, own_ref, part_ref, hits_ref = refs
        pltpu.sync_copy(in_ref, hits_ref)
        hits = sum_mem(hits_ref[:, :tiles, :], bands)
        if order == 1:
            for g in range(groups):
                mine = slice(g * bands, (g + 1) * bands)
                at = slice(g * share, (g + 1) * share)
                state_ref[0, :, at, :] = hits_ref[mine, tiles : tiles + share, :]
                state_ref[1, :, at, :] = hits_ref[mine, tiles + share : tiles + 2 * share, :]
            v, w = pull_of(state_ref[0], state_ref[1])
            observed, lam = 0.0, 0.0
        else:
            state_ref[0:2] = old_ref[0:2]
            v, w, observed, lam = old_ref[2], old_ref[3], old_ref[4], old_ref[5]
        step = step_of(hits, v, w)
        step_ref[...] = step
        step = step[0:1, 0:1][None]
        observed = observed + step * hits
        lam = lam + step * v
        pull, weight = pull_of(state_ref[0] - observed, state_ref[1])
        state_ref[2] = pull - lam
        state_ref[3] = weight
        state_ref[4] = observed
        state_ref[5] = lam
        lay_rows(vrow_ref, lambda b: state_ref[2, b], (band, bands))

    def v_of(d):
        return vrow_ref[pl.ds(d, 1), :]

    half = members * coarse_rows
    blocks = x_ref.shape[1] // BLK - 1
    cols = blocks * BLK
    scatter(bound_ref, q_ref, lambda d: tab_ref[band, 0, d], v_of, 0, NREL, lhs_ref, at_ref, x_ref, members, coarse_rows)
    b = lon_filter(x_ref[:, :cols], t2_ref)
    b_ref[...] = b
    hi, lo = split(b)
    bhl_ref[:half, :cols] = hi
    bhl_ref[half:, :cols] = lo
    bhl_ref[:, cols:] = bhl_ref[:, :BLK]
    own_ref[:, :slots] = q_ref[REACH]
    own_ref[:, slots:] = jnp.zeros((members + META, WINDOW), jnp.float32)
    rows_ref[...] = jnp.zeros_like(rows_ref)

    def gather(c, start, size):
        at = pl.ds(pl.multiple_of(start, 128), size)
        row = jnp.floor(own_ref[members + 1 : members + 2, at] * 0.5)
        hat = hat_of(own_ref[members : members + 1, at] - jnp.float32(c) * float(BLK), BLK)
        got = dot(bhl_ref[:, pl.ds(pl.multiple_of(c * BLK, BLK), BLK)], hat)
        mask = jnp.where(full((coarse_rows, size), 0) == row, scale2, 0.0)
        total = jnp.zeros((coarse_rows, size), jnp.float32)
        for k in range(members):
            r = slice(k * coarse_rows, (k + 1) * coarse_rows)
            r2 = slice(half + k * coarse_rows, half + (k + 1) * coarse_rows)
            total = total + own_ref[k : k + 1, at] * (got[r] + got[r2])
        rows_ref[0:1, at] = rows_ref[0:1, at] + jnp.sum(total * mask, axis=0, keepdims=True)

    for c in range(blocks):
        gather(c, window(bound_ref, REACH, c)[0], WINDOW)
    rest(bound_ref, REACH, blocks, WINDOW, gather)
    for i in range(tiles):
        part_ref[0, i : i + 1, :] = rows_ref[0:1, i * 128 : (i + 1) * 128]
    if order == 0:
        for r in range(2):
            mine = pl.ds(pl.multiple_of(place_ref[0] * (share * 128), 128), share * 128)
            row = q_ref[REACH, members + 2 + r : members + 3 + r, mine]
            for i in range(share):
                to = tiles + r * share + i
                part_ref[0, to : to + 1, :] = row[:, i * 128 : (i + 1) * 128]
    part_ref[1:] = jnp.broadcast_to(part_ref[0][None], (part_ref.shape[0] - 1,) + part_ref.shape[1:])
    pltpu.sync_copy(part_ref, out_ref)


def side_kernel(
    place_ref, bound_ref, vrow_ref, q_ref, tab_ref, t1_ref, b_ref, p_ref, control_ref, image_ref, lhs_ref, at_ref, x_ref,
    *, members, fine_rows, coarse_rows, scale,
):
    def v_of(d):
        return vrow_ref[pl.ds(d, 1), :]

    tab = lambda d: tab_ref[place_ref[1], 1, d]
    scatter(bound_ref, q_ref, tab, v_of, REACH - 1, REACH + 2, lhs_ref, at_ref, x_ref, members, coarse_rows)
    control_ref[...] = scale * lon_filter(x_ref[:, : b_ref.shape[1]], t1_ref)

    b = b_ref[...]
    half, cols = b.shape
    wide = 2 * half
    repeat = jnp.where(
        lax.broadcasted_iota(jnp.int32, (wide, half), 0) // 2 == lax.broadcasted_iota(jnp.int32, (wide, half), 1), 1.0, 0.0
    ).astype(jnp.bfloat16)
    hi, lo = split(jnp.concatenate([b, b[:, :EDGE]], axis=1))
    hi = dot(repeat, hi).astype(jnp.bfloat16)
    lo = dot(repeat, lo).astype(jnp.bfloat16)
    hat = jnp.maximum(1.0 - jnp.abs(0.5 * full((2 * EDGE, 2 * EDGE), 1) - full((2 * EDGE, 2 * EDGE), 0)), 0.0)
    hat = hat.astype(jnp.bfloat16)
    for f in range(cols // EDGE):
        at = slice(f * EDGE, f * EDGE + 2 * EDGE)
        fine = slice(2 * f * EDGE, 2 * (f + 1) * EDGE)
        field = dot(hi[:, at], hat) + dot(lo[:, at], hat)
        product = p_ref[:, fine].astype(jnp.float32) * field
        part = (scale * scale) * jnp.sum(product.reshape(members, fine_rows, 2 * EDGE), axis=0)
        width = image_ref.shape[2]
        for start in range(0, 2 * EDGE, min(width, 2 * EDGE)):
            stop = start + min(width, 2 * EDGE)
            group, to = divmod(2 * f * EDGE + start, width)
            image_ref[group, :, to : to + stop - start] = part[:, start:stop]


def combine_kernel(place_ref, state_ref, in_ref, *refs):
    steps, controls, images = refs[: ITERS - 1], refs[ITERS - 1 : 2 * ITERS - 1], refs[2 * ITERS - 1 : 3 * ITERS - 1]
    control_ref, block_refs, hits_ref = refs[3 * ITERS - 1], refs[3 * ITERS : -1], refs[-1]
    pltpu.sync_copy(in_ref, hits_ref)
    last = step_of(sum_mem(hits_ref[...], state_ref.shape[1]), state_ref[2], state_ref[3])[0:1, 0:1]
    steps = [s[0:1, 0:1] for s in steps] + [last]
    for away, block_ref in enumerate(block_refs):
        block_ref[...] = sum(s * i[place_ref[0] ^ away] for s, i in zip(steps, images))
    control_ref[...] = sum(s * c[...] for s, c in zip(steps, controls))


def on_device(perturbation, obs_cells, obs_count, innovation, obs_scale):
    bands = lax.axis_size("lat")
    members, fine_rows, lon_cells = perturbation.shape
    coarse_rows = fine_rows // 2
    coarse_cols = lon_cells // 2
    slots = obs_cells.shape[1]
    half = members * coarse_rows
    scale = float((members * lax.axis_size("mem") - 1) ** (-0.5))
    t1, t2 = lon_blocks(coarse_cols)
    tables = jnp.asarray(lat_tables(bands, coarse_rows))
    groups = lax.axis_size("mem")
    place = jnp.stack([lax.axis_index("mem"), lax.axis_index("lat")]).astype(jnp.int32)

    smem = pl.BlockSpec(memory_space=pltpu.SMEM)
    vmem = pl.BlockSpec(memory_space=pltpu.VMEM)
    anywhere = pl.BlockSpec(memory_space=pl.ANY)
    params = pltpu.CompilerParams(vmem_limit_bytes=VMEM_LIMIT)
    f32 = functools.partial(jax.ShapeDtypeStruct, dtype=jnp.float32)

    field = perturbation.reshape(members * fine_rows, lon_cells)
    own = pl.pallas_call(
        functools.partial(prepare_kernel, members=members, fine_rows=fine_rows),
        out_shape=f32((members + META, slots)),
        in_specs=[smem] + [vmem] * 4,
        out_specs=vmem,
        scratch_shapes=[
            pltpu.VMEM((8, slots), jnp.float32),
            pltpu.VMEM((slots, 128), jnp.float32),
            pltpu.VMEM((members + META, slots + 512), jnp.float32),
        ],
        cost_estimate=pl.CostEstimate(flops=4 * 10**9, bytes_accessed=2 * 10**6, transcendentals=0),
        compiler_params=params,
        name="prepare",
    )(obs_count, field, obs_cells, innovation, obs_scale)
    near = []
    for d in range(-REACH, REACH + 1):
        near.append(lax.ppermute(own, "lat", [(s, s - d) for s in range(bands) if 0 <= s - d < bands]) if d else own)
    near = jnp.stack(near)
    bound = near[:, members + 4, :128].astype(jnp.int32)

    padded = slots + WINDOW
    scratch = [
        pltpu.VMEM((2 * half, padded), jnp.bfloat16),
        pltpu.VMEM((8, padded), jnp.float32),
        pltpu.VMEM((half, coarse_cols + BLK), jnp.float32),
    ]
    tiles = slots // 128
    width = lon_cells // groups
    state, hits, steps, controls, images = None, None, [], [], []
    for iteration in range(ITERS):
        order = min(iteration, 2)
        ins = [place, bound, near, tables, t2] + [[], [obs_cells, hits], [state, hits]][order]
        block = (groups * bands, tiles + (0 if iteration else 2 * (tiles // groups)), 128)
        outs = [f32(block), f32((half, coarse_cols)), f32((8, slots))]
        outs += [f32((6, bands, tiles, 128)), f32((1, 128))] if iteration else []
        got = pl.pallas_call(
            functools.partial(
                iter_kernel, members=members, coarse_rows=coarse_rows, scale2=scale * scale, order=order, bands=bands, groups=groups
            ),
            out_shape=outs,
            in_specs=[smem] * 2 + [vmem] * 3 + ([vmem, anywhere] if iteration else []),
            out_specs=[anywhere] + [vmem] * (len(outs) - 1),
            scratch_shapes=scratch
            + [pltpu.VMEM((8, padded), jnp.float32)]
            + [pltpu.VMEM((2 * half, coarse_cols + BLK), jnp.bfloat16), pltpu.VMEM((members + META, padded), jnp.float32)]
            + [pltpu.VMEM(block, jnp.float32)]
            + ([pltpu.VMEM(hits.shape, jnp.float32)] if iteration else []),
            cost_estimate=pl.CostEstimate(flops=7 * 10**9, bytes_accessed=3 * 10**6, transcendentals=0),
            compiler_params=params,
            name="iterate",
        )(*ins)
        if iteration:
            state = got[3]
            steps.append(got[4])
        hits = lax.all_to_all(got[0], ("mem", "lat"), 0, 0, tiled=True)
        side = pl.pallas_call(
            functools.partial(side_kernel, members=members, fine_rows=fine_rows, coarse_rows=coarse_rows, scale=scale),
            out_shape=[f32((half, coarse_cols)), f32((groups, fine_rows, width))],
            in_specs=[smem] * 2 + [vmem] * 6,
            out_specs=[vmem] * 2,
            scratch_shapes=scratch,
            cost_estimate=pl.CostEstimate(flops=4 * 10**9, bytes_accessed=6 * 10**6, transcendentals=0),
            compiler_params=params,
            name="side",
        )
        control, image = side(place, bound, got[2], near, tables, t1, got[1], field)
        controls.append(control)
        images.append(image)
    control, image, *away = pl.pallas_call(
        combine_kernel,
        out_shape=[f32((half, coarse_cols))] + [f32((fine_rows, width))] * groups,
        in_specs=[smem, vmem, anywhere] + [vmem] * (3 * ITERS - 1),
        out_specs=[vmem] * (1 + groups),
        scratch_shapes=[pltpu.VMEM(hits.shape, jnp.float32)],
        cost_estimate=pl.CostEstimate(flops=10**7, bytes_accessed=4 * 10**6, transcendentals=0),
        compiler_params=params,
        name="combine",
    )(place, state, hits, *steps, *controls, *images)
    for n, block in enumerate(away):
        image = image + lax.ppermute(block, "mem", [(i, i ^ (n + 1)) for i in range(groups)])
    return control.reshape(members, coarse_rows, coarse_cols), image


def solution(mesh):
    in_specs = (P("mem", "lat", None), P("lat", None), P("lat"), P("lat", None), P("lat", None))
    out_specs = (P("mem", "lat", None), P("lat", "mem"))
    return jax.shard_map(on_device, mesh=mesh, in_specs=in_specs, out_specs=out_specs, check_vma=False)
```

```python
import functools

import jax
import jax.numpy as jnp
import numpy as np
from jax import lax
from jax.experimental import pallas as pl
from jax.experimental.pallas import tpu as pltpu
from jax.sharding import PartitionSpec as P

HALO = 8
LSIG = 3
ITERS = 3
REACH = 2
NREL = 2 * REACH + 1
BLK = 256
EDGE = 128
META = 8
WINDOW = 768
SMALL = 512
VMEM_LIMIT = 24 * 2**20
REST = 256


def lat_tables(bands, coarse_rows):
    rows = bands * coarse_rows
    offset = np.arange(rows)[:, None] - np.arange(rows)[None, :]
    spread = HALO / 2.0
    r1 = np.where(np.abs(offset) <= HALO, 0.5 * np.exp(-offset * offset / (2.0 * spread * spread)), 0.0)
    r2 = r1 @ r1
    out = np.zeros((bands, 2, NREL, coarse_rows, 128), np.float32)
    for b in range(bands):
        for d in range(NREL):
            s = b + d - REACH
            if 0 <= s < bands:
                own = slice(b * coarse_rows, (b + 1) * coarse_rows)
                other = slice(s * coarse_rows, (s + 1) * coarse_rows)
                out[b, 0, d, :, :coarse_rows] = r2[own, other]
                out[b, 1, d, :, :coarse_rows] = r1[own, other]
    return out


def lon_blocks(coarse_cols):
    d = np.arange(coarse_cols)
    d = np.minimum(d, coarse_cols - d).astype(np.float32)
    c1 = np.exp(-d * d / np.float32(2.0 * LSIG * LSIG)).astype(np.float32).astype(np.float64)
    c2 = np.real(np.fft.ifft(np.fft.fft(c1) ** 2))
    away = np.arange(BLK + 2 * EDGE)[:, None] - EDGE - np.arange(BLK)[None, :]
    inside = np.abs(away) <= EDGE
    blocks = []
    for c in (c1, c2):
        t = jnp.asarray(np.where(inside, c[away % coarse_cols], 0.0).astype(np.float32))
        hi = t.astype(jnp.bfloat16)
        lo = (t - hi.astype(jnp.float32)).astype(jnp.bfloat16)
        blocks.append(jnp.stack([hi, lo]))
    return blocks


def split(a):
    hi = a.astype(jnp.bfloat16)
    return hi, (a - hi.astype(jnp.float32)).astype(jnp.bfloat16)


def dot(a, b, dims=((1,), (0,))):
    return lax.dot_general(a, b, (dims, ((), ())), preferred_element_type=jnp.float32)


def full(ref_shape, dim):
    return lax.broadcasted_iota(jnp.int32, ref_shape, dim).astype(jnp.float32)


def hat_of(x, count):
    middle = 0.5 * (count - 1)
    near = x - middle
    near = jnp.where(jnp.abs(near) > middle + 0.75, float(count), near).astype(jnp.bfloat16)
    j = (full((count, x.shape[1]), 0) - middle).astype(jnp.bfloat16)
    one = jnp.asarray(1, jnp.bfloat16)
    return jnp.maximum(one - jnp.abs(near - j), jnp.asarray(0, jnp.bfloat16))


def pieces(a):
    out = []
    for _ in range(3):
        out.append(a.astype(jnp.bfloat16))
        a = a - out[-1].astype(jnp.float32)
    return out


def count(mask):
    return jnp.sum(jnp.where(mask, 1.0, 0.0)).astype(jnp.int32)


def fetch(*copies):
    started = [pltpu.make_async_copy(*copy) for copy in copies]
    for copy in started:
        copy.start()
    return started


def prepare_kernel(count_ref, far_ref, cell_ref, innovation_ref, scale_ref, out_ref, key_ref, kcol_ref, srt_ref, p_ref, sem, *, members, fine_rows):
    ready = fetch((far_ref, p_ref, sem.at[0]))
    lon = p_ref.shape[1]
    slots = cell_ref.shape[1]
    cell = cell_ref[...].astype(jnp.float32)
    row = jnp.floor((cell + 0.5) / float(lon))
    col = cell - row * float(lon)
    dead = full((1, slots), 1) >= count_ref[0].astype(jnp.float32)
    signed = jnp.where(dead, -scale_ref[...], scale_ref[...])
    key = jnp.where(dead, col + float(lon), col) * float(slots) + full((1, slots), 1)
    key_ref[0:1, :] = key
    top = jnp.floor(key / 65536.0)
    low = key - top * 65536.0
    mid = jnp.floor(low / 256.0)
    parts = jnp.concatenate([top, mid, low - mid * 256.0, jnp.zeros((13, slots), jnp.float32)], axis=0).astype(jnp.bfloat16)
    r = full((16, 128), 0)
    base = jnp.where(r == 0.0, 65536.0, jnp.where(r == 1.0, 256.0, jnp.where(r == 2.0, 1.0, 0.0))).astype(jnp.bfloat16)
    kcol_ref[...] = dot(parts, base, ((0,), (0,)))

    def rank(n, _):
        at = pl.ds(pl.multiple_of(n * 128, 128), 128)
        below = jnp.where(kcol_ref[...] < key_ref[0:1, at], 1.0, 0.0)
        below = jnp.sum(below.reshape(slots // 64, 64, 128), axis=0)
        key_ref[1:2, at] = jnp.sum(below, axis=0, keepdims=True)
        return 0

    lax.fori_loop(0, slots // 128, rank, 0)

    srt_ref[...] = jnp.zeros_like(srt_ref)
    high = jnp.floor(col / 256.0)
    rows = [high.astype(jnp.bfloat16), (col - high * 256.0).astype(jnp.bfloat16), row.astype(jnp.bfloat16)]
    rows += pieces(innovation_ref[...]) + pieces(signed)
    rows.append(jnp.zeros((16 - len(rows), slots), jnp.bfloat16))
    rows = jnp.concatenate([a.astype(jnp.float32) for a in rows], axis=0).astype(jnp.bfloat16)

    def permute(n, _):
        at = pl.ds(pl.multiple_of(n * BLK, BLK), BLK)
        place = key_ref[1:2, :] - (n * BLK).astype(jnp.float32)
        one = jnp.where(full((BLK, slots), 0) == place, 1.0, 0.0).astype(jnp.bfloat16)
        got = dot(rows, one, ((1,), (1,)))
        srt_ref[members : members + 1, at] = 128.0 * got[0:1] + 0.5 * got[1:2]
        srt_ref[members + 1 : members + 2, at] = got[2:3]
        srt_ref[members + 2 : members + 3, at] = got[3:4] + got[4:5] + got[5:6]
        srt_ref[members + 3 : members + 4, at] = got[6:7] + got[7:8] + got[8:9]
        return 0

    lax.fori_loop(0, slots // BLK, permute, 0)

    lane = full((1, 128), 1)
    bounds = jnp.zeros((1, 128), jnp.float32)
    blocks = lon // (2 * BLK)
    for c in range(blocks + 1):
        first = jnp.where(jnp.logical_and(jnp.logical_not(dead), col <= 2.0 * BLK * c - 2.0), 1.0, 0.0)
        last = jnp.where(jnp.logical_and(jnp.logical_not(dead), col < 2.0 * BLK * (c + 1)), 1.0, 0.0)
        bounds = jnp.where(lane == float(c), jnp.sum(first, axis=1, keepdims=True), bounds)
        bounds = jnp.where(lane == float(64 + c), jnp.sum(last, axis=1, keepdims=True), bounds)
    srt_ref[members + 4 : members + 5, 0:128] = bounds

    live = jnp.logical_not(dead)
    edges = [count(jnp.logical_and(live, col < float(c * BLK))) for c in range(lon // BLK + 1)]

    def window(c, start):
        at = pl.ds(pl.multiple_of(start, 128), 512)
        cols = 2.0 * srt_ref[members : members + 1, at] - float(c * BLK)
        one = jnp.where(full((BLK, 512), 0) == cols, 1.0, 0.0).astype(jnp.bfloat16)
        got = dot(p_ref[:, c * BLK : (c + 1) * BLK], one).reshape(members, fine_rows, 512)
        mask = jnp.where(full((fine_rows, 512), 0) == srt_ref[members + 1 : members + 2, at], 1.0, 0.0)
        srt_ref[0:members, at] = srt_ref[0:members, at] + jnp.sum(got * mask[None], axis=1)

    starts = [s // 128 * 128 for s in edges[:-1]]
    ready[0].wait()
    for c, start in enumerate(starts):
        window(c, start)
    for c, start in enumerate(starts):

        def more(i, _, c=c, start=start):
            window(c, start + i * 512)
            return 0

        lax.fori_loop(1, (edges[c + 1] - start + 511) // 512, more, 0)
    out_ref[...] = srt_ref[:, :slots]


def window(bound_ref, d, c):
    return bound_ref[d, c] // 128 * 128, bound_ref[d, 64 + c]


def rest(bound_ref, d, blocks, done, fn):
    def block(c, _):
        start, end = window(bound_ref, d, c)
        start = start + jnp.where(c < blocks, done, 0)
        trips = jnp.where(end > start, (end - start + REST - 1) // REST, 0)

        def more(i, _):
            fn(c, start + i * REST, REST)
            return 0

        return lax.fori_loop(0, trips, more, 0)

    lax.fori_loop(0, blocks + 1, block, 0)


def scatter(bound_ref, q_ref, tab, v_of, first, last, lhs_ref, at_ref, x_ref, members, coarse_rows, short=False):
    slots = q_ref.shape[2]
    half = members * coarse_rows
    blocks = x_ref.shape[1] // BLK - 1
    x_ref[...] = jnp.zeros_like(x_ref)
    lhs_ref[:, slots:] = jnp.zeros((2 * half, WINDOW), jnp.bfloat16)
    at_ref[...] = jnp.zeros_like(at_ref)

    def band(d, _):
        row = jnp.floor(q_ref[d, members + 1 : members + 2, :] * 0.5)
        v = v_of(d)
        at_ref[0:1, :slots] = q_ref[d, members : members + 1, :]
        weights = jnp.zeros((coarse_rows, slots), jnp.float32)
        taps = tab(d)
        for r in range(coarse_rows):
            weights = jnp.where(row == float(r), taps[:, r : r + 1], weights)
        weights = weights * v
        for k in range(members):
            hi, lo = split(weights * q_ref[d, k : k + 1, :])
            lhs_ref[k * coarse_rows : (k + 1) * coarse_rows, :slots] = hi
            lhs_ref[half + k * coarse_rows : half + (k + 1) * coarse_rows, :slots] = lo

        def one(c, start, size):
            at = pl.ds(pl.multiple_of(start, 128), size)
            to = pl.ds(pl.multiple_of(c * BLK, BLK), BLK)
            hat = hat_of(at_ref[0:1, at] - jnp.float32(c) * float(BLK), BLK)
            got = dot(lhs_ref[:, at], hat, ((1,), (1,)))
            x_ref[:, to] = x_ref[:, to] + (got[:half] + got[half:])

        longest = 0
        for c in range(blocks):
            start, end = window(bound_ref, d, c)
            longest = jnp.maximum(longest, end - start)

        def run(size):
            for c in range(blocks):
                one(c, window(bound_ref, d, c)[0], size)

        if short:
            pl.when(longest <= SMALL)(lambda: run(SMALL))
            pl.when(longest > SMALL)(lambda: run(WINDOW))
        else:
            run(WINDOW)
        rest(bound_ref, d, blocks, WINDOW, one)
        return 0

    lax.fori_loop(first, last, band, 0)
    x_ref[:, :EDGE] = x_ref[:, :EDGE] + x_ref[:, blocks * BLK : blocks * BLK + EDGE]


def lon_filter(x, t_ref):
    _, cols = x.shape
    ext = jnp.concatenate([x[:, cols - EDGE :], x, x[:, :EDGE]], axis=1)
    hi, lo = split(ext)
    parts = []
    for c in range(cols // BLK):
        at = slice(c * BLK, (c + 1) * BLK + 2 * EDGE)
        parts.append(dot(hi[:, at], t_ref[0]) + dot(lo[:, at], t_ref[0]) + dot(hi[:, at], t_ref[1]))
    return jnp.concatenate(parts, axis=1)


def step_of(hits, v, w):
    gg = jnp.full((1, 128), jnp.sum(v * hits), jnp.float32)
    cc = jnp.full((1, 128), jnp.sum(w * hits * hits), jnp.float32)
    return gg / (gg + cc + 1e-6)


def sum_mem(parts, bands):
    return jnp.sum(parts.reshape((parts.shape[0] // bands, bands) + parts.shape[1:]), axis=0)


def pull_of(target, signed):
    bounded = jnp.tanh(target / jnp.abs(signed))
    return jnp.where(signed > 0.0, signed * bounded, 0.0), jnp.where(signed > 0.0, 1.0 - bounded * bounded, 0.0)


def lay_rows(rows_ref, tile_of, bands):
    for d in range(NREL):
        tile = tile_of(jnp.clip(bands[0] + d - REACH, 0, bands[1] - 1))
        for i in range(tile.shape[0]):
            rows_ref[d : d + 1, i * 128 : (i + 1) * 128] = tile[i : i + 1, :]


def iter_kernel(place_ref, bound_ref, q_far, tab_far, t2_far, *refs, members, coarse_rows, scale2, order, bands, groups):
    q_ref, tab_ref, t2_ref, b_ref, sem = refs[-5:]
    refs = refs[:-5]
    slots = q_ref.shape[2]
    ready = fetch((q_far, q_ref, sem.at[0]), (tab_far.at[place_ref[1], 0], tab_ref, sem.at[1]), (t2_far, t2_ref, sem.at[2]))
    tiles = slots // 128
    share = tiles // groups
    band = place_ref[1]
    if order == 0:
        out_ref, b_far, vrow_ref, lhs_ref, at_ref, x_ref, rows_ref, bhl_ref, own_ref, part_ref = refs
        ready[0].wait()
        for d in range(NREL):
            vrow_ref[d : d + 1, :] = pull_of(q_ref[d, members + 2 : members + 3, :], q_ref[d, members + 3 : members + 4, :])[0]
    else:
        old_far, in_ref, out_ref, b_far, vrow_ref, state_far, step_ref = refs[:7]
        lhs_ref, at_ref, x_ref, rows_ref, bhl_ref, own_ref, part_ref, hits_ref, old_ref, state_ref = refs[7:]
        if order == 2:
            ready += fetch((old_far, old_ref, sem.at[3]))
        pltpu.sync_copy(in_ref, hits_ref)
        hits = sum_mem(hits_ref[:, :tiles, :], bands)
        if order == 1:
            for g in range(groups):
                mine = slice(g * bands, (g + 1) * bands)
                at = slice(g * share, (g + 1) * share)
                state_ref[0, :, at, :] = hits_ref[mine, tiles : tiles + share, :]
                state_ref[1, :, at, :] = hits_ref[mine, tiles + share : tiles + 2 * share, :]
            v, w = pull_of(state_ref[0], state_ref[1])
            observed, lam = 0.0, 0.0
        else:
            ready[3].wait()
            state_ref[0:2] = old_ref[0:2]
            v, w, observed, lam = old_ref[2], old_ref[3], old_ref[4], old_ref[5]
        step = step_of(hits, v, w)
        step_ref[...] = step
        step = step[0:1, 0:1][None]
        observed = observed + step * hits
        lam = lam + step * v
        pull, weight = pull_of(state_ref[0] - observed, state_ref[1])
        state_ref[2] = pull - lam
        state_ref[3] = weight
        state_ref[4] = observed
        state_ref[5] = lam
        saved = fetch((state_ref, state_far, sem.at[4]))
        lay_rows(vrow_ref, lambda b: state_ref[2, b], (band, bands))
        ready[0].wait()

    def v_of(d):
        return vrow_ref[pl.ds(d, 1), :]

    half = members * coarse_rows
    blocks = x_ref.shape[1] // BLK - 1
    cols = blocks * BLK
    ready[1].wait()
    scatter(bound_ref, q_ref, lambda d: tab_ref[d], v_of, 0, NREL, lhs_ref, at_ref, x_ref, members, coarse_rows, True)
    ready[2].wait()
    b = lon_filter(x_ref[:, :cols], t2_ref)
    b_ref[...] = b
    b_saved = fetch((b_ref, b_far, sem.at[5]))
    hi, lo = split(b)
    bhl_ref[:half, :cols] = hi
    bhl_ref[half:, :cols] = lo
    bhl_ref[:, cols:] = bhl_ref[:, :BLK]
    own_ref[:, :slots] = q_ref[REACH]
    own_ref[:, slots:] = jnp.zeros((members + META, WINDOW), jnp.float32)
    rows_ref[...] = jnp.zeros_like(rows_ref)

    def gather(c, start, size):
        at = pl.ds(pl.multiple_of(start, 128), size)
        row = jnp.floor(own_ref[members + 1 : members + 2, at] * 0.5)
        hat = hat_of(own_ref[members : members + 1, at] - jnp.float32(c) * float(BLK), BLK)
        got = dot(bhl_ref[:, pl.ds(pl.multiple_of(c * BLK, BLK), BLK)], hat)
        mask = jnp.where(full((coarse_rows, size), 0) == row, scale2, 0.0)
        total = jnp.zeros((coarse_rows, size), jnp.float32)
        for k in range(members):
            r = slice(k * coarse_rows, (k + 1) * coarse_rows)
            r2 = slice(half + k * coarse_rows, half + (k + 1) * coarse_rows)
            total = total + own_ref[k : k + 1, at] * (got[r] + got[r2])
        rows_ref[0:1, at] = rows_ref[0:1, at] + jnp.sum(total * mask, axis=0, keepdims=True)

    for c in range(blocks):
        gather(c, window(bound_ref, REACH, c)[0], WINDOW)
    rest(bound_ref, REACH, blocks, WINDOW, gather)
    for i in range(tiles):
        part_ref[0, i : i + 1, :] = rows_ref[0:1, i * 128 : (i + 1) * 128]
    if order == 0:
        for r in range(2):
            mine = pl.ds(pl.multiple_of(place_ref[0] * (share * 128), 128), share * 128)
            row = q_ref[REACH, members + 2 + r : members + 3 + r, mine]
            for i in range(share):
                to = tiles + r * share + i
                part_ref[0, to : to + 1, :] = row[:, i * 128 : (i + 1) * 128]
    part_ref[1:] = jnp.broadcast_to(part_ref[0][None], (part_ref.shape[0] - 1,) + part_ref.shape[1:])
    pltpu.sync_copy(part_ref, out_ref)
    b_saved[0].wait()
    if order:
        saved[0].wait()


def side_kernel(
    place_ref, bound_ref, vrow_ref, q_far, tab_far, t1_far, b_far, p_far, control_ref, image_ref, lhs_ref, at_ref, x_ref,
    q_ref, tab_ref, t1_ref, b_ref, p_ref, sem, *, members, fine_rows, coarse_rows, scale,
):
    def v_of(d):
        return vrow_ref[pl.ds(d, 1), :]

    near = pl.ds(REACH - 1, 3)
    ready = fetch(
        (q_far.at[near], q_ref.at[near], sem.at[0]), (tab_far.at[place_ref[1], 1], tab_ref, sem.at[1]), (t1_far, t1_ref, sem.at[2]),
        (b_far, b_ref, sem.at[3]), (p_far, p_ref, sem.at[4]),
    )
    ready[0].wait()
    ready[1].wait()
    tab = lambda d: tab_ref[d]
    scatter(bound_ref, q_ref, tab, v_of, REACH - 1, REACH + 2, lhs_ref, at_ref, x_ref, members, coarse_rows)
    for copy in ready[2:]:
        copy.wait()
    control_ref[...] = scale * lon_filter(x_ref[:, : b_ref.shape[1]], t1_ref)

    b = b_ref[...]
    half, cols = b.shape
    wide = 2 * half
    repeat = jnp.where(
        lax.broadcasted_iota(jnp.int32, (wide, half), 0) // 2 == lax.broadcasted_iota(jnp.int32, (wide, half), 1), 1.0, 0.0
    ).astype(jnp.bfloat16)
    hi, lo = split(jnp.concatenate([b, b[:, :EDGE]], axis=1))
    hi = dot(repeat, hi).astype(jnp.bfloat16)
    lo = dot(repeat, lo).astype(jnp.bfloat16)
    hat = jnp.maximum(1.0 - jnp.abs(0.5 * full((2 * EDGE, 2 * EDGE), 1) - full((2 * EDGE, 2 * EDGE), 0)), 0.0)
    hat = hat.astype(jnp.bfloat16)
    for f in range(cols // EDGE):
        at = slice(f * EDGE, f * EDGE + 2 * EDGE)
        fine = slice(2 * f * EDGE, 2 * (f + 1) * EDGE)
        field = dot(hi[:, at], hat) + dot(lo[:, at], hat)
        product = p_ref[:, fine].astype(jnp.float32) * field
        part = (scale * scale) * jnp.sum(product.reshape(members, fine_rows, 2 * EDGE), axis=0)
        width = image_ref.shape[2]
        for start in range(0, 2 * EDGE, min(width, 2 * EDGE)):
            stop = start + min(width, 2 * EDGE)
            group, to = divmod(2 * f * EDGE + start, width)
            image_ref[group, :, to : to + stop - start] = part[:, start:stop]


def combine_kernel(place_ref, state_ref, in_ref, *refs):
    steps, controls, images = refs[: ITERS - 1], refs[ITERS - 1 : 2 * ITERS - 1], refs[2 * ITERS - 1 : 3 * ITERS - 1]
    control_ref, block_refs, hits_ref = refs[3 * ITERS - 1], refs[3 * ITERS : -1], refs[-1]
    pltpu.sync_copy(in_ref, hits_ref)
    last = step_of(sum_mem(hits_ref[...], state_ref.shape[1]), state_ref[2], state_ref[3])[0:1, 0:1]
    steps = [s[0:1, 0:1] for s in steps] + [last]
    for away, block_ref in enumerate(block_refs):
        block_ref[...] = sum(s * i[place_ref[0] ^ away] for s, i in zip(steps, images))
    control_ref[...] = sum(s * c[...] for s, c in zip(steps, controls))


def on_device(perturbation, obs_cells, obs_count, innovation, obs_scale):
    bands = lax.axis_size("lat")
    members, fine_rows, lon_cells = perturbation.shape
    coarse_rows = fine_rows // 2
    coarse_cols = lon_cells // 2
    slots = obs_cells.shape[1]
    half = members * coarse_rows
    scale = float((members * lax.axis_size("mem") - 1) ** (-0.5))
    t1, t2 = lon_blocks(coarse_cols)
    tables = jnp.asarray(lat_tables(bands, coarse_rows))
    groups = lax.axis_size("mem")
    place = jnp.stack([lax.axis_index("mem"), lax.axis_index("lat")]).astype(jnp.int32)

    smem = pl.BlockSpec(memory_space=pltpu.SMEM)
    vmem = pl.BlockSpec(memory_space=pltpu.VMEM)
    anywhere = pl.BlockSpec(memory_space=pl.ANY)
    far = pl.BlockSpec(memory_space=pltpu.HBM)
    params = pltpu.CompilerParams(vmem_limit_bytes=VMEM_LIMIT)
    f32 = functools.partial(jax.ShapeDtypeStruct, dtype=jnp.float32)

    field = perturbation.reshape(members * fine_rows, lon_cells)
    own = pl.pallas_call(
        functools.partial(prepare_kernel, members=members, fine_rows=fine_rows),
        out_shape=f32((members + META, slots)),
        in_specs=[smem, far] + [vmem] * 3,
        out_specs=vmem,
        scratch_shapes=[
            pltpu.VMEM((8, slots), jnp.float32),
            pltpu.VMEM((slots, 128), jnp.float32),
            pltpu.VMEM((members + META, slots + 512), jnp.float32),
            pltpu.VMEM(field.shape, field.dtype),
            pltpu.SemaphoreType.DMA((1,)),
        ],
        cost_estimate=pl.CostEstimate(flops=4 * 10**9, bytes_accessed=2 * 10**6, transcendentals=0),
        name="prepare",
    )(obs_count, field, obs_cells, innovation, obs_scale)
    near = []
    for d in range(-REACH, REACH + 1):
        near.append(lax.ppermute(own, "lat", [(s, s - d) for s in range(bands) if 0 <= s - d < bands]) if d else own)
    near = jnp.stack(near)
    bound = near[:, members + 4, :128].astype(jnp.int32)

    padded = slots + WINDOW
    scratch = [
        pltpu.VMEM((2 * half, padded), jnp.bfloat16),
        pltpu.VMEM((8, padded), jnp.float32),
        pltpu.VMEM((half, coarse_cols + BLK), jnp.float32),
    ]
    tiles = slots // 128
    width = lon_cells // groups
    state, hits, steps, controls, images = None, None, [], [], []
    for iteration in range(ITERS):
        order = min(iteration, 2)
        ins = [place, bound, near, tables, t2] + [[], [obs_cells, hits], [state, hits]][order]
        block = (groups * bands, tiles + (0 if iteration else 2 * (tiles // groups)), 128)
        outs = [f32(block), f32((half, coarse_cols)), f32((8, slots))]
        outs += [f32((6, bands, tiles, 128)), f32((1, 128))] if iteration else []
        got = pl.pallas_call(
            functools.partial(
                iter_kernel, members=members, coarse_rows=coarse_rows, scale2=scale * scale, order=order, bands=bands, groups=groups
            ),
            out_shape=outs,
            in_specs=[smem] * 2 + [far] * 3 + ([far, anywhere] if iteration else []),
            out_specs=[anywhere, far, vmem] + ([far, vmem] if iteration else []),
            scratch_shapes=scratch
            + [pltpu.VMEM((8, padded), jnp.float32)]
            + [pltpu.VMEM((2 * half, coarse_cols + BLK), jnp.bfloat16), pltpu.VMEM((members + META, padded), jnp.float32)]
            + [pltpu.VMEM(block, jnp.float32)]
            + ([pltpu.VMEM(hits.shape, jnp.float32)] + [pltpu.VMEM((6, bands, tiles, 128), jnp.float32)] * 2 if iteration else [])
            + [pltpu.VMEM(near.shape, jnp.float32), pltpu.VMEM(tables.shape[2:], jnp.float32), pltpu.VMEM(t2.shape, t2.dtype)]
            + [pltpu.VMEM((half, coarse_cols), jnp.float32), pltpu.SemaphoreType.DMA((6,))],
            cost_estimate=pl.CostEstimate(flops=7 * 10**9, bytes_accessed=3 * 10**6, transcendentals=0),
            name="iterate",
        )(*ins)
        if iteration:
            state = got[3]
            steps.append(got[4])
        hits = lax.all_to_all(got[0], ("mem", "lat"), 0, 0, tiled=True)
        side = pl.pallas_call(
            functools.partial(side_kernel, members=members, fine_rows=fine_rows, coarse_rows=coarse_rows, scale=scale),
            out_shape=[f32((half, coarse_cols)), f32((groups, fine_rows, width))],
            in_specs=[smem] * 2 + [vmem] + [far] * 5,
            out_specs=[vmem] * 2,
            scratch_shapes=scratch
            + [pltpu.VMEM(near.shape, jnp.float32), pltpu.VMEM(tables.shape[2:], jnp.float32), pltpu.VMEM(t1.shape, t1.dtype)]
            + [pltpu.VMEM((half, coarse_cols), jnp.float32), pltpu.VMEM(field.shape, field.dtype), pltpu.SemaphoreType.DMA((5,))],
            cost_estimate=pl.CostEstimate(flops=4 * 10**9, bytes_accessed=6 * 10**6, transcendentals=0),
            name="side",
        )
        control, image = side(place, bound, got[2], near, tables, t1, got[1], field)
        controls.append(control)
        images.append(image)
    control, image, *away = pl.pallas_call(
        combine_kernel,
        out_shape=[f32((half, coarse_cols))] + [f32((fine_rows, width))] * groups,
        in_specs=[smem, vmem, anywhere] + [vmem] * (3 * ITERS - 1),
        out_specs=[vmem] * (1 + groups),
        scratch_shapes=[pltpu.VMEM(hits.shape, jnp.float32)],
        cost_estimate=pl.CostEstimate(flops=10**7, bytes_accessed=4 * 10**6, transcendentals=0),
        compiler_params=params,
        name="combine",
    )(place, state, hits, *steps, *controls, *images)
    for n, block in enumerate(away):
        image = image + lax.ppermute(block, "mem", [(i, i ^ (n + 1)) for i in range(groups)])
    return control.reshape(members, coarse_rows, coarse_cols), image


def solution(mesh):
    in_specs = (P("mem", "lat", None), P("lat", None), P("lat"), P("lat", None), P("lat", None))
    out_specs = (P("mem", "lat", None), P("lat", "mem"))
    return jax.shard_map(on_device, mesh=mesh, in_specs=in_specs, out_specs=out_specs, check_vma=False)
```

```python
import functools

import jax
import jax.numpy as jnp
import numpy as np
from jax import lax
from jax.experimental import pallas as pl
from jax.experimental.pallas import tpu as pltpu
from jax.sharding import PartitionSpec as P

HALO = 8
LSIG = 3
ITERS = 3
REACH = 2
NREL = 2 * REACH + 1
BLK = 256
EDGE = 128
META = 8
WINDOW = 640


def lat_tables(bands, coarse_rows):
    rows = bands * coarse_rows
    offset = np.arange(rows)[:, None] - np.arange(rows)[None, :]
    spread = HALO / 2.0
    r1 = np.where(np.abs(offset) <= HALO, 0.5 * np.exp(-offset * offset / (2.0 * spread * spread)), 0.0)
    r2 = r1 @ r1
    out = np.zeros((bands, 2, NREL, coarse_rows, 128), np.float32)
    for b in range(bands):
        for d in range(NREL):
            s = b + d - REACH
            if 0 <= s < bands:
                own = slice(b * coarse_rows, (b + 1) * coarse_rows)
                other = slice(s * coarse_rows, (s + 1) * coarse_rows)
                out[b, 0, d, :, :coarse_rows] = r2[own, other]
                out[b, 1, d, :, :coarse_rows] = r1[own, other]
    return out


def lon_blocks(coarse_cols):
    d = np.arange(coarse_cols)
    d = np.minimum(d, coarse_cols - d).astype(np.float32)
    c1 = np.exp(-d * d / np.float32(2.0 * LSIG * LSIG)).astype(np.float32).astype(np.float64)
    c2 = np.real(np.fft.ifft(np.fft.fft(c1) ** 2))
    away = np.arange(BLK + 2 * EDGE)[:, None] - EDGE - np.arange(BLK)[None, :]
    inside = np.abs(away) <= EDGE
    blocks = []
    for c in (c1, c2):
        t = jnp.asarray(np.where(inside, c[away % coarse_cols], 0.0).astype(np.float32))
        hi = t.astype(jnp.bfloat16)
        lo = (t - hi.astype(jnp.float32)).astype(jnp.bfloat16)
        blocks.append(jnp.stack([hi, lo]))
    return blocks


def split(a):
    hi = a.astype(jnp.bfloat16)
    return hi, (a - hi.astype(jnp.float32)).astype(jnp.bfloat16)


def dot(a, b, dims=((1,), (0,))):
    return lax.dot_general(a, b, (dims, ((), ())), preferred_element_type=jnp.float32)


def full(ref_shape, dim):
    return lax.broadcasted_iota(jnp.int32, ref_shape, dim).astype(jnp.float32)


def hat_of(x, count):
    middle = 0.5 * (count - 1)
    near = x - middle
    near = jnp.where(jnp.abs(near) > middle + 0.75, float(count), near).astype(jnp.bfloat16)
    j = (full((count, x.shape[1]), 0) - middle).astype(jnp.bfloat16)
    one = jnp.asarray(1, jnp.bfloat16)
    return jnp.maximum(one - jnp.abs(near - j), jnp.asarray(0, jnp.bfloat16))


def pieces(a):
    out = []
    for _ in range(3):
        out.append(a.astype(jnp.bfloat16))
        a = a - out[-1].astype(jnp.float32)
    return out


def count(mask):
    return jnp.sum(jnp.where(mask, 1.0, 0.0)).astype(jnp.int32)


def fetch(*copies):
    started = [pltpu.make_async_copy(*copy) for copy in copies]
    for copy in started:
        copy.start()
    return started


def prepare_kernel(count_ref, far_ref, cell_ref, innovation_ref, scale_ref, out_ref, key_ref, kcol_ref, srt_ref, p_ref, sem, *, members, fine_rows):
    ready = fetch((far_ref, p_ref, sem.at[0]))
    lon = p_ref.shape[1]
    slots = cell_ref.shape[1]
    cell = cell_ref[...].astype(jnp.float32)
    row = jnp.floor((cell + 0.5) / float(lon))
    col = cell - row * float(lon)
    dead = full((1, slots), 1) >= count_ref[0].astype(jnp.float32)
    signed = jnp.where(dead, -scale_ref[...], scale_ref[...])
    key = jnp.where(dead, col + float(lon), col) * float(slots) + full((1, slots), 1)
    key_ref[0:1, :] = key
    top = jnp.floor(key / 65536.0)
    low = key - top * 65536.0
    mid = jnp.floor(low / 256.0)
    parts = jnp.concatenate([top, mid, low - mid * 256.0, jnp.zeros((13, slots), jnp.float32)], axis=0).astype(jnp.bfloat16)
    r = full((16, 128), 0)
    base = jnp.where(r == 0.0, 65536.0, jnp.where(r == 1.0, 256.0, jnp.where(r == 2.0, 1.0, 0.0))).astype(jnp.bfloat16)
    kcol_ref[...] = dot(parts, base, ((0,), (0,)))

    def rank(n, _):
        at = pl.ds(pl.multiple_of(n * 128, 128), 128)
        below = jnp.where(kcol_ref[...] < key_ref[0:1, at], 1.0, 0.0)
        below = jnp.sum(below.reshape(slots // 64, 64, 128), axis=0)
        key_ref[1:2, at] = jnp.sum(below, axis=0, keepdims=True)
        return 0

    lax.fori_loop(0, slots // 128, rank, 0)

    srt_ref[...] = jnp.zeros_like(srt_ref)
    high = jnp.floor(col / 256.0)
    rows = [high.astype(jnp.bfloat16), (col - high * 256.0).astype(jnp.bfloat16), row.astype(jnp.bfloat16)]
    rows += pieces(innovation_ref[...]) + pieces(signed)
    rows.append(jnp.zeros((16 - len(rows), slots), jnp.bfloat16))
    rows = jnp.concatenate([a.astype(jnp.float32) for a in rows], axis=0).astype(jnp.bfloat16)

    def permute(n, _):
        at = pl.ds(pl.multiple_of(n * BLK, BLK), BLK)
        place = key_ref[1:2, :] - (n * BLK).astype(jnp.float32)
        one = jnp.where(full((BLK, slots), 0) == place, 1.0, 0.0).astype(jnp.bfloat16)
        got = dot(rows, one, ((1,), (1,)))
        srt_ref[members : members + 1, at] = 128.0 * got[0:1] + 0.5 * got[1:2]
        srt_ref[members + 1 : members + 2, at] = got[2:3]
        srt_ref[members + 2 : members + 3, at] = got[3:4] + got[4:5] + got[5:6]
        srt_ref[members + 3 : members + 4, at] = got[6:7] + got[7:8] + got[8:9]
        return 0

    lax.fori_loop(0, slots // BLK, permute, 0)

    lane = full((1, 128), 1)
    bounds = jnp.zeros((1, 128), jnp.float32)
    blocks = lon // (2 * BLK)
    for c in range(blocks + 1):
        first = jnp.where(jnp.logical_and(jnp.logical_not(dead), col <= 2.0 * BLK * c - 2.0), 1.0, 0.0)
        last = jnp.where(jnp.logical_and(jnp.logical_not(dead), col < 2.0 * BLK * (c + 1)), 1.0, 0.0)
        bounds = jnp.where(lane == float(c), jnp.sum(first, axis=1, keepdims=True), bounds)
        bounds = jnp.where(lane == float(64 + c), jnp.sum(last, axis=1, keepdims=True), bounds)
    srt_ref[members + 4 : members + 5, 0:128] = bounds

    live = jnp.logical_not(dead)
    edges = [count(jnp.logical_and(live, col < float(c * BLK))) for c in range(lon // BLK + 1)]

    def window(c, start):
        at = pl.ds(pl.multiple_of(start, 128), 512)
        cols = 2.0 * srt_ref[members : members + 1, at] - float(c * BLK)
        one = jnp.where(full((BLK, 512), 0) == cols, 1.0, 0.0).astype(jnp.bfloat16)
        got = dot(p_ref[:, c * BLK : (c + 1) * BLK], one).reshape(members, fine_rows, 512)
        mask = jnp.where(full((fine_rows, 512), 0) == srt_ref[members + 1 : members + 2, at], 1.0, 0.0)
        srt_ref[0:members, at] = srt_ref[0:members, at] + jnp.sum(got * mask[None], axis=1)

    starts = [s // 128 * 128 for s in edges[:-1]]
    ready[0].wait()
    for c, start in enumerate(starts):
        window(c, start)
    for c, start in enumerate(starts):

        def more(i, _, c=c, start=start):
            window(c, start + i * 512)
            return 0

        lax.fori_loop(1, (edges[c + 1] - start + 511) // 512, more, 0)
    out_ref[...] = srt_ref[:, :slots]


def windows(bound_ref, d, c):
    s, e = bound_ref[d, 0, c], bound_ref[d, 0, 64 + c]
    start = s // 128 * 128
    return start, jnp.where(e > s, (e - start + WINDOW - 1) // WINDOW, 0)


def scatter(bound_ref, q_ref, tab, v_of, first, last, lhs_ref, at_ref, x_ref, members, coarse_rows):
    slots = q_ref.shape[2]
    half = members * coarse_rows
    blocks = x_ref.shape[1] // BLK - 1
    x_ref[...] = jnp.zeros_like(x_ref)
    lhs_ref[:, slots:] = jnp.zeros((2 * half, WINDOW), jnp.bfloat16)
    at_ref[...] = jnp.zeros_like(at_ref)

    def band(d, _):
        row = jnp.floor(q_ref[d, members + 1 : members + 2, :] * 0.5)
        v = v_of(d)
        at_ref[0:1, :slots] = q_ref[d, members : members + 1, :]
        weights = jnp.zeros((coarse_rows, slots), jnp.float32)
        taps = tab(d)
        for r in range(coarse_rows):
            weights = jnp.where(row == float(r), taps[:, r : r + 1], weights)
        weights = weights * v
        for k in range(members):
            hi, lo = split(weights * q_ref[d, k : k + 1, :])
            lhs_ref[k * coarse_rows : (k + 1) * coarse_rows, :slots] = hi
            lhs_ref[half + k * coarse_rows : half + (k + 1) * coarse_rows, :slots] = lo

        def one(c, start):
            at = pl.ds(pl.multiple_of(start, 128), WINDOW)
            hat = hat_of(at_ref[0:1, at] - c * float(BLK), BLK)
            got = dot(lhs_ref[:, at], hat, ((1,), (1,)))
            return got[:half] + got[half:]

        for c in range(blocks):
            to = slice(c * BLK, (c + 1) * BLK)
            x_ref[:, to] = x_ref[:, to] + one(float(c), windows(bound_ref, d, c)[0])

        def rest(c, _):
            start, trips = windows(bound_ref, d, c)
            to = pl.ds(pl.multiple_of(c * BLK, BLK), BLK)

            def more(i, _):
                x_ref[:, to] = x_ref[:, to] + one(c.astype(jnp.float32), start + i * WINDOW)
                return 0

            return lax.fori_loop(jnp.where(c < blocks, 1, 0), trips, more, 0)

        return lax.fori_loop(0, blocks + 1, rest, 0)

    lax.fori_loop(first, last, band, 0)
    x_ref[:, :EDGE] = x_ref[:, :EDGE] + x_ref[:, blocks * BLK : blocks * BLK + EDGE]


def lon_filter(x, t_ref):
    _, cols = x.shape
    ext = jnp.concatenate([x[:, cols - EDGE :], x, x[:, :EDGE]], axis=1)
    hi, lo = split(ext)
    parts = []
    for c in range(cols // BLK):
        at = slice(c * BLK, (c + 1) * BLK + 2 * EDGE)
        parts.append(dot(hi[:, at], t_ref[0]) + dot(lo[:, at], t_ref[0]) + dot(hi[:, at], t_ref[1]))
    return jnp.concatenate(parts, axis=1)


def step_of(hits, v, w):
    gg = jnp.full((1, 128), jnp.sum(v * hits), jnp.float32)
    cc = jnp.full((1, 128), jnp.sum(w * hits * hits), jnp.float32)
    return gg / (gg + cc + 1e-6)


def sum_mem(parts, bands):
    return jnp.sum(parts.reshape((parts.shape[0] // bands, bands) + parts.shape[1:]), axis=0)


def pull_of(target, signed):
    bounded = jnp.tanh(target / jnp.abs(signed))
    return jnp.where(signed > 0.0, signed * bounded, 0.0), jnp.where(signed > 0.0, 1.0 - bounded * bounded, 0.0)


def lay_rows(rows_ref, tile_of, bands):
    for d in range(NREL):
        tile = tile_of(jnp.clip(bands[0] + d - REACH, 0, bands[1] - 1))
        for i in range(tile.shape[0]):
            rows_ref[d : d + 1, i * 128 : (i + 1) * 128] = tile[i : i + 1, :]


def iter_kernel(place_ref, bound_ref, q_ref, tab_ref, t2_ref, *refs, members, coarse_rows, scale2, order, bands, groups):
    slots = q_ref.shape[2]
    tiles = slots // 128
    share = tiles // groups
    band = place_ref[1]
    if order == 0:
        part_ref, b_ref, vrow_ref, lhs_ref, at_ref, x_ref, rows_ref, bhl_ref, own_ref = refs
        for d in range(NREL):
            vrow_ref[d : d + 1, :] = pull_of(q_ref[d, members + 2 : members + 3, :], q_ref[d, members + 3 : members + 4, :])[0]
    else:
        old_ref, hits_ref, part_ref, b_ref, vrow_ref, state_ref, step_ref, lhs_ref, at_ref, x_ref, rows_ref, bhl_ref, own_ref = refs
        hits = sum_mem(hits_ref[:, :tiles, :], bands)
        if order == 1:
            for g in range(groups):
                mine = slice(g * bands, (g + 1) * bands)
                at = slice(g * share, (g + 1) * share)
                state_ref[0, :, at, :] = hits_ref[mine, tiles : tiles + share, :]
                state_ref[1, :, at, :] = hits_ref[mine, tiles + share : tiles + 2 * share, :]
            v, w = pull_of(state_ref[0], state_ref[1])
            observed, lam = 0.0, 0.0
        else:
            state_ref[0:2] = old_ref[0:2]
            v, w, observed, lam = old_ref[2], old_ref[3], old_ref[4], old_ref[5]
        step = step_of(hits, v, w)
        step_ref[...] = step
        step = step[0:1, 0:1][None]
        observed = observed + step * hits
        lam = lam + step * v
        pull, weight = pull_of(state_ref[0] - observed, state_ref[1])
        state_ref[2] = pull - lam
        state_ref[3] = weight
        state_ref[4] = observed
        state_ref[5] = lam
        lay_rows(vrow_ref, lambda b: state_ref[2, b], (band, bands))

    def v_of(d):
        return vrow_ref[pl.ds(d, 1), :]

    half = members * coarse_rows
    blocks = x_ref.shape[1] // BLK - 1
    cols = blocks * BLK
    scatter(bound_ref, q_ref, lambda d: tab_ref[band, 0, d], v_of, 0, NREL, lhs_ref, at_ref, x_ref, members, coarse_rows)
    b = lon_filter(x_ref[:, :cols], t2_ref)
    b_ref[...] = b
    hi, lo = split(b)
    bhl_ref[:half, :cols] = hi
    bhl_ref[half:, :cols] = lo
    bhl_ref[:, cols:] = bhl_ref[:, :BLK]
    own_ref[:, :slots] = q_ref[REACH]
    own_ref[:, slots:] = jnp.zeros((members + META, WINDOW), jnp.float32)
    rows_ref[...] = jnp.zeros_like(rows_ref)

    def gather(c, start):
        at = pl.ds(pl.multiple_of(start, 128), WINDOW)
        row = jnp.floor(own_ref[members + 1 : members + 2, at] * 0.5)
        hat = hat_of(own_ref[members : members + 1, at] - jnp.float32(c) * float(BLK), BLK)
        got = dot(bhl_ref[:, pl.ds(pl.multiple_of(c * BLK, BLK), BLK)], hat)
        mask = jnp.where(full((coarse_rows, WINDOW), 0) == row, scale2, 0.0)
        total = jnp.zeros((coarse_rows, WINDOW), jnp.float32)
        for k in range(members):
            r = slice(k * coarse_rows, (k + 1) * coarse_rows)
            r2 = slice(half + k * coarse_rows, half + (k + 1) * coarse_rows)
            total = total + own_ref[k : k + 1, at] * (got[r] + got[r2])
        rows_ref[0:1, at] = rows_ref[0:1, at] + jnp.sum(total * mask, axis=0, keepdims=True)

    for c in range(blocks):
        gather(c, windows(bound_ref, REACH, c)[0])

    def rest(c, _):
        start, trips = windows(bound_ref, REACH, c)

        def more(i, _):
            gather(c, start + i * WINDOW)
            return 0

        return lax.fori_loop(jnp.where(c < blocks, 1, 0), trips, more, 0)

    lax.fori_loop(0, blocks + 1, rest, 0)
    for i in range(tiles):
        part_ref[0, i : i + 1, :] = rows_ref[0:1, i * 128 : (i + 1) * 128]
    if order == 0:
        for r in range(2):
            mine = pl.ds(pl.multiple_of(place_ref[0] * (share * 128), 128), share * 128)
            row = q_ref[REACH, members + 2 + r : members + 3 + r, mine]
            for i in range(share):
                to = tiles + r * share + i
                part_ref[0, to : to + 1, :] = row[:, i * 128 : (i + 1) * 128]
    part_ref[1:] = jnp.broadcast_to(part_ref[0][None], (part_ref.shape[0] - 1,) + part_ref.shape[1:])


def side_kernel(
    place_ref, bound_ref, vrow_ref, q_ref, tab_ref, t1_ref, b_ref, p_ref, control_ref, image_ref, lhs_ref, at_ref, x_ref,
    *, members, fine_rows, coarse_rows, scale,
):
    def v_of(d):
        return vrow_ref[pl.ds(d, 1), :]

    tab = lambda d: tab_ref[place_ref[1], 1, d]
    scatter(bound_ref, q_ref, tab, v_of, REACH - 1, REACH + 2, lhs_ref, at_ref, x_ref, members, coarse_rows)
    control_ref[...] = scale * lon_filter(x_ref[:, : b_ref.shape[1]], t1_ref)

    b = b_ref[...]
    half, cols = b.shape
    wide = 2 * half
    repeat = jnp.where(
        lax.broadcasted_iota(jnp.int32, (wide, half), 0) // 2 == lax.broadcasted_iota(jnp.int32, (wide, half), 1), 1.0, 0.0
    ).astype(jnp.bfloat16)
    hi, lo = split(jnp.concatenate([b, b[:, :EDGE]], axis=1))
    hi = dot(repeat, hi).astype(jnp.bfloat16)
    lo = dot(repeat, lo).astype(jnp.bfloat16)
    hat = jnp.maximum(1.0 - jnp.abs(0.5 * full((2 * EDGE, 2 * EDGE), 1) - full((2 * EDGE, 2 * EDGE), 0)), 0.0)
    hat = hat.astype(jnp.bfloat16)
    for f in range(cols // EDGE):
        at = slice(f * EDGE, f * EDGE + 2 * EDGE)
        fine = slice(2 * f * EDGE, 2 * (f + 1) * EDGE)
        field = dot(hi[:, at], hat) + dot(lo[:, at], hat)
        product = p_ref[:, fine].astype(jnp.float32) * field
        part = (scale * scale) * jnp.sum(product.reshape(members, fine_rows, 2 * EDGE), axis=0)
        width = image_ref.shape[2]
        for start in range(0, 2 * EDGE, min(width, 2 * EDGE)):
            stop = start + min(width, 2 * EDGE)
            group, to = divmod(2 * f * EDGE + start, width)
            image_ref[group, :, to : to + stop - start] = part[:, start:stop]


def combine_kernel(place_ref, state_ref, hits_ref, *refs):
    steps, controls, images = refs[: ITERS - 1], refs[ITERS - 1 : 2 * ITERS - 1], refs[2 * ITERS - 1 : 3 * ITERS - 1]
    control_ref, block_refs = refs[3 * ITERS - 1], refs[3 * ITERS :]
    last = step_of(sum_mem(hits_ref[...], state_ref.shape[1]), state_ref[2], state_ref[3])[0:1, 0:1]
    steps = [s[0:1, 0:1] for s in steps] + [last]
    for away, block_ref in enumerate(block_refs):
        block_ref[...] = sum(s * i[place_ref[0] ^ away] for s, i in zip(steps, images))
    control_ref[...] = sum(s * c[...] for s, c in zip(steps, controls))


def on_device(perturbation, obs_cells, obs_count, innovation, obs_scale):
    bands = lax.axis_size("lat")
    members, fine_rows, lon_cells = perturbation.shape
    coarse_rows = fine_rows // 2
    coarse_cols = lon_cells // 2
    slots = obs_cells.shape[1]
    half = members * coarse_rows
    scale = float((members * lax.axis_size("mem") - 1) ** (-0.5))
    t1, t2 = lon_blocks(coarse_cols)
    tables = jnp.asarray(lat_tables(bands, coarse_rows))
    groups = lax.axis_size("mem")
    place = jnp.stack([lax.axis_index("mem"), lax.axis_index("lat")]).astype(jnp.int32)

    smem = pl.BlockSpec(memory_space=pltpu.SMEM)
    vmem = pl.BlockSpec(memory_space=pltpu.VMEM)
    f32 = functools.partial(jax.ShapeDtypeStruct, dtype=jnp.float32)

    field = perturbation.reshape(members * fine_rows, lon_cells)
    own = pl.pallas_call(
        functools.partial(prepare_kernel, members=members, fine_rows=fine_rows),
        out_shape=f32((members + META, slots)),
        in_specs=[smem, pl.BlockSpec(memory_space=pltpu.HBM)] + [vmem] * 3,
        out_specs=vmem,
        scratch_shapes=[
            pltpu.VMEM((8, slots), jnp.float32),
            pltpu.VMEM((slots, 128), jnp.float32),
            pltpu.VMEM((members + META, slots + 512), jnp.float32),
            pltpu.VMEM(field.shape, field.dtype),
            pltpu.SemaphoreType.DMA((1,)),
        ],
        cost_estimate=pl.CostEstimate(flops=4 * 10**9, bytes_accessed=2 * 10**6, transcendentals=0),
        name="prepare",
    )(obs_count, field, obs_cells, innovation, obs_scale)
    near = []
    for d in range(-REACH, REACH + 1):
        near.append(lax.ppermute(own, "lat", [(s, s - d) for s in range(bands) if 0 <= s - d < bands]) if d else own)
    near = jnp.stack(near)
    bound = near[:, members + 4 : members + 5, :128].astype(jnp.int32)

    padded = slots + WINDOW
    scratch = [
        pltpu.VMEM((2 * half, padded), jnp.bfloat16),
        pltpu.VMEM((8, padded), jnp.float32),
        pltpu.VMEM((half, coarse_cols + BLK), jnp.float32),
    ]
    tiles = slots // 128
    width = lon_cells // groups
    state, hits, steps, controls, images = None, None, [], [], []
    for iteration in range(ITERS):
        order = min(iteration, 2)
        ins = [place, bound, near, tables, t2] + [[], [obs_cells, hits], [state, hits]][order]
        block = (groups * bands, tiles + (0 if iteration else 2 * (tiles // groups)), 128)
        outs = [f32(block), f32((half, coarse_cols)), f32((8, slots))]
        outs += [f32((6, bands, tiles, 128)), f32((1, 128))] if iteration else []
        got = pl.pallas_call(
            functools.partial(
                iter_kernel, members=members, coarse_rows=coarse_rows, scale2=scale * scale, order=order, bands=bands, groups=groups
            ),
            out_shape=outs,
            in_specs=[smem] * 2 + [vmem] * (len(ins) - 2),
            out_specs=[vmem] * len(outs),
            scratch_shapes=scratch
            + [pltpu.VMEM((8, padded), jnp.float32)]
            + [pltpu.VMEM((2 * half, coarse_cols + BLK), jnp.bfloat16), pltpu.VMEM((members + META, padded), jnp.float32)],
            cost_estimate=pl.CostEstimate(flops=7 * 10**9, bytes_accessed=3 * 10**6, transcendentals=0),
            name="iterate",
        )(*ins)
        if iteration:
            state = got[3]
            steps.append(got[4])
        hits = lax.all_to_all(got[0], ("mem", "lat"), 0, 0, tiled=True)
        side = pl.pallas_call(
            functools.partial(side_kernel, members=members, fine_rows=fine_rows, coarse_rows=coarse_rows, scale=scale),
            out_shape=[f32((half, coarse_cols)), f32((groups, fine_rows, width))],
            in_specs=[smem] * 2 + [vmem] * 6,
            out_specs=[vmem] * 2,
            scratch_shapes=scratch,
            cost_estimate=pl.CostEstimate(flops=4 * 10**9, bytes_accessed=6 * 10**6, transcendentals=0),
            name="side",
        )
        control, image = side(place, bound, got[2], near, tables, t1, got[1], field)
        controls.append(control)
        images.append(image)
    control, image, *away = pl.pallas_call(
        combine_kernel,
        out_shape=[f32((half, coarse_cols))] + [f32((fine_rows, width))] * groups,
        in_specs=[smem] + [vmem] * (3 * ITERS + 1),
        out_specs=[vmem] * (1 + groups),
        cost_estimate=pl.CostEstimate(flops=10**7, bytes_accessed=4 * 10**6, transcendentals=0),
        name="combine",
    )(place, state, hits, *steps, *controls, *images)
    for n, block in enumerate(away):
        image = image + lax.ppermute(block, "mem", [(i, i ^ (n + 1)) for i in range(groups)])
    return control.reshape(members, coarse_rows, coarse_cols), image


def solution(mesh):
    in_specs = (P("mem", "lat", None), P("lat", None), P("lat"), P("lat", None), P("lat", None))
    out_specs = (P("mem", "lat", None), P("lat", "mem"))
    return jax.shard_map(on_device, mesh=mesh, in_specs=in_specs, out_specs=out_specs, check_vma=False)
```
